8 devices in a mesh: dp: 8 (over z, y, x, core).
Axes of the slice: x: 2, y: 2, z: 1, core: 2. Of those that a mesh axis runs over, the one named last changes fastest.
Arguments:
- g_mat: bfloat16 [8, 14155776], P('dp')
- g_vec: bfloat16 [8, 19968], P('dp')
- p_mat: float32 [14155776], P('dp')
- m_mat: float32 [14155776], P('dp')
- v_mat: float32 [14155776], P('dp')
- p_vec: float32 [19968], replicated
- m_vec: float32 [19968], replicated
- v_vec: float32 [19968], replicated
- learn_rate: float32 [], replicated
Outputs:
- output 1: float32 [14155776], P('dp')
- output 2: float32 [14155776], P('dp')
- output 3: float32 [14155776], P('dp')
- output 4: float32 [19968], replicated
- output 5: float32 [19968], replicated
- output 6: float32 [19968], replicated
- output 7: bfloat16 [14155776], replicated
All inputs are finite; a program needn't handle non-finite values.
Results may differ from the reference program's by a relative error of at most 0.001.
Values are sent between devices in bfloat16 or wider.
A program may use at most 1 GiB of HBM per device.

```python
import jax
import jax.numpy as jnp
from jax import lax

D = 768
FF = 3072
TP = 1
DP = 8
STEP = 10

N_MAT = (8 * D * D + 4 * D * FF) // TP
N_VEC = 2 * ((3 * D + FF) // TP) + 12 * D
N_ALL = N_MAT + N_VEC
ELEM_SCALE = N_ALL ** -0.5
NOISE_GAIN = 6.0 * DP ** 0.5
ADAM_BETA1 = 0.9
ADAM_BETA2 = 0.98
ADAM_EPS = 1e-8
WEIGHT_DECAY = 0.01
MAX_NORM = 1.0
NORM_EPS = 1e-6
BIAS_ONE = 1.0 - ADAM_BETA1 ** STEP
BIAS_TWO = 1.0 - ADAM_BETA2 ** STEP


def draw_local_grads(draw_key, elem_count):
    key_base, key_dev = jax.random.split(draw_key)
    base_part = 2.0 * jax.random.normal(key_base, (elem_count,), jnp.float32)
    dev_keys = jax.random.split(key_dev, DP)

    def one_device(dev_key):
        noise_part = jax.random.normal(dev_key, (elem_count,), jnp.float32)
        return ((base_part + NOISE_GAIN * noise_part) * ELEM_SCALE).astype(jnp.bfloat16)

    return lax.map(one_device, dev_keys)


def setup_inputs(seed: int = 0) -> dict:
    key_list = jax.random.split(jax.random.key(seed), 9)
    return dict(
        g_mat=draw_local_grads(key_list[0], N_MAT),
        g_vec=draw_local_grads(key_list[1], N_VEC),
        p_mat=0.02 * jax.random.normal(key_list[2], (N_MAT,), jnp.float32),
        m_mat=0.1 * ELEM_SCALE * jax.random.normal(key_list[3], (N_MAT,), jnp.float32),
        v_mat=0.05 * ELEM_SCALE * ELEM_SCALE * jax.random.uniform(key_list[4], (N_MAT,), jnp.float32, minval=0.25, maxval=1.75),
        p_vec=0.05 * jax.random.normal(key_list[5], (N_VEC,), jnp.float32),
        m_vec=0.1 * ELEM_SCALE * jax.random.normal(key_list[6], (N_VEC,), jnp.float32),
        v_vec=0.05 * ELEM_SCALE * ELEM_SCALE * jax.random.uniform(key_list[7], (N_VEC,), jnp.float32, minval=0.25, maxval=1.75),
        learn_rate=jax.random.uniform(key_list[8], (), jnp.float32, minval=0.002, maxval=0.008),
    )


def mean_over_devices(local_grads):
    def add_row(acc_sum, grad_row):
        return acc_sum + grad_row.astype(jnp.float32), None

    total_sum, _ = lax.scan(add_row, jnp.zeros(local_grads.shape[1:], jnp.float32), local_grads)
    return total_sum / local_grads.shape[0]


def adam_update(grad_vals, param_vals, moment_one, moment_two, learn_rate, decay_rate):
    new_one = ADAM_BETA1 * moment_one + (1.0 - ADAM_BETA1) * grad_vals
    new_two = ADAM_BETA2 * moment_two + (1.0 - ADAM_BETA2) * grad_vals * grad_vals
    direction = (new_one / BIAS_ONE) / (jnp.sqrt(new_two / BIAS_TWO) + ADAM_EPS)
    return param_vals - learn_rate * (direction + decay_rate * param_vals), new_one, new_two


def reference(g_mat, g_vec, p_mat, m_mat, v_mat, p_vec, m_vec, v_vec, learn_rate):
    grad_mat = mean_over_devices(g_mat)
    grad_vec = mean_over_devices(g_vec)
    norm_sq = jnp.sum(grad_mat * grad_mat) + jnp.sum(grad_vec * grad_vec)
    clip_scale = jnp.minimum(1.0, MAX_NORM / (jnp.sqrt(norm_sq) + NORM_EPS))
    new_p_mat, new_m_mat, new_v_mat = adam_update(grad_mat * clip_scale, p_mat, m_mat, v_mat, learn_rate, WEIGHT_DECAY)
    new_p_vec, new_m_vec, new_v_vec = adam_update(grad_vec * clip_scale, p_vec, m_vec, v_vec, learn_rate, 0.0)
    return (new_p_mat, new_m_mat, new_v_mat, new_p_vec, new_m_vec, new_v_vec, new_p_mat.astype(jnp.bfloat16))
```

```python
import functools

import jax
import jax.numpy as jnp
from jax import lax
from jax.experimental import pallas as pl
from jax.experimental.pallas import tpu as pltpu
from jax.sharding import PartitionSpec as P

STEP = 10
ADAM_BETA1 = 0.9
ADAM_BETA2 = 0.98
ADAM_EPS = 1e-8
WEIGHT_DECAY = 0.01
MAX_NORM = 1.0
NORM_EPS = 1e-6
BIAS_ONE = 1.0 - ADAM_BETA1 ** STEP
BIAS_TWO = 1.0 - ADAM_BETA2 ** STEP

LANES = 128
N_DEV = 8
NC = 18
NRAW = 8
LAG = 2
VROWS = 80
MESH = pl.DeviceIdType.MESH
F32 = jnp.float32
BF16 = jnp.bfloat16


def adam_update(grad_vals, param_vals, moment_one, moment_two, learn_rate, decay_rate):
    new_one = ADAM_BETA1 * moment_one + (1.0 - ADAM_BETA1) * grad_vals
    new_two = ADAM_BETA2 * moment_two + (1.0 - ADAM_BETA2) * grad_vals * grad_vals
    direction = (new_one / BIAS_ONE) / (jnp.sqrt(new_two / BIAS_TWO) + ADAM_EPS)
    return param_vals - learn_rate * (direction + decay_rate * param_vals), new_one, new_two


def flip(device, mask):
    for bit in (1, 2, 4):
        if mask & bit:
            device = device + bit - 2 * bit * lax.rem(lax.div(device, bit), 2)
    return device


def step_kernel(
    half, rc, n_vec,
    g_hbm, gv_hbm, p_hbm, m_hbm, v_hbm, pv_ref, mv_ref, vv_ref, lr_ref,
    big, p_ref, m_ref, v_ref, pv_out, mv_out, vv_out,
    fin, raw, pk, rel, acc, norms, vraw, vpk, vland, vs1, vlx, vs2, vly, vfull,
    raw_sem, send_sem, rel_sem, rs, st_sem, ns_sem, nr_sem, vs_sem, vr_sem, ag_sem,
):
    piece_rows = 2 * half
    me = lax.axis_index("dp")
    core = lax.rem(me, 2)
    peer = {mask: flip(me, mask) for mask in range(1, N_DEV)}

    def remote(src, dst, ssem, rsem, mask):
        return pltpu.make_async_remote_copy(
            src_ref=src, dst_ref=dst, send_sem=ssem, recv_sem=rsem,
            device_id=(peer[mask],), device_id_type=MESH,
        )

    def rows(first, count, align=16):
        return pl.ds(pl.multiple_of(first, align), count)

    blocks = []
    for j in (0, 1):
        for h in (0, 1):
            via = (4, 2)[h]
            blocks.append(("send", h, 6 ^ j, via ^ j, h * 3 + j))
    for h in (0, 1):
        blocks.append(("send", h, (2, 4)[h] ^ 1, 1, h * 3 + 2))
        blocks.append(("own", h, (2, 4)[h], None, 14 + h))
    for j in (0, 1):
        for h in (0, 1):
            via = (4, 2)[h]
            blocks.append(("send", h, via ^ j, via ^ j, 6 + h * 3 + j))
    for h in (0, 1):
        blocks.append(("send", h, 1, 1, 6 + h * 3 + 2))
        blocks.append(("own", h, 0, None, 12 + h))
    n_blocks = len(blocks)
    send_slot = {}
    for b, block in enumerate(blocks):
        if block[0] == "send":
            send_slot[b] = len(send_slot)

    def raw_copy(b, c):
        _, h, mask, _, _ = blocks[b]
        piece = flip(me, mask) if mask else me
        start = (piece * piece_rows + h * half + c * rc) * LANES
        return pltpu.make_async_copy(
            g_hbm.at[:, pl.ds(pl.multiple_of(start, 2048), rc * LANES)],
            raw.at[b % NRAW], raw_sem.at[b % NRAW],
        )

    def block_copy(b, c):
        _, h, _, dest, slot = blocks[b]
        s = send_slot[b]
        par = lax.rem(c, 2)
        return remote(
            pk.at[par, s], big.at[rows(slot * half + c * rc, rc)],
            send_sem.at[par, s], rs.at[slot, c], dest,
        )

    def landed(slot, c):
        ref = big.at[rows(slot * half + c * rc, rc)]
        return remote(ref, ref, send_sem.at[0, 0], rs.at[slot, c], 1)

    def rel_copy(h, c):
        par = lax.rem(c, 2)
        return remote(
            rel.at[par, h], fin.at[rows(h * half + c * rc, rc)],
            rel_sem.at[par, h], rs.at[12 + h, c], (2, 4)[h],
        )

    state_copies = [
        pltpu.make_async_copy(src, dst, st_sem.at[i])
        for i, (src, dst) in enumerate(((p_hbm, p_ref), (m_hbm, m_ref), (v_hbm, v_ref)))
    ]
    vraw_copy = pltpu.make_async_copy(gv_hbm, vraw.at[:, pl.ds(0, n_vec)], st_sem.at[3])

    barrier = pltpu.get_barrier_semaphore()
    for mask in range(1, N_DEV):
        pl.semaphore_signal(barrier, inc=1, device_id=(peer[mask],), device_id_type=MESH)
    for b in range(NRAW):
        raw_copy(b, 0).start()
    vraw[:, pl.ds(n_vec // 1024 * 1024, 2 * VROWS * LANES - n_vec // 1024 * 1024)] = jnp.zeros(
        (1, 2 * VROWS * LANES - n_vec // 1024 * 1024), BF16)
    acc[...] = jnp.zeros_like(acc)
    pl.semaphore_wait(barrier, N_DEV - 1)

    step_rows = 64

    def pack_rows(src, dst, first):
        def body(i, _):
            vals = src[:, pl.ds(pl.multiple_of(i * step_rows * LANES, 2048), step_rows * LANES)]
            dst[rows(first + i * step_rows, step_rows), :] = (
                vals.astype(F32).reshape(step_rows, LANES).astype(BF16))
            return 0
        lax.fori_loop(0, rc // step_rows, body, 0)

    def send_chunk(c):
        par = lax.rem(c, 2)
        waiting = None
        for b, (kind, h, mask, dest, slot) in enumerate(blocks):
            raw_copy(b, c).wait()
            if kind == "send":
                @pl.when(c >= 2)
                def _():
                    block_copy(b, c - 2).wait_send()
                pack_rows(raw.at[b % NRAW], pk.at[par, send_slot[b]], 0)
            else:
                pack_rows(raw.at[b % NRAW], big, slot * half + c * rc)
            if b + NRAW < n_blocks:
                raw_copy(b + NRAW, c).start()
            else:
                @pl.when(c + 1 < NC)
                def _():
                    raw_copy(b + NRAW - n_blocks, c + 1).start()
            if waiting is not None:
                block_copy(waiting, c).start()
            waiting = b if kind == "send" else None
        if waiting is not None:
            block_copy(waiting, c).start()

    sum_rows = 32

    def relay_chunk(c):
        par = lax.rem(c, 2)
        for h in (0, 1):
            for j in range(3):
                landed(h * 3 + j, c).wait_recv()

            @pl.when(c >= 2)
            def _():
                rel_copy(h, c - 2).wait_send()

            def body(i, _):
                at = c * rc + i * sum_rows
                total = big[rows((14 + h) * half + at, sum_rows), :].astype(F32)
                for j in (2, 0, 1):
                    total = total + big[rows((h * 3 + j) * half + at, sum_rows), :].astype(F32)
                rel[par, h, rows(i * sum_rows, sum_rows), :] = total
                return 0
            lax.fori_loop(0, rc // sum_rows, body, 0)
        for h in (0, 1):
            rel_copy(h, c).start()

    def final_chunk(c):
        for h in (0, 1):
            for j in range(3):
                landed(6 + h * 3 + j, c).wait_recv()
            rel_copy(h, c).wait_recv()

            def body(i, sq):
                at = c * rc + i * sum_rows
                total = big[rows((12 + h) * half + at, sum_rows), :].astype(F32)
                for j in (2, 0, 1):
                    total = total + big[rows((6 + h * 3 + j) * half + at, sum_rows), :].astype(F32)
                total = total + fin[rows(h * half + at, sum_rows), :]
                fin[rows(h * half + at, sum_rows), :] = total
                total = total * total
                for k in range(sum_rows // 8):
                    sq = sq + total[8 * k:8 * k + 8]
                return sq
            acc[...] = lax.fori_loop(0, rc // sum_rows, body, acc[...])

    mine = rows(core * VROWS, VROWS)
    other = rows((1 - core) * VROWS, VROWS)
    vec_core = remote(vpk.at[other], vland, vs_sem.at[0], vr_sem.at[0], 1)
    vec_x = remote(vs1, vlx, vs_sem.at[1], vr_sem.at[1], 2)
    vec_y = remote(vs2, vly, vs_sem.at[2], vr_sem.at[2], 4)
    vec_back = remote(vfull.at[mine], vfull.at[mine], vs_sem.at[3], vr_sem.at[3], 1)
    vec_back_in = remote(vfull.at[other], vfull.at[other], vs_sem.at[3], vr_sem.at[3], 1)

    def vec_step(c):
        @pl.when(c == 1)
        def _():
            vraw_copy.wait()
            vpk[...] = vraw[...].astype(F32).reshape(2 * VROWS, LANES).astype(BF16)

        @pl.when(c == 2)
        def _():
            vec_core.start()

        @pl.when(c == 3)
        def _():
            vec_core.wait_recv()
            vs1[...] = vpk[mine, :].astype(F32) + vland[...].astype(F32)

        @pl.when(c == 4)
        def _():
            vec_x.start()

        @pl.when(c == 6)
        def _():
            vec_x.wait_recv()
            vs2[...] = vs1[...] + vlx[...]

        @pl.when(c == 7)
        def _():
            vec_y.start()

        @pl.when(c == 9)
        def _():
            vec_y.wait_recv()
            vfull[mine, :] = vs2[...] + vly[...]

        @pl.when(c == 10)
        def _():
            vec_back.start()

        @pl.when(c == 12)
        def _():
            vec_back_in.wait_recv()
            vec_core.wait_send()
            vec_x.wait_send()
            vec_y.wait_send()
            vec_back.wait_send()

    def scatter_step(c, _):
        @pl.when(c < NC)
        def _():
            send_chunk(c)

        @pl.when(c == 0)
        def _():
            vraw_copy.start()

        @pl.when(c == 3)
        def _():
            for copy in state_copies:
                copy.start()

        vec_step(c)

        @pl.when((c >= 1) & (c < NC + 1))
        def _():
            relay_chunk(c - 1)

        @pl.when(c >= 2)
        def _():
            final_chunk(c - 2)
        return 0

    lax.fori_loop(0, NC + 2, scatter_step, 0)

    norms[me] = acc[...]
    vec_sq = jnp.sum(vfull[...] * vfull[...], keepdims=True)
    for copy in state_copies:
        copy.wait()

    def norm_copy(mask):
        return remote(norms.at[me], norms.at[me], ns_sem.at[mask - 1], nr_sem.at[mask - 1], mask)

    for mask in (6, 7, 2, 4, 3, 5, 1):
        norm_copy(mask).start()
    for c in (NC - 2, NC - 1):
        for b in send_slot:
            block_copy(b, c).wait_send()
        for h in (0, 1):
            rel_copy(h, c).wait_send()
    for mask in range(1, N_DEV):
        norm_copy(mask).wait_recv()
    total = norms[0]
    for k in range(1, N_DEV):
        total = total + norms[k]
    norm_sq = (jnp.sum(total, keepdims=True) + vec_sq) * (1.0 / (N_DEV * N_DEV))
    clip = jnp.minimum(1.0, MAX_NORM / (jnp.sqrt(norm_sq) + NORM_EPS)) * (1.0 / N_DEV)
    lr = lr_ref[0]

    upd_rows = 32
    clip_rows = jnp.broadcast_to(clip, (upd_rows, LANES))

    def update_chunk(h, c):
        def body(i, _):
            at = h * half + c * rc + i * upd_rows
            here = rows(at, upd_rows)
            new_p, new_m, new_v = adam_update(
                fin[here, :] * clip_rows, p_ref[here, :], m_ref[here, :], v_ref[here, :], lr, WEIGHT_DECAY)
            p_ref[here, :] = new_p
            m_ref[here, :] = new_m
            v_ref[here, :] = new_v
            big[rows(me * piece_rows + at, upd_rows), :] = new_p.astype(BF16)
            return 0
        lax.fori_loop(0, rc // upd_rows, body, 0)

    def gather_copy(mask, h, c, dest, ssem, slot):
        piece = flip(me, mask) if mask else me
        ref = big.at[rows(piece * piece_rows + h * half + c * rc, rc)]
        return remote(ref, ref, ag_sem.at[ssem], rs.at[slot, c], dest)

    def own_x(h, c):
        return gather_copy(0, h, c, 2, 0, h)

    def own_y(h, c):
        return gather_copy(0, h, c, 4, 1, 2 + h)

    def own_core(h, c):
        return gather_copy(0, h, c, 1, 2, 6 + h)

    def arrived(mask, h, c, slot):
        gather_copy(mask, h, c, 1, 0, slot).wait_recv()

    def to_core(mask, h, c):
        return gather_copy(mask, h, c, 1, {2: 5, 4: 6, 6: 7}[mask], {2: 8, 4: 10, 6: 12}[mask] + h)

    def first_half(i, _):
        @pl.when(i < NC)
        def _():
            update_chunk(0, i)
            update_chunk(1, i)
            own_x(0, i).start()
            own_y(1, i).start()
            own_core(0, i).start()
            own_core(1, i).start()

        @pl.when(i >= LAG)
        def _():
            j = i - LAG
            arrived(2, 0, j, 0)
            gather_copy(2, 0, j, 4, 3, 4).start()
            to_core(2, 0, j).start()
            arrived(4, 1, j, 3)
            gather_copy(4, 1, j, 2, 4, 5).start()
            to_core(4, 1, j).start()

        @pl.when(i >= NC)
        def _():
            own_x(1, i - NC).start()
            own_y(0, i - NC).start()
        return 0

    lax.fori_loop(0, NC + LAG, first_half, 0)

    vrows = n_vec // LANES
    new_p, new_m, new_v = adam_update(
        vfull[pl.ds(0, vrows), :] * clip, pv_ref[...], mv_ref[...], vv_ref[...], lr, 0.0)
    pv_out[...] = new_p
    mv_out[...] = new_m
    vv_out[...] = new_v

    def second_half(j, _):
        @pl.when(j + LAG < NC)
        def _():
            own_x(1, j + LAG).start()
            own_y(0, j + LAG).start()
        arrived(6, 0, j, 4)
        to_core(6, 0, j).start()
        arrived(6, 1, j, 5)
        to_core(6, 1, j).start()
        arrived(2, 1, j, 1)
        to_core(2, 1, j).start()
        arrived(4, 0, j, 2)
        to_core(4, 0, j).start()
        return 0

    lax.fori_loop(0, NC, second_half, 0)

    def last_arrivals(c, _):
        for k, mask in enumerate((1, 3, 5, 7)):
            for h in (0, 1):
                arrived(mask, h, c, 6 + 2 * k + h)
        return 0

    lax.fori_loop(0, NC, last_arrivals, 0)
    for ssem, count in ((0, 2), (1, 2), (2, 2), (3, 1), (4, 1), (5, 2), (6, 2), (7, 2)):
        ref = big.at[pl.ds(0, count * half)]
        remote(ref, ref, ag_sem.at[ssem], rs.at[0, 0], 1).wait_send()
    for mask in range(1, N_DEV):
        norm_copy(mask).wait_send()


def write_kernel(splits, *refs):
    n = len(splits)
    srcs, dsts, sem = refs[:n], refs[n:2 * n], refs[2 * n]
    copies = []
    for src, dst, count in zip(srcs, dsts, splits):
        part = src.shape[0] // count
        for k in range(count):
            at = pl.ds(k * part, part)
            copies.append(pltpu.make_async_copy(src.at[at], dst.at[at], sem.at[len(copies)]))
    for copy in copies:
        copy.start()
    for copy in copies:
        copy.wait()


def solution(mesh):
    axis_name = mesh.axis_names[0]

    def local_step(g_mat, g_vec, p_mat, m_mat, v_mat, p_vec, m_vec, v_vec, learn_rate):
        n_piece = p_mat.shape[0]
        n_vec = p_vec.shape[0]
        piece_rows = n_piece // LANES
        half = piece_rows // 2
        rc = half // NC
        state = (piece_rows, LANES)
        vec = (n_vec // LANES, LANES)
        full = (N_DEV * piece_rows, LANES)
        any_spec = pl.BlockSpec(memory_space=pl.ANY)
        vmem_spec = pl.BlockSpec(memory_space=pltpu.VMEM)
        outs = pl.pallas_call(
            functools.partial(step_kernel, half, rc, n_vec),
            out_shape=[pltpu.VMEM(full, BF16)] + [pltpu.VMEM(state, F32)] * 3 + [pltpu.VMEM(vec, F32)] * 3,
            in_specs=[any_spec] * 5 + [vmem_spec] * 3 + [pl.BlockSpec(memory_space=pltpu.SMEM)],
            out_specs=[vmem_spec] * 7,
            scratch_shapes=[
                pltpu.VMEM(state, F32),
                pltpu.VMEM((NRAW, 1, rc * LANES), BF16),
                pltpu.VMEM((2, 12, rc, LANES), BF16),
                pltpu.VMEM((2, 2, rc, LANES), F32),
                pltpu.VMEM((8, LANES), F32),
                pltpu.VMEM((N_DEV, 8, LANES), F32),
                pltpu.VMEM((1, 2 * VROWS * LANES), BF16),
                pltpu.VMEM((2 * VROWS, LANES), BF16),
                pltpu.VMEM((VROWS, LANES), BF16),
                pltpu.VMEM((VROWS, LANES), F32),
                pltpu.VMEM((VROWS, LANES), F32),
                pltpu.VMEM((VROWS, LANES), F32),
                pltpu.VMEM((VROWS, LANES), F32),
                pltpu.VMEM((2 * VROWS, LANES), F32),
                pltpu.SemaphoreType.DMA((NRAW,)),
                pltpu.SemaphoreType.DMA((2, 12)),
                pltpu.SemaphoreType.DMA((2, 2)),
                pltpu.SemaphoreType.DMA((14, NC)),
                pltpu.SemaphoreType.DMA((4,)),
                pltpu.SemaphoreType.DMA((7,)),
                pltpu.SemaphoreType.DMA((7,)),
                pltpu.SemaphoreType.DMA((4,)),
                pltpu.SemaphoreType.DMA((4,)),
                pltpu.SemaphoreType.DMA((8,)),
            ],
            compiler_params=pltpu.CompilerParams(
                collective_id=0, has_side_effects=True, vmem_limit_bytes=15 * 2 ** 20),
            name="step",
        )(
            g_mat, g_vec, p_mat.reshape(state), m_mat.reshape(state), v_mat.reshape(state),
            p_vec.reshape(vec), m_vec.reshape(vec), v_vec.reshape(vec), learn_rate.reshape(1),
        )
        splits = (16, 4, 4, 4, 1, 1, 1)
        pb, p_new, m_new, v_new, pv_new, mv_new, vv_new = pl.pallas_call(
            functools.partial(write_kernel, splits),
            out_shape=[jax.ShapeDtypeStruct(o.shape, o.dtype) for o in outs],
            in_specs=[vmem_spec] * 7,
            out_specs=[any_spec] * 7,
            scratch_shapes=[pltpu.SemaphoreType.DMA((sum(splits),))],
            compiler_params=pltpu.CompilerParams(vmem_limit_bytes=2 ** 20),
            name="write",
        )(*outs)
        return (
            p_new.reshape(-1), m_new.reshape(-1), v_new.reshape(-1),
            pv_new.reshape(-1), mv_new.reshape(-1), vv_new.reshape(-1), pb.reshape(-1),
        )

    return jax.shard_map(
        local_step,
        mesh=mesh,
        in_specs=(P(axis_name, None), P(axis_name, None), P(axis_name), P(axis_name), P(axis_name), P(), P(), P(), P()),
        out_specs=(P(axis_name), P(axis_name), P(axis_name), P(), P(), P(), P()),
        check_vma=False,
    )
```

```python
import functools

import jax
import jax.numpy as jnp
from jax import lax
from jax.experimental import pallas as pl
from jax.experimental.pallas import tpu as pltpu
from jax.sharding import PartitionSpec as P

STEP = 10
ADAM_BETA1 = 0.9
ADAM_BETA2 = 0.98
ADAM_EPS = 1e-8
WEIGHT_DECAY = 0.01
MAX_NORM = 1.0
NORM_EPS = 1e-6
BIAS_ONE = 1.0 - ADAM_BETA1 ** STEP
BIAS_TWO = 1.0 - ADAM_BETA2 ** STEP

LANES = 128
N_DEV = 8
NC = 18
NRAW = 8
LAG = 2
VROWS = 80
MESH = pl.DeviceIdType.MESH
F32 = jnp.float32
BF16 = jnp.bfloat16


def adam_update(grad_vals, param_vals, moment_one, moment_two, learn_rate, decay_rate):
    new_one = ADAM_BETA1 * moment_one + (1.0 - ADAM_BETA1) * grad_vals
    new_two = ADAM_BETA2 * moment_two + (1.0 - ADAM_BETA2) * grad_vals * grad_vals
    direction = (new_one / BIAS_ONE) / (jnp.sqrt(new_two / BIAS_TWO) + ADAM_EPS)
    return param_vals - learn_rate * (direction + decay_rate * param_vals), new_one, new_two


def flip(device, mask):
    for bit in (1, 2, 4):
        if mask & bit:
            device = device + bit - 2 * bit * lax.rem(lax.div(device, bit), 2)
    return device


def step_kernel(
    half, rc, n_vec,
    g_hbm, gv_hbm, p_hbm, m_hbm, v_hbm, pv_ref, mv_ref, vv_ref, lr_ref,
    state, big,
    fin, raw, pk, rel, acc, norms, vraw, vpk, vland, vs1, vlx, vs2, vly, vfull,
    raw_sem, send_sem, rel_sem, rs, st_sem, ns_sem, nr_sem, vs_sem, vr_sem, ag_sem,
):
    piece_rows = 2 * half
    p_ref, m_ref, v_ref = (state.at[pl.ds(k * piece_rows, piece_rows)] for k in range(3))
    pv_out, mv_out, vv_out = (
        state.at[pl.ds(3 * piece_rows + k * 2 * VROWS, n_vec // LANES)] for k in range(3))
    me = lax.axis_index("dp")
    core = lax.rem(me, 2)
    peer = {mask: flip(me, mask) for mask in range(1, N_DEV)}

    def remote(src, dst, ssem, rsem, mask):
        return pltpu.make_async_remote_copy(
            src_ref=src, dst_ref=dst, send_sem=ssem, recv_sem=rsem,
            device_id=(peer[mask],), device_id_type=MESH,
        )

    def rows(first, count, align=16):
        return pl.ds(pl.multiple_of(first, align), count)

    blocks = []
    for j in (0, 1):
        for h in (0, 1):
            via = (4, 2)[h]
            blocks.append(("send", h, 6 ^ j, via ^ j, h * 3 + j))
    for h in (0, 1):
        blocks.append(("send", h, (2, 4)[h] ^ 1, 1, h * 3 + 2))
        blocks.append(("own", h, (2, 4)[h], None, 14 + h))
    for j in (0, 1):
        for h in (0, 1):
            via = (4, 2)[h]
            blocks.append(("send", h, via ^ j, via ^ j, 6 + h * 3 + j))
    for h in (0, 1):
        blocks.append(("send", h, 1, 1, 6 + h * 3 + 2))
        blocks.append(("own", h, 0, None, 12 + h))
    n_blocks = len(blocks)
    send_slot = {}
    for b, block in enumerate(blocks):
        if block[0] == "send":
            send_slot[b] = len(send_slot)

    def raw_copy(b, c):
        _, h, mask, _, _ = blocks[b]
        piece = flip(me, mask) if mask else me
        start = (piece * piece_rows + h * half + c * rc) * LANES
        return pltpu.make_async_copy(
            g_hbm.at[:, pl.ds(pl.multiple_of(start, 2048), rc * LANES)],
            raw.at[b % NRAW], raw_sem.at[b % NRAW],
        )

    def block_copy(b, c):
        _, h, _, dest, slot = blocks[b]
        s = send_slot[b]
        par = lax.rem(c, 2)
        return remote(
            pk.at[par, s], big.at[rows(slot * half + c * rc, rc)],
            send_sem.at[par, s], rs.at[slot, c], dest,
        )

    def landed(slot, c):
        ref = big.at[rows(slot * half + c * rc, rc)]
        return remote(ref, ref, send_sem.at[0, 0], rs.at[slot, c], 1)

    def rel_copy(h, c):
        par = lax.rem(c, 2)
        return remote(
            rel.at[par, h], fin.at[rows(h * half + c * rc, rc)],
            rel_sem.at[par, h], rs.at[12 + h, c], (2, 4)[h],
        )

    state_copies = [
        pltpu.make_async_copy(src, dst, st_sem.at[i])
        for i, (src, dst) in enumerate(((p_hbm, p_ref), (m_hbm, m_ref), (v_hbm, v_ref)))
    ]
    vraw_copy = pltpu.make_async_copy(gv_hbm, vraw.at[:, pl.ds(0, n_vec)], st_sem.at[3])

    barrier = pltpu.get_barrier_semaphore()
    for mask in range(1, N_DEV):
        pl.semaphore_signal(barrier, inc=1, device_id=(peer[mask],), device_id_type=MESH)
    for b in range(NRAW):
        raw_copy(b, 0).start()
    vraw[:, pl.ds(n_vec // 1024 * 1024, 2 * VROWS * LANES - n_vec // 1024 * 1024)] = jnp.zeros(
        (1, 2 * VROWS * LANES - n_vec // 1024 * 1024), BF16)
    acc[...] = jnp.zeros_like(acc)
    pl.semaphore_wait(barrier, N_DEV - 1)

    step_rows = 64

    def pack_rows(src, dst, first):
        def body(i, _):
            vals = src[:, pl.ds(pl.multiple_of(i * step_rows * LANES, 2048), step_rows * LANES)]
            dst[rows(first + i * step_rows, step_rows), :] = (
                vals.astype(F32).reshape(step_rows, LANES).astype(BF16))
            return 0
        lax.fori_loop(0, rc // step_rows, body, 0)

    def send_chunk(c):
        par = lax.rem(c, 2)
        waiting = None
        for b, (kind, h, mask, dest, slot) in enumerate(blocks):
            raw_copy(b, c).wait()
            if kind == "send":
                @pl.when(c >= 2)
                def _():
                    block_copy(b, c - 2).wait_send()
                pack_rows(raw.at[b % NRAW], pk.at[par, send_slot[b]], 0)
            else:
                pack_rows(raw.at[b % NRAW], big, slot * half + c * rc)
            if b + NRAW < n_blocks:
                raw_copy(b + NRAW, c).start()
            else:
                @pl.when(c + 1 < NC)
                def _():
                    raw_copy(b + NRAW - n_blocks, c + 1).start()
            if waiting is not None:
                block_copy(waiting, c).start()
            waiting = b if kind == "send" else None
        if waiting is not None:
            block_copy(waiting, c).start()

    sum_rows = 32

    def relay_chunk(c):
        par = lax.rem(c, 2)
        for h in (0, 1):
            for j in range(3):
                landed(h * 3 + j, c).wait_recv()

            @pl.when(c >= 2)
            def _():
                rel_copy(h, c - 2).wait_send()

            def body(i, _):
                at = c * rc + i * sum_rows
                total = big[rows((14 + h) * half + at, sum_rows), :].astype(F32)
                for j in (2, 0, 1):
                    total = total + big[rows((h * 3 + j) * half + at, sum_rows), :].astype(F32)
                rel[par, h, rows(i * sum_rows, sum_rows), :] = total
                return 0
            lax.fori_loop(0, rc // sum_rows, body, 0)
        for h in (0, 1):
            rel_copy(h, c).start()

    def final_chunk(c):
        for h in (0, 1):
            for j in range(3):
                landed(6 + h * 3 + j, c).wait_recv()
            rel_copy(h, c).wait_recv()

            def body(i, sq):
                at = c * rc + i * sum_rows
                total = big[rows((12 + h) * half + at, sum_rows), :].astype(F32)
                for j in (2, 0, 1):
                    total = total + big[rows((6 + h * 3 + j) * half + at, sum_rows), :].astype(F32)
                total = total + fin[rows(h * half + at, sum_rows), :]
                fin[rows(h * half + at, sum_rows), :] = total
                total = total * total
                for k in range(sum_rows // 8):
                    sq = sq + total[8 * k:8 * k + 8]
                return sq
            acc[...] = lax.fori_loop(0, rc // sum_rows, body, acc[...])

    mine = rows(core * VROWS, VROWS)
    other = rows((1 - core) * VROWS, VROWS)
    vec_core = remote(vpk.at[other], vland, vs_sem.at[0], vr_sem.at[0], 1)
    vec_x = remote(vs1, vlx, vs_sem.at[1], vr_sem.at[1], 2)
    vec_y = remote(vs2, vly, vs_sem.at[2], vr_sem.at[2], 4)
    vec_back = remote(vfull.at[mine], vfull.at[mine], vs_sem.at[3], vr_sem.at[3], 1)
    vec_back_in = remote(vfull.at[other], vfull.at[other], vs_sem.at[3], vr_sem.at[3], 1)

    def vec_step(c):
        @pl.when(c == 1)
        def _():
            vraw_copy.wait()
            vpk[...] = vraw[...].astype(F32).reshape(2 * VROWS, LANES).astype(BF16)

        @pl.when(c == 2)
        def _():
            vec_core.start()

        @pl.when(c == 3)
        def _():
            vec_core.wait_recv()
            vs1[...] = vpk[mine, :].astype(F32) + vland[...].astype(F32)

        @pl.when(c == 4)
        def _():
            vec_x.start()

        @pl.when(c == 6)
        def _():
            vec_x.wait_recv()
            vs2[...] = vs1[...] + vlx[...]

        @pl.when(c == 7)
        def _():
            vec_y.start()

        @pl.when(c == 9)
        def _():
            vec_y.wait_recv()
            vfull[mine, :] = vs2[...] + vly[...]

        @pl.when(c == 10)
        def _():
            vec_back.start()

        @pl.when(c == 12)
        def _():
            vec_back_in.wait_recv()
            vec_core.wait_send()
            vec_x.wait_send()
            vec_y.wait_send()
            vec_back.wait_send()

    def scatter_step(c, _):
        @pl.when(c < NC)
        def _():
            send_chunk(c)

        @pl.when(c == 0)
        def _():
            vraw_copy.start()

        @pl.when(c == 3)
        def _():
            for copy in state_copies:
                copy.start()

        vec_step(c)

        @pl.when((c >= 1) & (c < NC + 1))
        def _():
            relay_chunk(c - 1)

        @pl.when(c >= 2)
        def _():
            final_chunk(c - 2)
        return 0

    lax.fori_loop(0, NC + 2, scatter_step, 0)

    norms[me] = acc[...]
    vec_sq = jnp.sum(vfull[...] * vfull[...], keepdims=True)
    for copy in state_copies:
        copy.wait()

    def norm_copy(mask):
        return remote(norms.at[me], norms.at[me], ns_sem.at[mask - 1], nr_sem.at[mask - 1], mask)

    for mask in (6, 7, 2, 4, 3, 5, 1):
        norm_copy(mask).start()
    for c in (NC - 2, NC - 1):
        for b in send_slot:
            block_copy(b, c).wait_send()
        for h in (0, 1):
            rel_copy(h, c).wait_send()
    for mask in range(1, N_DEV):
        norm_copy(mask).wait_recv()
    total = norms[0]
    for k in range(1, N_DEV):
        total = total + norms[k]
    norm_sq = (jnp.sum(total, keepdims=True) + vec_sq) * (1.0 / (N_DEV * N_DEV))
    clip = jnp.minimum(1.0, MAX_NORM / (jnp.sqrt(norm_sq) + NORM_EPS)) * (1.0 / N_DEV)
    lr = lr_ref[0]

    upd_rows = 32
    clip_rows = jnp.broadcast_to(clip, (upd_rows, LANES))

    def update_chunk(h, c):
        def body(i, _):
            at = h * half + c * rc + i * upd_rows
            here = rows(at, upd_rows)
            new_p, new_m, new_v = adam_update(
                fin[here, :] * clip_rows, p_ref[here, :], m_ref[here, :], v_ref[here, :], lr, WEIGHT_DECAY)
            p_ref[here, :] = new_p
            m_ref[here, :] = new_m
            v_ref[here, :] = new_v
            big[rows(me * piece_rows + at, upd_rows), :] = new_p.astype(BF16)
            return 0
        lax.fori_loop(0, rc // upd_rows, body, 0)

    def gather_copy(mask, h, c, dest, ssem, slot):
        piece = flip(me, mask) if mask else me
        ref = big.at[rows(piece * piece_rows + h * half + c * rc, rc)]
        return remote(ref, ref, ag_sem.at[ssem], rs.at[slot, c], dest)

    def own_x(h, c):
        return gather_copy(0, h, c, 2, 0, h)

    def own_y(h, c):
        return gather_copy(0, h, c, 4, 1, 2 + h)

    def own_core(h, c):
        return gather_copy(0, h, c, 1, 2, 6 + h)

    def arrived(mask, h, c, slot):
        gather_copy(mask, h, c, 1, 0, slot).wait_recv()

    def to_core(mask, h, c):
        return gather_copy(mask, h, c, 1, {2: 5, 4: 6, 6: 7}[mask], {2: 8, 4: 10, 6: 12}[mask] + h)

    def first_half(i, _):
        @pl.when(i < NC)
        def _():
            update_chunk(0, i)
            update_chunk(1, i)
            own_x(0, i).start()
            own_y(1, i).start()
            own_core(0, i).start()
            own_core(1, i).start()

        @pl.when(i >= LAG)
        def _():
            j = i - LAG
            arrived(2, 0, j, 0)
            gather_copy(2, 0, j, 4, 3, 4).start()
            to_core(2, 0, j).start()
            arrived(4, 1, j, 3)
            gather_copy(4, 1, j, 2, 4, 5).start()
            to_core(4, 1, j).start()

        @pl.when(i >= NC)
        def _():
            own_x(1, i - NC).start()
            own_y(0, i - NC).start()
        return 0

    lax.fori_loop(0, NC + LAG, first_half, 0)

    vrows = n_vec // LANES
    new_p, new_m, new_v = adam_update(
        vfull[pl.ds(0, vrows), :] * clip, pv_ref[...], mv_ref[...], vv_ref[...], lr, 0.0)
    pv_out[...] = new_p
    mv_out[...] = new_m
    vv_out[...] = new_v

    def second_half(j, _):
        @pl.when(j + LAG < NC)
        def _():
            own_x(1, j + LAG).start()
            own_y(0, j + LAG).start()
        arrived(6, 0, j, 4)
        to_core(6, 0, j).start()
        arrived(6, 1, j, 5)
        to_core(6, 1, j).start()
        arrived(2, 1, j, 1)
        to_core(2, 1, j).start()
        arrived(4, 0, j, 2)
        to_core(4, 0, j).start()
        return 0

    lax.fori_loop(0, NC, second_half, 0)

    def last_arrivals(c, _):
        for k, mask in enumerate((1, 3, 5, 7)):
            for h in (0, 1):
                arrived(mask, h, c, 6 + 2 * k + h)
        return 0

    lax.fori_loop(0, NC, last_arrivals, 0)
    for ssem, count in ((0, 2), (1, 2), (2, 2), (3, 1), (4, 1), (5, 2), (6, 2), (7, 2)):
        ref = big.at[pl.ds(0, count * half)]
        remote(ref, ref, ag_sem.at[ssem], rs.at[0, 0], 1).wait_send()
    for mask in range(1, N_DEV):
        norm_copy(mask).wait_send()


def write_kernel(state, big, *refs):
    dsts, sem = refs[:-1], refs[-1]
    copies = []

    def add(src, dst, count):
        part = dst.shape[0] // count
        for k in range(count):
            copies.append(pltpu.make_async_copy(
                src.at[pl.ds(k * part, part)], dst.at[pl.ds(k * part, part)], sem.at[len(copies)]))

    at = 0
    for dst in dsts[:6]:
        add(state.at[pl.ds(at, dst.shape[0])], dst, 4 if dst.shape[0] > 2 * VROWS else 1)
        at += max(dst.shape[0], 2 * VROWS)
    add(big, dsts[6], 16)
    for copy in copies:
        copy.start()
    for copy in copies:
        copy.wait()


def solution(mesh):
    axis_name = mesh.axis_names[0]

    def local_step(g_mat, g_vec, p_mat, m_mat, v_mat, p_vec, m_vec, v_vec, learn_rate):
        n_piece = p_mat.shape[0]
        n_vec = p_vec.shape[0]
        piece_rows = n_piece // LANES
        half = piece_rows // 2
        rc = half // NC
        state = (piece_rows, LANES)
        vec = (n_vec // LANES, LANES)
        full = (N_DEV * piece_rows, LANES)
        any_spec = pl.BlockSpec(memory_space=pl.ANY)
        vmem_spec = pl.BlockSpec(memory_space=pltpu.VMEM)
        outs = pl.pallas_call(
            functools.partial(step_kernel, half, rc, n_vec),
            out_shape=[pltpu.VMEM((3 * piece_rows + 6 * VROWS, LANES), F32), pltpu.VMEM(full, BF16)],
            in_specs=[any_spec] * 5 + [vmem_spec] * 3 + [pl.BlockSpec(memory_space=pltpu.SMEM)],
            out_specs=[vmem_spec] * 2,
            scratch_shapes=[
                pltpu.VMEM(state, F32),
                pltpu.VMEM((NRAW, 1, rc * LANES), BF16),
                pltpu.VMEM((2, 12, rc, LANES), BF16),
                pltpu.VMEM((2, 2, rc, LANES), F32),
                pltpu.VMEM((8, LANES), F32),
                pltpu.VMEM((N_DEV, 8, LANES), F32),
                pltpu.VMEM((1, 2 * VROWS * LANES), BF16),
                pltpu.VMEM((2 * VROWS, LANES), BF16),
                pltpu.VMEM((VROWS, LANES), BF16),
                pltpu.VMEM((VROWS, LANES), F32),
                pltpu.VMEM((VROWS, LANES), F32),
                pltpu.VMEM((VROWS, LANES), F32),
                pltpu.VMEM((VROWS, LANES), F32),
                pltpu.VMEM((2 * VROWS, LANES), F32),
                pltpu.SemaphoreType.DMA((NRAW,)),
                pltpu.SemaphoreType.DMA((2, 12)),
                pltpu.SemaphoreType.DMA((2, 2)),
                pltpu.SemaphoreType.DMA((14, NC)),
                pltpu.SemaphoreType.DMA((4,)),
                pltpu.SemaphoreType.DMA((7,)),
                pltpu.SemaphoreType.DMA((7,)),
                pltpu.SemaphoreType.DMA((4,)),
                pltpu.SemaphoreType.DMA((4,)),
                pltpu.SemaphoreType.DMA((8,)),
            ],
            compiler_params=pltpu.CompilerParams(
                collective_id=0, has_side_effects=True, vmem_limit_bytes=15 * 2 ** 20),
            name="step",
        )(
            g_mat, g_vec, p_mat.reshape(state), m_mat.reshape(state), v_mat.reshape(state),
            p_vec.reshape(vec), m_vec.reshape(vec), v_vec.reshape(vec), learn_rate.reshape(1),
        )
        p_new, m_new, v_new, pv_new, mv_new, vv_new, pb = pl.pallas_call(
            write_kernel,
            out_shape=[jax.ShapeDtypeStruct(state, F32)] * 3 + [jax.ShapeDtypeStruct(vec, F32)] * 3
            + [jax.ShapeDtypeStruct(full, BF16)],
            in_specs=[vmem_spec] * 2,
            out_specs=[any_spec] * 7,
            scratch_shapes=[pltpu.SemaphoreType.DMA((31,))],
            compiler_params=pltpu.CompilerParams(vmem_limit_bytes=2 ** 20),
            name="write",
        )(*outs)
        return (
            p_new.reshape(-1), m_new.reshape(-1), v_new.reshape(-1),
            pv_new.reshape(-1), mv_new.reshape(-1), vv_new.reshape(-1), pb.reshape(-1),
        )

    return jax.shard_map(
        local_step,
        mesh=mesh,
        in_specs=(P(axis_name, None), P(axis_name, None), P(axis_name), P(axis_name), P(axis_name), P(), P(), P(), P()),
        out_specs=(P(axis_name), P(axis_name), P(axis_name), P(), P(), P(), P()),
        check_vma=False,
    )
```

```python
import functools

import jax
import jax.numpy as jnp
from jax import lax
from jax.experimental import pallas as pl
from jax.experimental.pallas import tpu as pltpu
from jax.sharding import PartitionSpec as P

STEP = 10
ADAM_BETA1 = 0.9
ADAM_BETA2 = 0.98
ADAM_EPS = 1e-8
WEIGHT_DECAY = 0.01
MAX_NORM = 1.0
NORM_EPS = 1e-6
BIAS_ONE = 1.0 - ADAM_BETA1 ** STEP
BIAS_TWO = 1.0 - ADAM_BETA2 ** STEP

LANES = 128
N_DEV = 8
NC = 18
NRAW = 8
EARLY = 4
LAG = 2
VROWS = 80
MESH = pl.DeviceIdType.MESH
F32 = jnp.float32
BF16 = jnp.bfloat16


def adam_update(grad_vals, param_vals, moment_one, moment_two, learn_rate, decay_rate):
    new_one = ADAM_BETA1 * moment_one + (1.0 - ADAM_BETA1) * grad_vals
    new_two = ADAM_BETA2 * moment_two + (1.0 - ADAM_BETA2) * grad_vals * grad_vals
    direction = (new_one / BIAS_ONE) / (jnp.sqrt(new_two / BIAS_TWO) + ADAM_EPS)
    return param_vals - learn_rate * (direction + decay_rate * param_vals), new_one, new_two


def flip(device, mask):
    for bit in (1, 2, 4):
        if mask & bit:
            device = device + bit - 2 * bit * lax.rem(lax.div(device, bit), 2)
    return device


def step_kernel(
    half, rc, n_vec,
    g_hbm, gv_hbm, p_hbm, m_hbm, v_hbm, pv_hbm, mv_hbm, vv_hbm, lr_hbm,
    state, big,
    fin, raw, pk, rel, acc, norms, vraw, vpk, vland, vs1, vlx, vs2, vly, vfull, lr_ref,
    raw_sem, send_sem, rel_sem, rs, st_sem, ns_sem, nr_sem, vs_sem, vr_sem, ag_sem,
):
    piece_rows = 2 * half
    p_ref, m_ref, v_ref = (state.at[pl.ds(k * piece_rows, piece_rows)] for k in range(3))
    pv_out, mv_out, vv_out = (
        state.at[pl.ds(3 * piece_rows + k * 2 * VROWS, n_vec // LANES)] for k in range(3))
    me = lax.axis_index("dp")
    core = lax.rem(me, 2)
    peer = {mask: flip(me, mask) for mask in range(1, N_DEV)}

    def remote(src, dst, ssem, rsem, mask):
        return pltpu.make_async_remote_copy(
            src_ref=src, dst_ref=dst, send_sem=ssem, recv_sem=rsem,
            device_id=(peer[mask],), device_id_type=MESH,
        )

    def rows(first, count, align=16):
        return pl.ds(pl.multiple_of(first, align), count)

    blocks = []
    for j in (0, 1):
        for h in (0, 1):
            via = (4, 2)[h]
            blocks.append(("send", h, 6 ^ j, via ^ j, h * 3 + j))
    for h in (0, 1):
        blocks.append(("send", h, (2, 4)[h] ^ 1, 1, h * 3 + 2))
        blocks.append(("own", h, (2, 4)[h], None, 14 + h))
    for j in (0, 1):
        for h in (0, 1):
            via = (4, 2)[h]
            blocks.append(("send", h, via ^ j, via ^ j, 6 + h * 3 + j))
    for h in (0, 1):
        blocks.append(("send", h, 1, 1, 6 + h * 3 + 2))
        blocks.append(("own", h, 0, None, 12 + h))
    n_blocks = len(blocks)
    send_slot = {}
    for b, block in enumerate(blocks):
        if block[0] == "send":
            send_slot[b] = len(send_slot)

    def raw_copy(b, c):
        _, h, mask, _, _ = blocks[b]
        piece = flip(me, mask) if mask else me
        start = (piece * piece_rows + h * half + c * rc) * LANES
        return pltpu.make_async_copy(
            g_hbm.at[:, pl.ds(pl.multiple_of(start, 2048), rc * LANES)],
            raw.at[b % NRAW], raw_sem.at[b % NRAW],
        )

    def block_copy(b, c):
        _, h, _, dest, slot = blocks[b]
        s = send_slot[b]
        par = lax.rem(c, 2)
        return remote(
            pk.at[par, s], big.at[rows(slot * half + c * rc, rc)],
            send_sem.at[par, s], rs.at[slot, c], dest,
        )

    def landed(slot, c):
        ref = big.at[rows(slot * half + c * rc, rc)]
        return remote(ref, ref, send_sem.at[0, 0], rs.at[slot, c], 1)

    def rel_copy(h, c):
        par = lax.rem(c, 2)
        return remote(
            rel.at[par, h], fin.at[rows(h * half + c * rc, rc)],
            rel_sem.at[par, h], rs.at[12 + h, c], (2, 4)[h],
        )

    state_copies = [
        pltpu.make_async_copy(src, dst, st_sem.at[i])
        for i, (src, dst) in enumerate((
            (p_hbm, p_ref), (m_hbm, m_ref), (v_hbm, v_ref),
            (pv_hbm, pv_out), (mv_hbm, mv_out), (vv_hbm, vv_out), (lr_hbm, lr_ref)))
    ]
    vraw_copy = pltpu.make_async_copy(gv_hbm, vraw.at[:, pl.ds(0, n_vec)], st_sem.at[7])

    barrier = pltpu.get_barrier_semaphore()
    for mask in range(1, N_DEV):
        pl.semaphore_signal(barrier, inc=1, device_id=(peer[mask],), device_id_type=MESH)
    for b in range(NRAW):
        raw_copy(b, 0).start()
    vraw[:, pl.ds(n_vec // 1024 * 1024, 2 * VROWS * LANES - n_vec // 1024 * 1024)] = jnp.zeros(
        (1, 2 * VROWS * LANES - n_vec // 1024 * 1024), BF16)
    acc[...] = jnp.zeros_like(acc)
    step_rows = 64

    def pack_rows(src, dst, first):
        def body(i, _):
            vals = src[:, pl.ds(pl.multiple_of(i * step_rows * LANES, 2048), step_rows * LANES)]
            dst[rows(first + i * step_rows, step_rows), :] = (
                vals.astype(F32).reshape(step_rows, LANES).astype(BF16))
            return 0
        lax.fori_loop(0, rc // step_rows, body, 0, unroll=2)

    def load_block(b, c):
        kind, _, _, _, slot = blocks[b]
        raw_copy(b, c).wait()
        if kind == "send":
            @pl.when(c >= 2)
            def _():
                block_copy(b, c - 2).wait_send()
            pack_rows(raw.at[b % NRAW], pk.at[lax.rem(c, 2), send_slot[b]], 0)
        else:
            pack_rows(raw.at[b % NRAW], big, slot * half + c * rc)
        if b + NRAW < n_blocks:
            raw_copy(b + NRAW, c).start()
        else:
            @pl.when(c + 1 < NC)
            def _():
                raw_copy(b + NRAW - n_blocks, c + 1).start()

    for b in range(EARLY):
        load_block(b, 0)
    pl.semaphore_wait(barrier, N_DEV - 1)

    def send_chunk(c):
        waiting = None
        for b, (kind, h, mask, dest, slot) in enumerate(blocks):
            if b < EARLY:
                @pl.when(c >= 1)
                def _():
                    load_block(b, c)
            else:
                load_block(b, c)
            if waiting is not None:
                block_copy(waiting, c).start()
            waiting = b if kind == "send" else None
        if waiting is not None:
            block_copy(waiting, c).start()

    sum_rows = 32

    def relay_chunk(c):
        par = lax.rem(c, 2)
        for h in (0, 1):
            for j in range(3):
                landed(h * 3 + j, c).wait_recv()

            @pl.when(c >= 2)
            def _():
                rel_copy(h, c - 2).wait_send()

            def body(i, _):
                at = c * rc + i * sum_rows
                total = big[rows((14 + h) * half + at, sum_rows), :].astype(F32)
                for j in (2, 0, 1):
                    total = total + big[rows((h * 3 + j) * half + at, sum_rows), :].astype(F32)
                rel[par, h, rows(i * sum_rows, sum_rows), :] = total
                return 0
            lax.fori_loop(0, rc // sum_rows, body, 0)
        for h in (0, 1):
            rel_copy(h, c).start()

    def final_chunk(c):
        for h in (0, 1):
            for j in range(3):
                landed(6 + h * 3 + j, c).wait_recv()
            rel_copy(h, c).wait_recv()

            def body(i, sq):
                at = c * rc + i * sum_rows
                total = big[rows((12 + h) * half + at, sum_rows), :].astype(F32)
                for j in (2, 0, 1):
                    total = total + big[rows((6 + h * 3 + j) * half + at, sum_rows), :].astype(F32)
                total = total + fin[rows(h * half + at, sum_rows), :]
                fin[rows(h * half + at, sum_rows), :] = total
                total = total * total
                for k in range(sum_rows // 8):
                    sq = sq + total[8 * k:8 * k + 8]
                return sq
            acc[...] = lax.fori_loop(0, rc // sum_rows, body, acc[...], unroll=4)

    mine = rows(core * VROWS, VROWS)
    other = rows((1 - core) * VROWS, VROWS)
    vec_core = remote(vpk.at[other], vland, vs_sem.at[0], vr_sem.at[0], 1)
    vec_x = remote(vs1, vlx, vs_sem.at[1], vr_sem.at[1], 2)
    vec_y = remote(vs2, vly, vs_sem.at[2], vr_sem.at[2], 4)
    vec_back = remote(vfull.at[mine], vfull.at[mine], vs_sem.at[3], vr_sem.at[3], 1)
    vec_back_in = remote(vfull.at[other], vfull.at[other], vs_sem.at[3], vr_sem.at[3], 1)

    def vec_step(c):
        @pl.when(c == 1)
        def _():
            vraw_copy.wait()
            vpk[...] = vraw[...].astype(F32).reshape(2 * VROWS, LANES).astype(BF16)

        @pl.when(c == 2)
        def _():
            vec_core.start()

        @pl.when(c == 3)
        def _():
            vec_core.wait_recv()
            vs1[...] = vpk[mine, :].astype(F32) + vland[...].astype(F32)

        @pl.when(c == 4)
        def _():
            vec_x.start()

        @pl.when(c == 6)
        def _():
            vec_x.wait_recv()
            vs2[...] = vs1[...] + vlx[...]

        @pl.when(c == 7)
        def _():
            vec_y.start()

        @pl.when(c == 9)
        def _():
            vec_y.wait_recv()
            vfull[mine, :] = vs2[...] + vly[...]

        @pl.when(c == 10)
        def _():
            vec_back.start()

        @pl.when(c == 12)
        def _():
            vec_back_in.wait_recv()
            vec_core.wait_send()
            vec_x.wait_send()
            vec_y.wait_send()
            vec_back.wait_send()

    def scatter_step(c, _):
        @pl.when(c < NC)
        def _():
            send_chunk(c)

        @pl.when(c == 0)
        def _():
            vraw_copy.start()

        @pl.when(c == 3)
        def _():
            for copy in state_copies:
                copy.start()

        vec_step(c)

        @pl.when((c >= 1) & (c < NC + 1))
        def _():
            relay_chunk(c - 1)

        @pl.when(c >= 2)
        def _():
            final_chunk(c - 2)
        return 0

    lax.fori_loop(0, NC + 2, scatter_step, 0)

    norms[me] = acc[...]
    vec_sq = jnp.sum(vfull[...] * vfull[...], keepdims=True)
    for copy in state_copies:
        copy.wait()

    def norm_copy(mask):
        return remote(norms.at[me], norms.at[me], ns_sem.at[mask - 1], nr_sem.at[mask - 1], mask)

    for mask in (6, 7, 2, 4, 3, 5, 1):
        norm_copy(mask).start()
    for c in (NC - 2, NC - 1):
        for b in send_slot:
            block_copy(b, c).wait_send()
        for h in (0, 1):
            rel_copy(h, c).wait_send()
    for mask in range(1, N_DEV):
        norm_copy(mask).wait_recv()
    total = norms[0]
    for k in range(1, N_DEV):
        total = total + norms[k]
    norm_sq = (jnp.sum(total, keepdims=True) + vec_sq) * (1.0 / (N_DEV * N_DEV))
    clip = jnp.minimum(1.0, MAX_NORM / (jnp.sqrt(norm_sq) + NORM_EPS)) * (1.0 / N_DEV)
    lr = lr_ref[...]

    upd_rows = 32
    clip_rows = jnp.broadcast_to(clip, (upd_rows, LANES))
    lr_rows = jnp.broadcast_to(lr, (upd_rows, LANES))

    def update_chunk(h, c):
        def body(i, _):
            at = h * half + c * rc + i * upd_rows
            here = rows(at, upd_rows)
            new_p, new_m, new_v = adam_update(
                fin[here, :] * clip_rows, p_ref[here, :], m_ref[here, :], v_ref[here, :], lr_rows, WEIGHT_DECAY)
            p_ref[here, :] = new_p
            m_ref[here, :] = new_m
            v_ref[here, :] = new_v
            big[rows(me * piece_rows + at, upd_rows), :] = new_p.astype(BF16)
            return 0
        lax.fori_loop(0, rc // upd_rows, body, 0, unroll=4)

    def gather_copy(mask, h, c, dest, ssem, slot):
        piece = flip(me, mask) if mask else me
        ref = big.at[rows(piece * piece_rows + h * half + c * rc, rc)]
        return remote(ref, ref, ag_sem.at[ssem], rs.at[slot, c], dest)

    def own_x(h, c):
        return gather_copy(0, h, c, 2, 0, h)

    def own_y(h, c):
        return gather_copy(0, h, c, 4, 1, 2 + h)

    def own_core(h, c):
        return gather_copy(0, h, c, 1, 2, 6 + h)

    def arrived(mask, h, c, slot):
        gather_copy(mask, h, c, 1, 0, slot).wait_recv()

    def to_core(mask, h, c):
        return gather_copy(mask, h, c, 1, {2: 5, 4: 6, 6: 7}[mask], {2: 8, 4: 10, 6: 12}[mask] + h)

    def first_half(i, _):
        @pl.when(i < NC)
        def _():
            update_chunk(0, i)
            own_x(0, i).start()
            update_chunk(1, i)
            own_y(1, i).start()
            own_core(0, i).start()
            own_core(1, i).start()

        @pl.when(i >= LAG)
        def _():
            j = i - LAG
            arrived(2, 0, j, 0)
            gather_copy(2, 0, j, 4, 3, 4).start()
            to_core(2, 0, j).start()
            arrived(4, 1, j, 3)
            gather_copy(4, 1, j, 2, 4, 5).start()
            to_core(4, 1, j).start()

        @pl.when(i >= NC)
        def _():
            own_x(1, i - NC).start()
            own_y(0, i - NC).start()
        return 0

    lax.fori_loop(0, NC + LAG, first_half, 0)

    vrows = n_vec // LANES
    new_p, new_m, new_v = adam_update(
        vfull[pl.ds(0, vrows), :] * clip, pv_out[...], mv_out[...], vv_out[...], lr, 0.0)
    pv_out[...] = new_p
    mv_out[...] = new_m
    vv_out[...] = new_v

    def second_half(j, _):
        @pl.when(j + LAG < NC)
        def _():
            own_x(1, j + LAG).start()
            own_y(0, j + LAG).start()
        arrived(6, 0, j, 4)
        to_core(6, 0, j).start()
        arrived(6, 1, j, 5)
        to_core(6, 1, j).start()
        arrived(2, 1, j, 1)
        to_core(2, 1, j).start()
        arrived(4, 0, j, 2)
        to_core(4, 0, j).start()
        return 0

    lax.fori_loop(0, NC, second_half, 0)

    def last_arrivals(c, _):
        for k, mask in enumerate((1, 3, 5, 7)):
            for h in (0, 1):
                arrived(mask, h, c, 6 + 2 * k + h)
        return 0

    lax.fori_loop(0, NC, last_arrivals, 0)
    for ssem, count in ((0, 2), (1, 2), (2, 2), (3, 1), (4, 1), (5, 2), (6, 2), (7, 2)):
        ref = big.at[pl.ds(0, count * half)]
        remote(ref, ref, ag_sem.at[ssem], rs.at[0, 0], 1).wait_send()
    for mask in range(1, N_DEV):
        norm_copy(mask).wait_send()


def write_kernel(state, big, *refs):
    dsts, sem = refs[:-1], refs[-1]
    copies = []

    def add(src, dst, count):
        part = dst.shape[0] // count
        for k in range(count):
            copies.append(pltpu.make_async_copy(
                src.at[pl.ds(k * part, part)], dst.at[pl.ds(k * part, part)], sem.at[len(copies)]))

    at = 0
    for dst in dsts[:6]:
        add(state.at[pl.ds(at, dst.shape[0])], dst, 4 if dst.shape[0] > 2 * VROWS else 1)
        at += max(dst.shape[0], 2 * VROWS)
    add(big, dsts[6], 16)
    for copy in copies:
        copy.start()
    for copy in copies:
        copy.wait()


def solution(mesh):
    axis_name = mesh.axis_names[0]

    def local_step(g_mat, g_vec, p_mat, m_mat, v_mat, p_vec, m_vec, v_vec, learn_rate):
        n_piece = p_mat.shape[0]
        n_vec = p_vec.shape[0]
        piece_rows = n_piece // LANES
        half = piece_rows // 2
        rc = half // NC
        state = (piece_rows, LANES)
        vec = (n_vec // LANES, LANES)
        full = (N_DEV * piece_rows, LANES)
        any_spec = pl.BlockSpec(memory_space=pl.ANY)
        vmem_spec = pl.BlockSpec(memory_space=pltpu.VMEM)
        outs = pl.pallas_call(
            functools.partial(step_kernel, half, rc, n_vec),
            out_shape=[pltpu.VMEM((3 * piece_rows + 6 * VROWS, LANES), F32), pltpu.VMEM(full, BF16)],
            in_specs=[any_spec] * 9,
            out_specs=[vmem_spec] * 2,
            scratch_shapes=[
                pltpu.VMEM(state, F32),
                pltpu.VMEM((NRAW, 1, rc * LANES), BF16),
                pltpu.VMEM((2, 12, rc, LANES), BF16),
                pltpu.VMEM((2, 2, rc, LANES), F32),
                pltpu.VMEM((8, LANES), F32),
                pltpu.VMEM((N_DEV, 8, LANES), F32),
                pltpu.VMEM((1, 2 * VROWS * LANES), BF16),
                pltpu.VMEM((2 * VROWS, LANES), BF16),
                pltpu.VMEM((VROWS, LANES), BF16),
                pltpu.VMEM((VROWS, LANES), F32),
                pltpu.VMEM((VROWS, LANES), F32),
                pltpu.VMEM((VROWS, LANES), F32),
                pltpu.VMEM((VROWS, LANES), F32),
                pltpu.VMEM((2 * VROWS, LANES), F32),
                pltpu.VMEM((1, 1), F32),
                pltpu.SemaphoreType.DMA((NRAW,)),
                pltpu.SemaphoreType.DMA((2, 12)),
                pltpu.SemaphoreType.DMA((2, 2)),
                pltpu.SemaphoreType.DMA((14, NC)),
                pltpu.SemaphoreType.DMA((8,)),
                pltpu.SemaphoreType.DMA((7,)),
                pltpu.SemaphoreType.DMA((7,)),
                pltpu.SemaphoreType.DMA((4,)),
                pltpu.SemaphoreType.DMA((4,)),
                pltpu.SemaphoreType.DMA((8,)),
            ],
            compiler_params=pltpu.CompilerParams(
                collective_id=0, has_side_effects=True, vmem_limit_bytes=15 * 2 ** 20),
            name="step",
        )(
            g_mat, g_vec, p_mat.reshape(state), m_mat.reshape(state), v_mat.reshape(state),
            p_vec.reshape(vec), m_vec.reshape(vec), v_vec.reshape(vec), learn_rate.reshape(1, 1),
        )
        p_new, m_new, v_new, pv_new, mv_new, vv_new, pb = pl.pallas_call(
            write_kernel,
            out_shape=[jax.ShapeDtypeStruct(state, F32)] * 3 + [jax.ShapeDtypeStruct(vec, F32)] * 3
            + [jax.ShapeDtypeStruct(full, BF16)],
            in_specs=[vmem_spec] * 2,
            out_specs=[any_spec] * 7,
            scratch_shapes=[pltpu.SemaphoreType.DMA((31,))],
            compiler_params=pltpu.CompilerParams(vmem_limit_bytes=2 ** 20),
            name="write",
        )(*outs)
        return (
            p_new.reshape(-1), m_new.reshape(-1), v_new.reshape(-1),
            pv_new.reshape(-1), mv_new.reshape(-1), vv_new.reshape(-1), pb.reshape(-1),
        )

    return jax.shard_map(
        local_step,
        mesh=mesh,
        in_specs=(P(axis_name, None), P(axis_name, None), P(axis_name), P(axis_name), P(axis_name), P(), P(), P(), P()),
        out_specs=(P(axis_name), P(axis_name), P(axis_name), P(), P(), P(), P()),
        check_vma=False,
    )
```

```python
import functools

import jax
import jax.numpy as jnp
from jax import lax
from jax.experimental import pallas as pl
from jax.experimental.pallas import tpu as pltpu
from jax.sharding import PartitionSpec as P

STEP = 10
ADAM_BETA1 = 0.9
ADAM_BETA2 = 0.98
ADAM_EPS = 1e-8
WEIGHT_DECAY = 0.01
MAX_NORM = 1.0
NORM_EPS = 1e-6
BIAS_ONE = 1.0 - ADAM_BETA1 ** STEP
BIAS_TWO = 1.0 - ADAM_BETA2 ** STEP

LANES = 128
N_DEV = 8
NC = 18
NRAW = 8
EARLY = 4
TAIL = 6
SPLIT = 14
LAG = 2
VROWS = 80
MESH = pl.DeviceIdType.MESH
F32 = jnp.float32
BF16 = jnp.bfloat16


def adam_update(grad_vals, param_vals, moment_one, moment_two, learn_rate, decay_rate):
    new_one = ADAM_BETA1 * moment_one + (1.0 - ADAM_BETA1) * grad_vals
    new_two = ADAM_BETA2 * moment_two + (1.0 - ADAM_BETA2) * grad_vals * grad_vals
    direction = (new_one / BIAS_ONE) / (jnp.sqrt(new_two / BIAS_TWO) + ADAM_EPS)
    return param_vals - learn_rate * (direction + decay_rate * param_vals), new_one, new_two


def flip(device, mask):
    for bit in (1, 2, 4):
        if mask & bit:
            device = device + bit - 2 * bit * lax.rem(lax.div(device, bit), 2)
    return device


def step_kernel(
    half, rc, n_vec,
    g_hbm, gv_hbm, p_hbm, m_hbm, v_hbm, pv_hbm, mv_hbm, vv_hbm, lr_hbm,
    state, big, px_hbm, py_hbm,
    fin, raw, pk, rel, acc, norms, vraw, vpk, vland, vs1, vlx, vs2, vly, vfull, lr_ref,
    raw_sem, send_sem, rel_sem, rs, st_sem, ns_sem, nr_sem, vs_sem, vr_sem, ag_sem, px_sem,
):
    piece_rows = 2 * half
    p_ref, m_ref, v_ref = (state.at[pl.ds(k * piece_rows, piece_rows)] for k in range(3))
    pv_out, mv_out, vv_out = (
        state.at[pl.ds(3 * piece_rows + k * 2 * VROWS, n_vec // LANES)] for k in range(3))
    me = lax.axis_index("dp")
    core = lax.rem(me, 2)
    peer = {mask: flip(me, mask) for mask in range(1, N_DEV)}

    def remote(src, dst, ssem, rsem, mask):
        return pltpu.make_async_remote_copy(
            src_ref=src, dst_ref=dst, send_sem=ssem, recv_sem=rsem,
            device_id=(peer[mask],), device_id_type=MESH,
        )

    def rows(first, count, align=16):
        return pl.ds(pl.multiple_of(first, align), count)

    blocks = []
    for j in (0, 1):
        for h in (0, 1):
            via = (4, 2)[h]
            blocks.append(("send", h, 6 ^ j, via ^ j, h * 3 + j))
    for h in (0, 1):
        blocks.append(("send", h, (2, 4)[h] ^ 1, 1, h * 3 + 2))
        blocks.append(("own", h, (2, 4)[h], None, 14 + h))
    for j in (0, 1):
        for h in (0, 1):
            via = (4, 2)[h]
            blocks.append(("send", h, via ^ j, via ^ j, 6 + h * 3 + j))
    for h in (0, 1):
        blocks.append(("send", h, 1, 1, 6 + h * 3 + 2))
        blocks.append(("own", h, 0, None, 12 + h))
    n_blocks = len(blocks)
    send_slot = {}
    for b, block in enumerate(blocks):
        if block[0] == "send":
            send_slot[b] = len(send_slot)

    def raw_copy(b, c):
        _, h, mask, _, _ = blocks[b]
        piece = flip(me, mask) if mask else me
        start = (piece * piece_rows + h * half + c * rc) * LANES
        return pltpu.make_async_copy(
            g_hbm.at[:, pl.ds(pl.multiple_of(start, 2048), rc * LANES)],
            raw.at[b % NRAW], raw_sem.at[b % NRAW],
        )

    def block_copy(b, c):
        _, h, _, dest, slot = blocks[b]
        s = send_slot[b]
        par = lax.rem(c, 2)
        return remote(
            pk.at[par, s], big.at[rows(slot * half + c * rc, rc)],
            send_sem.at[par, s], rs.at[slot, c], dest,
        )

    def landed(slot, c):
        ref = big.at[rows(slot * half + c * rc, rc)]
        return remote(ref, ref, send_sem.at[0, 0], rs.at[slot, c], 1)

    def rel_copy(h, c):
        par = lax.rem(c, 2)
        return remote(
            rel.at[par, h], fin.at[rows(h * half + c * rc, rc)],
            rel_sem.at[par, h], rs.at[12 + h, c], (2, 4)[h],
        )

    state_copies = [
        pltpu.make_async_copy(src, dst, st_sem.at[i])
        for i, (src, dst) in enumerate((
            (p_hbm, p_ref), (m_hbm, m_ref), (v_hbm, v_ref),
            (pv_hbm, pv_out), (mv_hbm, mv_out), (vv_hbm, vv_out), (lr_hbm, lr_ref)))
    ]
    vraw_copy = pltpu.make_async_copy(gv_hbm, vraw.at[:, pl.ds(0, n_vec)], st_sem.at[7])

    barrier = pltpu.get_barrier_semaphore()
    for mask in range(1, N_DEV):
        pl.semaphore_signal(barrier, inc=1, device_id=(peer[mask],), device_id_type=MESH)
    for b in range(NRAW):
        raw_copy(b, 0).start()
    vraw[:, pl.ds(n_vec // 1024 * 1024, 2 * VROWS * LANES - n_vec // 1024 * 1024)] = jnp.zeros(
        (1, 2 * VROWS * LANES - n_vec // 1024 * 1024), BF16)
    acc[...] = jnp.zeros_like(acc)
    step_rows = 64

    def pack_rows(src, dst, first):
        def body(i, _):
            vals = src[:, pl.ds(pl.multiple_of(i * step_rows * LANES, 2048), step_rows * LANES)]
            dst[rows(first + i * step_rows, step_rows), :] = (
                vals.astype(F32).reshape(step_rows, LANES).astype(BF16))
            return 0
        lax.fori_loop(0, rc // step_rows, body, 0, unroll=2)

    def load_block(b, c):
        kind, _, _, _, slot = blocks[b]
        raw_copy(b, c).wait()
        if kind == "send":
            @pl.when(c >= 2)
            def _():
                block_copy(b, c - 2).wait_send()
            pack_rows(raw.at[b % NRAW], pk.at[lax.rem(c, 2), send_slot[b]], 0)
        else:
            pack_rows(raw.at[b % NRAW], big, slot * half + c * rc)
        if b + NRAW < n_blocks:
            raw_copy(b + NRAW, c).start()
        else:
            @pl.when(c + 1 < NC)
            def _():
                raw_copy(b + NRAW - n_blocks, c + 1).start()

    for b in range(EARLY):
        load_block(b, 0)
    pl.semaphore_wait(barrier, N_DEV - 1)

    def send_chunk(c):
        waiting = None
        for b, (kind, h, mask, dest, slot) in enumerate(blocks):
            if b < EARLY:
                @pl.when(c >= 1)
                def _():
                    load_block(b, c)
            else:
                load_block(b, c)
            if waiting is not None:
                block_copy(waiting, c).start()
            waiting = b if kind == "send" else None
        if waiting is not None:
            block_copy(waiting, c).start()

    sum_rows = 32

    def relay_chunk(c):
        par = lax.rem(c, 2)
        for h in (0, 1):
            for j in range(3):
                landed(h * 3 + j, c).wait_recv()

            @pl.when(c >= 2)
            def _():
                rel_copy(h, c - 2).wait_send()

            def body(i, _):
                at = c * rc + i * sum_rows
                total = big[rows((14 + h) * half + at, sum_rows), :].astype(F32)
                for j in (2, 0, 1):
                    total = total + big[rows((h * 3 + j) * half + at, sum_rows), :].astype(F32)
                rel[par, h, rows(i * sum_rows, sum_rows), :] = total
                return 0
            lax.fori_loop(0, rc // sum_rows, body, 0)
        for h in (0, 1):
            rel_copy(h, c).start()

    def final_chunk(c):
        for h in (0, 1):
            for j in range(3):
                landed(6 + h * 3 + j, c).wait_recv()
            rel_copy(h, c).wait_recv()

            def body(i, sq):
                at = c * rc + i * sum_rows
                total = big[rows((12 + h) * half + at, sum_rows), :].astype(F32)
                for j in (2, 0, 1):
                    total = total + big[rows((6 + h * 3 + j) * half + at, sum_rows), :].astype(F32)
                total = total + fin[rows(h * half + at, sum_rows), :]
                fin[rows(h * half + at, sum_rows), :] = total
                total = total * total
                for k in range(sum_rows // 8):
                    sq = sq + total[8 * k:8 * k + 8]
                return sq
            acc[...] = lax.fori_loop(0, rc // sum_rows, body, acc[...], unroll=4)

    mine = rows(core * VROWS, VROWS)
    other = rows((1 - core) * VROWS, VROWS)
    vec_core = remote(vpk.at[other], vland, vs_sem.at[0], vr_sem.at[0], 1)
    vec_x = remote(vs1, vlx, vs_sem.at[1], vr_sem.at[1], 2)
    vec_y = remote(vs2, vly, vs_sem.at[2], vr_sem.at[2], 4)
    vec_back = remote(vfull.at[mine], vfull.at[mine], vs_sem.at[3], vr_sem.at[3], 1)
    vec_back_in = remote(vfull.at[other], vfull.at[other], vs_sem.at[3], vr_sem.at[3], 1)

    def vec_step(c):
        @pl.when(c == 1)
        def _():
            vraw_copy.wait()
            vpk[...] = vraw[...].astype(F32).reshape(2 * VROWS, LANES).astype(BF16)

        @pl.when(c == 2)
        def _():
            vec_core.start()

        @pl.when(c == 3)
        def _():
            vec_core.wait_recv()
            vs1[...] = vpk[mine, :].astype(F32) + vland[...].astype(F32)

        @pl.when(c == 4)
        def _():
            vec_x.start()

        @pl.when(c == 6)
        def _():
            vec_x.wait_recv()
            vs2[...] = vs1[...] + vlx[...]

        @pl.when(c == 7)
        def _():
            vec_y.start()

        @pl.when(c == 9)
        def _():
            vec_y.wait_recv()
            vfull[mine, :] = vs2[...] + vly[...]

        @pl.when(c == 10)
        def _():
            vec_back.start()

        @pl.when(c == 12)
        def _():
            vec_back_in.wait_recv()
            vec_core.wait_send()
            vec_x.wait_send()
            vec_y.wait_send()
            vec_back.wait_send()

    def scatter_step(c, _):
        @pl.when(c < NC)
        def _():
            send_chunk(c)

        @pl.when(c == 0)
        def _():
            vraw_copy.start()

        @pl.when(c == 3)
        def _():
            for copy in state_copies:
                copy.start()

        vec_step(c)

        @pl.when((c >= 1) & (c < NC + 1))
        def _():
            relay_chunk(c - 1)

        @pl.when(c >= 2)
        def _():
            final_chunk(c - 2)
        return 0

    lax.fori_loop(0, NC + 2, scatter_step, 0)

    norms[me] = acc[...]
    vec_sq = jnp.sum(vfull[...] * vfull[...], keepdims=True)
    for copy in state_copies:
        copy.wait()

    def norm_copy(mask):
        return remote(norms.at[me], norms.at[me], ns_sem.at[mask - 1], nr_sem.at[mask - 1], mask)

    for mask in (6, 7, 2, 4, 3, 5, 1):
        norm_copy(mask).start()
    for c in (NC - 2, NC - 1):
        for b in send_slot:
            block_copy(b, c).wait_send()
        for h in (0, 1):
            rel_copy(h, c).wait_send()
    for mask in range(1, N_DEV):
        norm_copy(mask).wait_recv()
    total = norms[0]
    for k in range(1, N_DEV):
        total = total + norms[k]
    norm_sq = (jnp.sum(total, keepdims=True) + vec_sq) * (1.0 / (N_DEV * N_DEV))
    clip = jnp.minimum(1.0, MAX_NORM / (jnp.sqrt(norm_sq) + NORM_EPS)) * (1.0 / N_DEV)
    lr = lr_ref[...]

    upd_rows = 32
    clip_rows = jnp.broadcast_to(clip, (upd_rows, LANES))
    lr_rows = jnp.broadcast_to(lr, (upd_rows, LANES))

    def update_chunk(h, c):
        def body(i, _):
            at = h * half + c * rc + i * upd_rows
            here = rows(at, upd_rows)
            new_p, new_m, new_v = adam_update(
                fin[here, :] * clip_rows, p_ref[here, :], m_ref[here, :], v_ref[here, :], lr_rows, WEIGHT_DECAY)
            p_ref[here, :] = new_p
            m_ref[here, :] = new_m
            v_ref[here, :] = new_v
            big[rows(me * piece_rows + at, upd_rows), :] = new_p.astype(BF16)
            return 0
        lax.fori_loop(0, rc // upd_rows, body, 0, unroll=4)

    def gather_copy(mask, h, c, dest, ssem, slot):
        piece = flip(me, mask) if mask else me
        ref = big.at[rows(piece * piece_rows + h * half + c * rc, rc)]
        return remote(ref, ref, ag_sem.at[ssem], rs.at[slot, c], dest)

    def own_x(h, c):
        return gather_copy(0, h, c, 2, 0, h)

    def own_y(h, c):
        return gather_copy(0, h, c, 4, 1, 2 + h)

    def own_core(h, c):
        return gather_copy(0, h, c, 1, 2, 6 + h)

    def arrived(mask, h, c, slot):
        gather_copy(mask, h, c, 1, 0, slot).wait_recv()

    def to_core(mask, h, c):
        return gather_copy(mask, h, c, 1, {2: 5, 4: 6, 6: 7}[mask], {2: 8, 4: 10, 6: 12}[mask] + h)

    def first_half(i, _):
        @pl.when(i < NC)
        def _():
            update_chunk(0, i)
            own_x(0, i).start()
            update_chunk(1, i)
            own_y(1, i).start()
            own_core(0, i).start()
            own_core(1, i).start()

        @pl.when(i >= LAG)
        def _():
            j = i - LAG
            arrived(2, 0, j, 0)
            gather_copy(2, 0, j, 4, 3, 4).start()
            to_core(2, 0, j).start()
            arrived(4, 1, j, 3)
            gather_copy(4, 1, j, 2, 4, 5).start()
            to_core(4, 1, j).start()

        @pl.when(i >= NC)
        def _():
            own_x(1, i - NC).start()
            own_y(0, i - NC).start()
        return 0

    lax.fori_loop(0, NC + LAG, first_half, 0)

    kept = half - TAIL * rc
    tail_copies = [
        pltpu.make_async_copy(
            big.at[rows(me * piece_rows + h * half + kept, TAIL * rc)], dst, px_sem.at[h])
        for h, dst in ((1, px_hbm), (0, py_hbm))
    ]
    for copy in tail_copies:
        copy.start()

    vrows = n_vec // LANES
    new_p, new_m, new_v = adam_update(
        vfull[pl.ds(0, vrows), :] * clip, pv_out[...], mv_out[...], vv_out[...], lr, 0.0)
    pv_out[...] = new_p
    mv_out[...] = new_m
    vv_out[...] = new_v

    def second_half(j, _):
        @pl.when(j + LAG < NC - TAIL)
        def _():
            own_x(1, j + LAG).start()
            own_y(0, j + LAG).start()
        arrived(6, 0, j, 4)
        to_core(6, 0, j).start()
        arrived(6, 1, j, 5)
        to_core(6, 1, j).start()

        @pl.when(j < NC - TAIL)
        def _():
            arrived(2, 1, j, 1)
            to_core(2, 1, j).start()
            arrived(4, 0, j, 2)
            to_core(4, 0, j).start()
        return 0

    lax.fori_loop(0, NC, second_half, 0)

    def last_arrivals(c, _):
        for mask, h in ((1, 0), (1, 1), (3, 0), (5, 1), (7, 0), (7, 1)):
            arrived(mask, h, c, 5 + mask + h)

        @pl.when(c < NC - TAIL)
        def _():
            for mask, h in ((3, 1), (5, 0)):
                arrived(mask, h, c, 5 + mask + h)
        return 0

    lax.fori_loop(0, NC, last_arrivals, 0)
    for ssem, count in (
        (0, half + kept), (1, half + kept), (2, 2 * half), (3, half), (4, half),
        (5, half + kept), (6, half + kept), (7, 2 * half),
    ):
        ref = big.at[pl.ds(0, count)]
        remote(ref, ref, ag_sem.at[ssem], rs.at[0, 0], 1).wait_send()
    for mask in range(1, N_DEV):
        norm_copy(mask).wait_send()
    for copy in tail_copies:
        copy.wait()


def run_all(copies):
    for copy in copies:
        copy.start()
    for copy in copies:
        copy.wait()


def first_write(half, state, big, *refs):
    dsts, sem = refs[:-1], refs[-1]
    copies = []

    def add(src, src_at, dst, count, size):
        part = size // count
        for k in range(count):
            copies.append(pltpu.make_async_copy(
                src.at[pl.ds(src_at + k * part, part)], dst.at[pl.ds(k * part, part)], sem.at[len(copies)]))

    at = 0
    for dst in dsts[:6]:
        size = dst.shape[0]
        add(state, at, dst, 4 if size > 2 * VROWS else 1, size)
        at += max(size, 2 * VROWS)
    add(big, 0, dsts[6], SPLIT, SPLIT * half)
    run_all(copies)


def second_write(half, big, _, dst, sem):
    run_all([
        pltpu.make_async_copy(big.at[pl.ds(k * half, half)], dst.at[pl.ds(k * half, half)], sem.at[k - SPLIT])
        for k in range(SPLIT, 2 * N_DEV)
    ])


def tail_write(half, tail, rx, ry, cx, cy, _, dst, buf, sem):
    me = lax.axis_index("dp")
    parts = ((rx, 2, 1), (ry, 4, 0), (cx, 3, 1), (cy, 5, 0))
    fetches, stores = [], []
    for i, (src, mask, h) in enumerate(parts):
        at = flip(me, mask) * (2 * half) + (h + 1) * half - tail
        fetches.append(pltpu.make_async_copy(src, buf.at[i], sem.at[i]))
        stores.append(pltpu.make_async_copy(
            buf.at[i], dst.at[pl.ds(pl.multiple_of(at, 16), tail)], sem.at[4 + i]))
    for fetch in fetches:
        fetch.start()
    for fetch, store in zip(fetches, stores):
        fetch.wait()
        store.start()
    for store in stores:
        store.wait()


def solution(mesh):
    axis_name = mesh.axis_names[0]

    def local_step(g_mat, g_vec, p_mat, m_mat, v_mat, p_vec, m_vec, v_vec, learn_rate):
        n_piece = p_mat.shape[0]
        n_vec = p_vec.shape[0]
        piece_rows = n_piece // LANES
        half = piece_rows // 2
        rc = half // NC
        state = (piece_rows, LANES)
        vec = (n_vec // LANES, LANES)
        full = (N_DEV * piece_rows, LANES)
        any_spec = pl.BlockSpec(memory_space=pl.ANY)
        vmem_spec = pl.BlockSpec(memory_space=pltpu.VMEM)
        state_new, big, px, py = pl.pallas_call(
            functools.partial(step_kernel, half, rc, n_vec),
            out_shape=[pltpu.VMEM((3 * piece_rows + 6 * VROWS, LANES), F32), pltpu.VMEM(full, BF16)]
            + [jax.ShapeDtypeStruct((TAIL * rc, LANES), BF16)] * 2,
            in_specs=[any_spec] * 9,
            out_specs=[vmem_spec] * 2 + [any_spec] * 2,
            scratch_shapes=[
                pltpu.VMEM(state, F32),
                pltpu.VMEM((NRAW, 1, rc * LANES), BF16),
                pltpu.VMEM((2, 12, rc, LANES), BF16),
                pltpu.VMEM((2, 2, rc, LANES), F32),
                pltpu.VMEM((8, LANES), F32),
                pltpu.VMEM((N_DEV, 8, LANES), F32),
                pltpu.VMEM((1, 2 * VROWS * LANES), BF16),
                pltpu.VMEM((2 * VROWS, LANES), BF16),
                pltpu.VMEM((VROWS, LANES), BF16),
                pltpu.VMEM((VROWS, LANES), F32),
                pltpu.VMEM((VROWS, LANES), F32),
                pltpu.VMEM((VROWS, LANES), F32),
                pltpu.VMEM((VROWS, LANES), F32),
                pltpu.VMEM((2 * VROWS, LANES), F32),
                pltpu.VMEM((1, 1), F32),
                pltpu.SemaphoreType.DMA((NRAW,)),
                pltpu.SemaphoreType.DMA((2, 12)),
                pltpu.SemaphoreType.DMA((2, 2)),
                pltpu.SemaphoreType.DMA((14, NC)),
                pltpu.SemaphoreType.DMA((8,)),
                pltpu.SemaphoreType.DMA((7,)),
                pltpu.SemaphoreType.DMA((7,)),
                pltpu.SemaphoreType.DMA((4,)),
                pltpu.SemaphoreType.DMA((4,)),
                pltpu.SemaphoreType.DMA((8,)),
                pltpu.SemaphoreType.DMA((2,)),
            ],
            compiler_params=pltpu.CompilerParams(
                collective_id=0, has_side_effects=True, vmem_limit_bytes=15 * 2 ** 20),
            name="step",
        )(
            g_mat, g_vec, p_mat.reshape(state), m_mat.reshape(state), v_mat.reshape(state),
            p_vec.reshape(vec), m_vec.reshape(vec), v_vec.reshape(vec), learn_rate.reshape(1, 1),
        )
        def permute(values, mask):
            return lax.ppermute(values, axis_name, [(d, d ^ mask) for d in range(N_DEV)])

        def cost(n_bytes):
            return pl.CostEstimate(flops=0, bytes_accessed=n_bytes, transcendentals=0)

        rx, ry = permute(px, 2), permute(py, 4)
        p_new, m_new, v_new, pv_new, mv_new, vv_new, pb = pl.pallas_call(
            functools.partial(first_write, half),
            out_shape=[jax.ShapeDtypeStruct(state, F32)] * 3 + [jax.ShapeDtypeStruct(vec, F32)] * 3
            + [jax.ShapeDtypeStruct(full, BF16)],
            in_specs=[vmem_spec] * 2,
            out_specs=[any_spec] * 7,
            scratch_shapes=[pltpu.SemaphoreType.DMA((15 + SPLIT,))],
            cost_estimate=cost(12 * n_piece + SPLIT * n_piece),
            compiler_params=pltpu.CompilerParams(vmem_limit_bytes=2 ** 20),
            name="write1",
        )(state_new, big)
        rx, ry, p_new = lax.optimization_barrier((rx, ry, p_new))
        cx, cy = permute(rx, 1), permute(ry, 1)
        pb = pl.pallas_call(
            functools.partial(second_write, half),
            out_shape=jax.ShapeDtypeStruct(full, BF16),
            in_specs=[vmem_spec, any_spec],
            out_specs=any_spec,
            input_output_aliases={1: 0},
            scratch_shapes=[pltpu.SemaphoreType.DMA((2 * N_DEV - SPLIT,))],
            cost_estimate=cost((2 * N_DEV - SPLIT) * n_piece),
            compiler_params=pltpu.CompilerParams(vmem_limit_bytes=2 ** 20),
            name="write2",
        )(big, pb)
        pb = pl.pallas_call(
            functools.partial(tail_write, half, TAIL * rc),
            out_shape=jax.ShapeDtypeStruct(full, BF16),
            in_specs=[any_spec] * 5,
            out_specs=any_spec,
            input_output_aliases={4: 0},
            scratch_shapes=[pltpu.VMEM((4, TAIL * rc, LANES), BF16), pltpu.SemaphoreType.DMA((8,))],
            compiler_params=pltpu.CompilerParams(vmem_limit_bytes=4 * 2 ** 20),
            name="write3",
        )(rx, ry, cx, cy, pb)
        return (
            p_new.reshape(-1), m_new.reshape(-1), v_new.reshape(-1),
            pv_new.reshape(-1), mv_new.reshape(-1), vv_new.reshape(-1), pb.reshape(-1),
        )

    return jax.shard_map(
        local_step,
        mesh=mesh,
        in_specs=(P(axis_name, None), P(axis_name, None), P(axis_name), P(axis_name), P(axis_name), P(), P(), P(), P()),
        out_specs=(P(axis_name), P(axis_name), P(axis_name), P(), P(), P(), P()),
        check_vma=False,
    )
```

```python
import functools

import jax
import jax.numpy as jnp
from jax import lax
from jax.experimental import pallas as pl
from jax.experimental.pallas import tpu as pltpu
from jax.sharding import PartitionSpec as P

STEP = 10
ADAM_BETA1 = 0.9
ADAM_BETA2 = 0.98
ADAM_EPS = 1e-8
WEIGHT_DECAY = 0.01
MAX_NORM = 1.0
NORM_EPS = 1e-6
BIAS_ONE = 1.0 - ADAM_BETA1 ** STEP
BIAS_TWO = 1.0 - ADAM_BETA2 ** STEP

LANES = 128
N_DEV = 8
NC = 18
NRAW = 8
EARLY = 4
TAIL = 7
SPLIT = 15
DIAG_LAG = 6
LAG = 2
VROWS = 80
MESH = pl.DeviceIdType.MESH
F32 = jnp.float32
BF16 = jnp.bfloat16


def adam_update(grad_vals, param_vals, moment_one, moment_two, learn_rate, decay_rate):
    new_one = ADAM_BETA1 * moment_one + (1.0 - ADAM_BETA1) * grad_vals
    new_two = ADAM_BETA2 * moment_two + (1.0 - ADAM_BETA2) * grad_vals * grad_vals
    direction = (new_one / BIAS_ONE) / (jnp.sqrt(new_two / BIAS_TWO) + ADAM_EPS)
    return param_vals - learn_rate * (direction + decay_rate * param_vals), new_one, new_two


def flip(device, mask):
    for bit in (1, 2, 4):
        if mask & bit:
            device = device + bit - 2 * bit * lax.rem(lax.div(device, bit), 2)
    return device


def step_kernel(
    half, rc, n_vec,
    g_hbm, gv_hbm, p_hbm, m_hbm, v_hbm, pv_hbm, mv_hbm, vv_hbm, lr_hbm,
    state, big, px_hbm, py_hbm,
    fin, raw, pk, rel, acc, norms, vraw, vpk, vland, vs1, vlx, vs2, vly, vfull, lr_ref,
    raw_sem, send_sem, rel_sem, rs, st_sem, ns_sem, nr_sem, vs_sem, vr_sem, ag_sem, px_sem,
):
    piece_rows = 2 * half
    p_ref, m_ref, v_ref = (state.at[pl.ds(k * piece_rows, piece_rows)] for k in range(3))
    pv_out, mv_out, vv_out = (
        state.at[pl.ds(3 * piece_rows + k * 2 * VROWS, n_vec // LANES)] for k in range(3))
    me = lax.axis_index("dp")
    core = lax.rem(me, 2)
    peer = {mask: flip(me, mask) for mask in range(1, N_DEV)}

    def remote(src, dst, ssem, rsem, mask):
        return pltpu.make_async_remote_copy(
            src_ref=src, dst_ref=dst, send_sem=ssem, recv_sem=rsem,
            device_id=(peer[mask],), device_id_type=MESH,
        )

    def rows(first, count, align=16):
        return pl.ds(pl.multiple_of(first, align), count)

    blocks = []
    for j in (0, 1):
        for h in (0, 1):
            via = (4, 2)[h]
            blocks.append(("send", h, 6 ^ j, via ^ j, h * 3 + j))
    for h in (0, 1):
        blocks.append(("send", h, (2, 4)[h] ^ 1, 1, h * 3 + 2))
        blocks.append(("own", h, (2, 4)[h], None, 14 + h))
    for j in (0, 1):
        for h in (0, 1):
            via = (4, 2)[h]
            blocks.append(("send", h, via ^ j, via ^ j, 6 + h * 3 + j))
    for h in (0, 1):
        blocks.append(("send", h, 1, 1, 6 + h * 3 + 2))
        blocks.append(("own", h, 0, None, 12 + h))
    n_blocks = len(blocks)
    send_slot = {}
    for b, block in enumerate(blocks):
        if block[0] == "send":
            send_slot[b] = len(send_slot)

    def raw_copy(b, c):
        _, h, mask, _, _ = blocks[b]
        piece = flip(me, mask) if mask else me
        start = (piece * piece_rows + h * half + c * rc) * LANES
        return pltpu.make_async_copy(
            g_hbm.at[:, pl.ds(pl.multiple_of(start, 2048), rc * LANES)],
            raw.at[b % NRAW], raw_sem.at[b % NRAW],
        )

    def block_copy(b, c):
        _, h, _, dest, slot = blocks[b]
        s = send_slot[b]
        par = lax.rem(c, 2)
        return remote(
            pk.at[par, s], big.at[rows(slot * half + c * rc, rc)],
            send_sem.at[par, s], rs.at[slot, c], dest,
        )

    def landed(slot, c):
        ref = big.at[rows(slot * half + c * rc, rc)]
        return remote(ref, ref, send_sem.at[0, 0], rs.at[slot, c], 1)

    def rel_copy(h, c):
        par = lax.rem(c, 2)
        return remote(
            rel.at[par, h], fin.at[rows(h * half + c * rc, rc)],
            rel_sem.at[par, h], rs.at[12 + h, c], (2, 4)[h],
        )

    state_copies = [
        pltpu.make_async_copy(src, dst, st_sem.at[i])
        for i, (src, dst) in enumerate((
            (p_hbm, p_ref), (m_hbm, m_ref), (v_hbm, v_ref),
            (pv_hbm, pv_out), (mv_hbm, mv_out), (vv_hbm, vv_out), (lr_hbm, lr_ref)))
    ]
    vraw_copy = pltpu.make_async_copy(gv_hbm, vraw.at[:, pl.ds(0, n_vec)], st_sem.at[7])

    barrier = pltpu.get_barrier_semaphore()
    for mask in range(1, N_DEV):
        pl.semaphore_signal(barrier, inc=1, device_id=(peer[mask],), device_id_type=MESH)
    for b in range(NRAW):
        raw_copy(b, 0).start()
    vraw[:, pl.ds(n_vec // 1024 * 1024, 2 * VROWS * LANES - n_vec // 1024 * 1024)] = jnp.zeros(
        (1, 2 * VROWS * LANES - n_vec // 1024 * 1024), BF16)
    acc[...] = jnp.zeros_like(acc)
    step_rows = 64

    def pack_rows(src, dst, first):
        def body(i, _):
            vals = src[:, pl.ds(pl.multiple_of(i * step_rows * LANES, 2048), step_rows * LANES)]
            dst[rows(first + i * step_rows, step_rows), :] = (
                vals.astype(F32).reshape(step_rows, LANES).astype(BF16))
            return 0
        lax.fori_loop(0, rc // step_rows, body, 0, unroll=2)

    def load_block(b, c):
        kind, _, _, _, slot = blocks[b]
        raw_copy(b, c).wait()
        if kind == "send":
            @pl.when(c >= 2)
            def _():
                block_copy(b, c - 2).wait_send()
            pack_rows(raw.at[b % NRAW], pk.at[lax.rem(c, 2), send_slot[b]], 0)
        else:
            pack_rows(raw.at[b % NRAW], big, slot * half + c * rc)
        if b + NRAW < n_blocks:
            raw_copy(b + NRAW, c).start()
        else:
            @pl.when(c + 1 < NC)
            def _():
                raw_copy(b + NRAW - n_blocks, c + 1).start()

    for b in range(EARLY):
        load_block(b, 0)
    pl.semaphore_wait(barrier, N_DEV - 1)

    def send_chunk(c):
        waiting = None
        for b, (kind, h, mask, dest, slot) in enumerate(blocks):
            if b < EARLY:
                @pl.when(c >= 1)
                def _():
                    load_block(b, c)
            else:
                load_block(b, c)
            if waiting is not None:
                block_copy(waiting, c).start()
            waiting = b if kind == "send" else None
        if waiting is not None:
            block_copy(waiting, c).start()

    sum_rows = 32

    def relay_chunk(c):
        par = lax.rem(c, 2)
        for h in (0, 1):
            for j in range(3):
                landed(h * 3 + j, c).wait_recv()

            @pl.when(c >= 2)
            def _():
                rel_copy(h, c - 2).wait_send()

            def body(i, _):
                at = c * rc + i * sum_rows
                total = big[rows((14 + h) * half + at, sum_rows), :].astype(F32)
                for j in (2, 0, 1):
                    total = total + big[rows((h * 3 + j) * half + at, sum_rows), :].astype(F32)
                rel[par, h, rows(i * sum_rows, sum_rows), :] = total
                return 0
            lax.fori_loop(0, rc // sum_rows, body, 0)
        for h in (0, 1):
            rel_copy(h, c).start()

    def final_chunk(c):
        for h in (0, 1):
            for j in range(3):
                landed(6 + h * 3 + j, c).wait_recv()
            rel_copy(h, c).wait_recv()

            def body(i, sq):
                at = c * rc + i * sum_rows
                total = big[rows((12 + h) * half + at, sum_rows), :].astype(F32)
                for j in (2, 0, 1):
                    total = total + big[rows((6 + h * 3 + j) * half + at, sum_rows), :].astype(F32)
                total = total + fin[rows(h * half + at, sum_rows), :]
                fin[rows(h * half + at, sum_rows), :] = total
                total = total * total
                for k in range(sum_rows // 8):
                    sq = sq + total[8 * k:8 * k + 8]
                return sq
            acc[...] = lax.fori_loop(0, rc // sum_rows, body, acc[...], unroll=4)

    mine = rows(core * VROWS, VROWS)
    other = rows((1 - core) * VROWS, VROWS)
    vec_core = remote(vpk.at[other], vland, vs_sem.at[0], vr_sem.at[0], 1)
    vec_x = remote(vs1, vlx, vs_sem.at[1], vr_sem.at[1], 2)
    vec_y = remote(vs2, vly, vs_sem.at[2], vr_sem.at[2], 4)
    vec_back = remote(vfull.at[mine], vfull.at[mine], vs_sem.at[3], vr_sem.at[3], 1)
    vec_back_in = remote(vfull.at[other], vfull.at[other], vs_sem.at[3], vr_sem.at[3], 1)

    def vec_step(c):
        @pl.when(c == 1)
        def _():
            vraw_copy.wait()
            vpk[...] = vraw[...].astype(F32).reshape(2 * VROWS, LANES).astype(BF16)

        @pl.when(c == 2)
        def _():
            vec_core.start()

        @pl.when(c == 3)
        def _():
            vec_core.wait_recv()
            vs1[...] = vpk[mine, :].astype(F32) + vland[...].astype(F32)

        @pl.when(c == 4)
        def _():
            vec_x.start()

        @pl.when(c == 6)
        def _():
            vec_x.wait_recv()
            vs2[...] = vs1[...] + vlx[...]

        @pl.when(c == 7)
        def _():
            vec_y.start()

        @pl.when(c == 9)
        def _():
            vec_y.wait_recv()
            vfull[mine, :] = vs2[...] + vly[...]

        @pl.when(c == 10)
        def _():
            vec_back.start()

        @pl.when(c == 12)
        def _():
            vec_back_in.wait_recv()
            vec_core.wait_send()
            vec_x.wait_send()
            vec_y.wait_send()
            vec_back.wait_send()

    def scatter_step(c, _):
        @pl.when(c < NC)
        def _():
            send_chunk(c)

        @pl.when(c == 0)
        def _():
            vraw_copy.start()

        @pl.when(c == 3)
        def _():
            for copy in state_copies:
                copy.start()

        vec_step(c)

        @pl.when((c >= 1) & (c < NC + 1))
        def _():
            relay_chunk(c - 1)

        @pl.when(c >= 2)
        def _():
            final_chunk(c - 2)
        return 0

    lax.fori_loop(0, NC + 2, scatter_step, 0)

    norms[me] = acc[...]
    vec_sq = jnp.sum(vfull[...] * vfull[...], keepdims=True)
    for copy in state_copies:
        copy.wait()

    def norm_copy(mask):
        return remote(norms.at[me], norms.at[me], ns_sem.at[mask - 1], nr_sem.at[mask - 1], mask)

    for mask in (6, 7, 2, 4, 3, 5, 1):
        norm_copy(mask).start()
    for c in (NC - 2, NC - 1):
        for b in send_slot:
            block_copy(b, c).wait_send()
        for h in (0, 1):
            rel_copy(h, c).wait_send()
    for mask in range(1, N_DEV):
        norm_copy(mask).wait_recv()
    total = norms[0]
    for k in range(1, N_DEV):
        total = total + norms[k]
    norm_sq = (jnp.sum(total, keepdims=True) + vec_sq) * (1.0 / (N_DEV * N_DEV))
    clip = jnp.minimum(1.0, MAX_NORM / (jnp.sqrt(norm_sq) + NORM_EPS)) * (1.0 / N_DEV)
    lr = lr_ref[...]

    upd_rows = 32
    clip_rows = jnp.broadcast_to(clip, (upd_rows, LANES))
    lr_rows = jnp.broadcast_to(lr, (upd_rows, LANES))

    def update_chunk(h, c):
        def body(i, _):
            at = h * half + c * rc + i * upd_rows
            here = rows(at, upd_rows)
            new_p, new_m, new_v = adam_update(
                fin[here, :] * clip_rows, p_ref[here, :], m_ref[here, :], v_ref[here, :], lr_rows, WEIGHT_DECAY)
            p_ref[here, :] = new_p
            m_ref[here, :] = new_m
            v_ref[here, :] = new_v
            big[rows(me * piece_rows + at, upd_rows), :] = new_p.astype(BF16)
            return 0
        lax.fori_loop(0, rc // upd_rows, body, 0, unroll=4)

    def gather_copy(mask, h, c, dest, ssem, slot):
        piece = flip(me, mask) if mask else me
        ref = big.at[rows(piece * piece_rows + h * half + c * rc, rc)]
        return remote(ref, ref, ag_sem.at[ssem], rs.at[slot, c], dest)

    def own_x(h, c):
        return gather_copy(0, h, c, 2, 0, h)

    def own_y(h, c):
        return gather_copy(0, h, c, 4, 1, 2 + h)

    def own_core(h, c):
        return gather_copy(0, h, c, 1, 2, 6 + h)

    def arrived(mask, h, c, slot):
        gather_copy(mask, h, c, 1, 0, slot).wait_recv()

    def to_core(mask, h, c):
        return gather_copy(mask, h, c, 1, {2: 5, 4: 6, 6: 7}[mask], {2: 8, 4: 10, 6: 12}[mask] + h)

    def diagonal(j):
        arrived(6, 0, j, 4)
        to_core(6, 0, j).start()
        arrived(6, 1, j, 5)
        to_core(6, 1, j).start()

    def first_half(i, _):
        @pl.when(i < NC)
        def _():
            update_chunk(0, i)
            own_x(0, i).start()
            update_chunk(1, i)
            own_y(1, i).start()
            own_core(0, i).start()
            own_core(1, i).start()

        @pl.when(i >= LAG)
        def _():
            j = i - LAG
            arrived(2, 0, j, 0)
            gather_copy(2, 0, j, 4, 3, 4).start()
            to_core(2, 0, j).start()
            arrived(4, 1, j, 3)
            gather_copy(4, 1, j, 2, 4, 5).start()
            to_core(4, 1, j).start()

        @pl.when(i >= DIAG_LAG)
        def _():
            diagonal(i - DIAG_LAG)

        @pl.when(i >= NC)
        def _():
            own_x(1, i - NC).start()
            own_y(0, i - NC).start()
        return 0

    lax.fori_loop(0, NC + LAG, first_half, 0)

    kept = half - TAIL * rc
    tail_copies = [
        pltpu.make_async_copy(
            big.at[rows(me * piece_rows + h * half + kept, TAIL * rc)], dst, px_sem.at[h])
        for h, dst in ((1, px_hbm), (0, py_hbm))
    ]
    for copy in tail_copies:
        copy.start()

    vrows = n_vec // LANES
    new_p, new_m, new_v = adam_update(
        vfull[pl.ds(0, vrows), :] * clip, pv_out[...], mv_out[...], vv_out[...], lr, 0.0)
    pv_out[...] = new_p
    mv_out[...] = new_m
    vv_out[...] = new_v

    def second_half(j, _):
        @pl.when(j + LAG < NC - TAIL)
        def _():
            own_x(1, j + LAG).start()
            own_y(0, j + LAG).start()
        @pl.when(j < DIAG_LAG - LAG)
        def _():
            diagonal(NC + LAG - DIAG_LAG + j)
        arrived(2, 1, j, 1)
        to_core(2, 1, j).start()
        arrived(4, 0, j, 2)
        to_core(4, 0, j).start()
        return 0

    lax.fori_loop(0, NC - TAIL, second_half, 0)

    def last_arrivals(c, _):
        for mask, h in ((1, 0), (1, 1), (3, 0), (5, 1), (7, 0), (7, 1)):
            arrived(mask, h, c, 5 + mask + h)

        @pl.when(c < NC - TAIL)
        def _():
            for mask, h in ((3, 1), (5, 0)):
                arrived(mask, h, c, 5 + mask + h)
        return 0

    lax.fori_loop(0, NC, last_arrivals, 0)
    for ssem, count in (
        (0, half + kept), (1, half + kept), (2, 2 * half), (3, half), (4, half),
        (5, half + kept), (6, half + kept), (7, 2 * half),
    ):
        ref = big.at[pl.ds(0, count)]
        remote(ref, ref, ag_sem.at[ssem], rs.at[0, 0], 1).wait_send()
    for mask in range(1, N_DEV):
        norm_copy(mask).wait_send()
    for copy in tail_copies:
        copy.wait()


def run_all(copies):
    for copy in copies:
        copy.start()
    for copy in copies:
        copy.wait()


def first_write(half, state, big, *refs):
    dsts, sem = refs[:-1], refs[-1]
    copies = []

    def add(src, src_at, dst, count, size):
        part = size // count
        for k in range(count):
            copies.append(pltpu.make_async_copy(
                src.at[pl.ds(src_at + k * part, part)], dst.at[pl.ds(k * part, part)], sem.at[len(copies)]))

    at = 0
    for dst in dsts[:6]:
        size = dst.shape[0]
        add(state, at, dst, 4 if size > 2 * VROWS else 1, size)
        at += max(size, 2 * VROWS)
    add(big, 0, dsts[6], SPLIT, SPLIT * half)
    run_all(copies)


def place_tails(half, tail, parts, dst, buf, sem, others=()):
    me = lax.axis_index("dp")
    fetches, stores = [], []
    for i, (src, mask, h) in enumerate(parts):
        at = flip(me, mask) * (2 * half) + (h + 1) * half - tail
        fetches.append(pltpu.make_async_copy(src, buf.at[i], sem.at[i]))
        stores.append(pltpu.make_async_copy(
            buf.at[i], dst.at[pl.ds(pl.multiple_of(at, 16), tail)], sem.at[2 + i]))
    for copy in (*others, *fetches):
        copy.start()
    for copy in (*others, *fetches):
        copy.wait()
    run_all(stores)


def second_write(half, tail, big, rx, ry, _, dst, buf, sem):
    place_tails(half, tail, ((rx, 2, 1), (ry, 4, 0)), dst, buf, sem, [
        pltpu.make_async_copy(big.at[pl.ds(k * half, half)], dst.at[pl.ds(k * half, half)], sem.at[4 + k - SPLIT])
        for k in range(SPLIT, 2 * N_DEV)
    ])


def third_write(half, tail, cx, cy, _, dst, buf, sem):
    place_tails(half, tail, ((cx, 3, 1), (cy, 5, 0)), dst, buf, sem)


def solution(mesh):
    axis_name = mesh.axis_names[0]

    def local_step(g_mat, g_vec, p_mat, m_mat, v_mat, p_vec, m_vec, v_vec, learn_rate):
        n_piece = p_mat.shape[0]
        n_vec = p_vec.shape[0]
        piece_rows = n_piece // LANES
        half = piece_rows // 2
        rc = half // NC
        state = (piece_rows, LANES)
        vec = (n_vec // LANES, LANES)
        full = (N_DEV * piece_rows, LANES)
        any_spec = pl.BlockSpec(memory_space=pl.ANY)
        vmem_spec = pl.BlockSpec(memory_space=pltpu.VMEM)
        state_new, big, px, py = pl.pallas_call(
            functools.partial(step_kernel, half, rc, n_vec),
            out_shape=[pltpu.VMEM((3 * piece_rows + 6 * VROWS, LANES), F32), pltpu.VMEM(full, BF16)]
            + [jax.ShapeDtypeStruct((TAIL * rc, LANES), BF16)] * 2,
            in_specs=[any_spec] * 9,
            out_specs=[vmem_spec] * 2 + [any_spec] * 2,
            scratch_shapes=[
                pltpu.VMEM(state, F32),
                pltpu.VMEM((NRAW, 1, rc * LANES), BF16),
                pltpu.VMEM((2, 12, rc, LANES), BF16),
                pltpu.VMEM((2, 2, rc, LANES), F32),
                pltpu.VMEM((8, LANES), F32),
                pltpu.VMEM((N_DEV, 8, LANES), F32),
                pltpu.VMEM((1, 2 * VROWS * LANES), BF16),
                pltpu.VMEM((2 * VROWS, LANES), BF16),
                pltpu.VMEM((VROWS, LANES), BF16),
                pltpu.VMEM((VROWS, LANES), F32),
                pltpu.VMEM((VROWS, LANES), F32),
                pltpu.VMEM((VROWS, LANES), F32),
                pltpu.VMEM((VROWS, LANES), F32),
                pltpu.VMEM((2 * VROWS, LANES), F32),
                pltpu.VMEM((1, 1), F32),
                pltpu.SemaphoreType.DMA((NRAW,)),
                pltpu.SemaphoreType.DMA((2, 12)),
                pltpu.SemaphoreType.DMA((2, 2)),
                pltpu.SemaphoreType.DMA((14, NC)),
                pltpu.SemaphoreType.DMA((8,)),
                pltpu.SemaphoreType.DMA((7,)),
                pltpu.SemaphoreType.DMA((7,)),
                pltpu.SemaphoreType.DMA((4,)),
                pltpu.SemaphoreType.DMA((4,)),
                pltpu.SemaphoreType.DMA((8,)),
                pltpu.SemaphoreType.DMA((2,)),
            ],
            compiler_params=pltpu.CompilerParams(
                collective_id=0, has_side_effects=True, vmem_limit_bytes=15 * 2 ** 20),
            name="step",
        )(
            g_mat, g_vec, p_mat.reshape(state), m_mat.reshape(state), v_mat.reshape(state),
            p_vec.reshape(vec), m_vec.reshape(vec), v_vec.reshape(vec), learn_rate.reshape(1, 1),
        )
        def permute(values, mask):
            return lax.ppermute(values, axis_name, [(d, d ^ mask) for d in range(N_DEV)])

        def cost(n_bytes):
            return pl.CostEstimate(flops=0, bytes_accessed=n_bytes, transcendentals=0)

        rx, ry = permute(px, 2), permute(py, 4)
        p_new, m_new, v_new, pv_new, mv_new, vv_new, pb = pl.pallas_call(
            functools.partial(first_write, half),
            out_shape=[jax.ShapeDtypeStruct(state, F32)] * 3 + [jax.ShapeDtypeStruct(vec, F32)] * 3
            + [jax.ShapeDtypeStruct(full, BF16)],
            in_specs=[vmem_spec] * 2,
            out_specs=[any_spec] * 7,
            scratch_shapes=[pltpu.SemaphoreType.DMA((15 + SPLIT,))],
            cost_estimate=cost(12 * n_piece + SPLIT * n_piece),
            compiler_params=pltpu.CompilerParams(vmem_limit_bytes=2 ** 20),
            name="write1",
        )(state_new, big)
        rx, ry, p_new = lax.optimization_barrier((rx, ry, p_new))
        cx, cy = permute(rx, 1), permute(ry, 1)
        tail_buf = pltpu.VMEM((2, TAIL * rc, LANES), BF16)
        pb = pl.pallas_call(
            functools.partial(second_write, half, TAIL * rc),
            out_shape=jax.ShapeDtypeStruct(full, BF16),
            in_specs=[vmem_spec] + [any_spec] * 3,
            out_specs=any_spec,
            input_output_aliases={3: 0},
            scratch_shapes=[tail_buf, pltpu.SemaphoreType.DMA((4 + 2 * N_DEV - SPLIT,))],
            cost_estimate=cost((2 * N_DEV - SPLIT) * n_piece),
            compiler_params=pltpu.CompilerParams(vmem_limit_bytes=2 * 2 ** 20),
            name="write2",
        )(big, rx, ry, pb)
        pb = pl.pallas_call(
            functools.partial(third_write, half, TAIL * rc),
            out_shape=jax.ShapeDtypeStruct(full, BF16),
            in_specs=[any_spec] * 3,
            out_specs=any_spec,
            input_output_aliases={2: 0},
            scratch_shapes=[tail_buf, pltpu.SemaphoreType.DMA((4,))],
            compiler_params=pltpu.CompilerParams(vmem_limit_bytes=2 * 2 ** 20),
            name="write3",
        )(cx, cy, pb)
        return (
            p_new.reshape(-1), m_new.reshape(-1), v_new.reshape(-1),
            pv_new.reshape(-1), mv_new.reshape(-1), vv_new.reshape(-1), pb.reshape(-1),
        )

    return jax.shard_map(
        local_step,
        mesh=mesh,
        in_specs=(P(axis_name, None), P(axis_name, None), P(axis_name), P(axis_name), P(axis_name), P(), P(), P(), P()),
        out_specs=(P(axis_name), P(axis_name), P(axis_name), P(), P(), P(), P()),
        check_vma=False,
    )
```

```python
import functools

import jax
import jax.numpy as jnp
from jax import lax
from jax.experimental import pallas as pl
from jax.experimental.pallas import tpu as pltpu
from jax.sharding import PartitionSpec as P

STEP = 10
ADAM_BETA1 = 0.9
ADAM_BETA2 = 0.98
ADAM_EPS = 1e-8
WEIGHT_DECAY = 0.01
MAX_NORM = 1.0
NORM_EPS = 1e-6
BIAS_ONE = 1.0 - ADAM_BETA1 ** STEP
BIAS_TWO = 1.0 - ADAM_BETA2 ** STEP

LANES = 128
N_DEV = 8
NC = 18
NRAW = 8
EARLY = 4
FIRST_PARTS = 3
TAIL = 7
SPLIT = 15
DIAG_LAG = 6
LAG = 2
VROWS = 80
MESH = pl.DeviceIdType.MESH
F32 = jnp.float32
BF16 = jnp.bfloat16


def adam_update(grad_vals, param_vals, moment_one, moment_two, learn_rate, decay_rate):
    new_one = ADAM_BETA1 * moment_one + (1.0 - ADAM_BETA1) * grad_vals
    new_two = ADAM_BETA2 * moment_two + (1.0 - ADAM_BETA2) * grad_vals * grad_vals
    direction = (new_one / BIAS_ONE) / (jnp.sqrt(new_two / BIAS_TWO) + ADAM_EPS)
    return param_vals - learn_rate * (direction + decay_rate * param_vals), new_one, new_two


def flip(device, mask):
    for bit in (1, 2, 4):
        if mask & bit:
            device = device + bit - 2 * bit * lax.rem(lax.div(device, bit), 2)
    return device


def step_kernel(
    half, rc, n_vec,
    g_hbm, gv_hbm, p_hbm, m_hbm, v_hbm, pv_hbm, mv_hbm, vv_hbm, lr_hbm,
    state, big, px_hbm, py_hbm,
    fin, raw, pk, rel, acc, norms, vraw, vpk, vland, vs1, vlx, vs2, vly, vfull, lr_ref,
    raw_sem, send_sem, rel_sem, rs, st_sem, ns_sem, nr_sem, vs_sem, vr_sem, ag_sem, px_sem,
):
    piece_rows = 2 * half
    p_ref, m_ref, v_ref = (state.at[pl.ds(k * piece_rows, piece_rows)] for k in range(3))
    pv_out, mv_out, vv_out = (
        state.at[pl.ds(3 * piece_rows + k * 2 * VROWS, n_vec // LANES)] for k in range(3))
    me = lax.axis_index("dp")
    core = lax.rem(me, 2)
    peer = {mask: flip(me, mask) for mask in range(1, N_DEV)}

    def remote(src, dst, ssem, rsem, mask):
        return pltpu.make_async_remote_copy(
            src_ref=src, dst_ref=dst, send_sem=ssem, recv_sem=rsem,
            device_id=(peer[mask],), device_id_type=MESH,
        )

    def rows(first, count, align=16):
        return pl.ds(pl.multiple_of(first, align), count)

    blocks = []
    for j in (0, 1):
        for h in (0, 1):
            via = (4, 2)[h]
            blocks.append(("send", h, 6 ^ j, via ^ j, h * 3 + j))
    for h in (0, 1):
        blocks.append(("send", h, (2, 4)[h] ^ 1, 1, h * 3 + 2))
        blocks.append(("own", h, (2, 4)[h], None, 14 + h))
    for j in (0, 1):
        for h in (0, 1):
            via = (4, 2)[h]
            blocks.append(("send", h, via ^ j, via ^ j, 6 + h * 3 + j))
    for h in (0, 1):
        blocks.append(("send", h, 1, 1, 6 + h * 3 + 2))
        blocks.append(("own", h, 0, None, 12 + h))
    n_blocks = len(blocks)
    send_slot = {}
    for b, block in enumerate(blocks):
        if block[0] == "send":
            send_slot[b] = len(send_slot)

    def raw_copy(b, c):
        _, h, mask, _, _ = blocks[b]
        piece = flip(me, mask) if mask else me
        start = (piece * piece_rows + h * half + c * rc) * LANES
        return pltpu.make_async_copy(
            g_hbm.at[:, pl.ds(pl.multiple_of(start, 2048), rc * LANES)],
            raw.at[b % NRAW], raw_sem.at[b % NRAW],
        )

    def block_copy(b, c):
        _, h, _, dest, slot = blocks[b]
        s = send_slot[b]
        par = lax.rem(c, 2)
        return remote(
            pk.at[par, s], big.at[rows(slot * half + c * rc, rc)],
            send_sem.at[par, s], rs.at[slot, c], dest,
        )

    def landed(slot, c):
        ref = big.at[rows(slot * half + c * rc, rc)]
        return remote(ref, ref, send_sem.at[0, 0], rs.at[slot, c], 1)

    def rel_copy(h, c):
        par = lax.rem(c, 2)
        return remote(
            rel.at[par, h], fin.at[rows(h * half + c * rc, rc)],
            rel_sem.at[par, h], rs.at[12 + h, c], (2, 4)[h],
        )

    state_copies = [
        pltpu.make_async_copy(src, dst, st_sem.at[i])
        for i, (src, dst) in enumerate((
            (p_hbm, p_ref), (m_hbm, m_ref), (v_hbm, v_ref),
            (pv_hbm, pv_out), (mv_hbm, mv_out), (vv_hbm, vv_out), (lr_hbm, lr_ref)))
    ]
    vraw_copy = pltpu.make_async_copy(gv_hbm, vraw.at[:, pl.ds(0, n_vec)], st_sem.at[7])

    barrier = pltpu.get_barrier_semaphore()
    for mask in range(1, N_DEV):
        pl.semaphore_signal(barrier, inc=1, device_id=(peer[mask],), device_id_type=MESH)
    for b in range(NRAW):
        raw_copy(b, 0).start()
    vraw[:, pl.ds(n_vec // 1024 * 1024, 2 * VROWS * LANES - n_vec // 1024 * 1024)] = jnp.zeros(
        (1, 2 * VROWS * LANES - n_vec // 1024 * 1024), BF16)
    acc[...] = jnp.zeros_like(acc)
    step_rows = 64

    def pack_rows(src, dst, first):
        def body(i, _):
            vals = src[:, pl.ds(pl.multiple_of(i * step_rows * LANES, 2048), step_rows * LANES)]
            dst[rows(first + i * step_rows, step_rows), :] = (
                vals.astype(F32).reshape(step_rows, LANES).astype(BF16))
            return 0
        lax.fori_loop(0, rc // step_rows, body, 0, unroll=2)

    def load_block(b, c):
        kind, _, _, _, slot = blocks[b]
        raw_copy(b, c).wait()
        if kind == "send":
            @pl.when(c >= 2)
            def _():
                block_copy(b, c - 2).wait_send()
            pack_rows(raw.at[b % NRAW], pk.at[lax.rem(c, 2), send_slot[b]], 0)
        else:
            pack_rows(raw.at[b % NRAW], big, slot * half + c * rc)
        if b + NRAW < n_blocks:
            raw_copy(b + NRAW, c).start()
        else:
            @pl.when(c + 1 < NC)
            def _():
                raw_copy(b + NRAW - n_blocks, c + 1).start()

    for b in range(EARLY):
        load_block(b, 0)
    pl.semaphore_wait(barrier, N_DEV - 1)

    def send_chunk(c):
        waiting = None
        for b, (kind, h, mask, dest, slot) in enumerate(blocks):
            if b < EARLY:
                @pl.when(c >= 1)
                def _():
                    load_block(b, c)
            else:
                load_block(b, c)
            if waiting is not None:
                block_copy(waiting, c).start()
            waiting = b if kind == "send" else None
        if waiting is not None:
            block_copy(waiting, c).start()

    sum_rows = 32

    def relay_chunk(c):
        par = lax.rem(c, 2)
        for h in (0, 1):
            for j in range(3):
                landed(h * 3 + j, c).wait_recv()

            @pl.when(c >= 2)
            def _():
                rel_copy(h, c - 2).wait_send()

            def body(i, _):
                at = c * rc + i * sum_rows
                total = big[rows((14 + h) * half + at, sum_rows), :].astype(F32)
                for j in (2, 0, 1):
                    total = total + big[rows((h * 3 + j) * half + at, sum_rows), :].astype(F32)
                rel[par, h, rows(i * sum_rows, sum_rows), :] = total
                return 0
            lax.fori_loop(0, rc // sum_rows, body, 0)
        for h in (0, 1):
            rel_copy(h, c).start()

    def final_chunk(c):
        for h in (0, 1):
            for j in range(3):
                landed(6 + h * 3 + j, c).wait_recv()
            rel_copy(h, c).wait_recv()

            def body(i, sq):
                at = c * rc + i * sum_rows
                total = big[rows((12 + h) * half + at, sum_rows), :].astype(F32)
                for j in (2, 0, 1):
                    total = total + big[rows((6 + h * 3 + j) * half + at, sum_rows), :].astype(F32)
                total = (total + fin[rows(h * half + at, sum_rows), :]) * (1.0 / N_DEV)
                fin[rows(h * half + at, sum_rows), :] = total
                total = total * total
                for k in range(sum_rows // 8):
                    sq = sq + total[8 * k:8 * k + 8]
                return sq
            acc[...] = lax.fori_loop(0, rc // sum_rows, body, acc[...], unroll=4)

    mine = rows(core * VROWS, VROWS)
    other = rows((1 - core) * VROWS, VROWS)
    vec_core = remote(vpk.at[other], vland, vs_sem.at[0], vr_sem.at[0], 1)
    vec_x = remote(vs1, vlx, vs_sem.at[1], vr_sem.at[1], 2)
    vec_y = remote(vs2, vly, vs_sem.at[2], vr_sem.at[2], 4)
    vec_back = remote(vfull.at[mine], vfull.at[mine], vs_sem.at[3], vr_sem.at[3], 1)
    vec_back_in = remote(vfull.at[other], vfull.at[other], vs_sem.at[3], vr_sem.at[3], 1)

    def vec_step(c):
        @pl.when(c == 1)
        def _():
            vraw_copy.wait()
            vpk[...] = vraw[...].astype(F32).reshape(2 * VROWS, LANES).astype(BF16)

        @pl.when(c == 2)
        def _():
            vec_core.start()

        @pl.when(c == 3)
        def _():
            vec_core.wait_recv()
            vs1[...] = vpk[mine, :].astype(F32) + vland[...].astype(F32)

        @pl.when(c == 4)
        def _():
            vec_x.start()

        @pl.when(c == 6)
        def _():
            vec_x.wait_recv()
            vs2[...] = vs1[...] + vlx[...]

        @pl.when(c == 7)
        def _():
            vec_y.start()

        @pl.when(c == 9)
        def _():
            vec_y.wait_recv()
            vfull[mine, :] = (vs2[...] + vly[...]) * (1.0 / N_DEV)

        @pl.when(c == 10)
        def _():
            vec_back.start()

        @pl.when(c == 12)
        def _():
            vec_back_in.wait_recv()
            vec_core.wait_send()
            vec_x.wait_send()
            vec_y.wait_send()
            vec_back.wait_send()

    def scatter_step(c, _):
        @pl.when(c < NC)
        def _():
            send_chunk(c)

        @pl.when(c == 0)
        def _():
            vraw_copy.start()

        @pl.when(c == 3)
        def _():
            for copy in state_copies:
                copy.start()

        vec_step(c)

        @pl.when((c >= 1) & (c < NC + 1))
        def _():
            relay_chunk(c - 1)

        @pl.when(c >= 2)
        def _():
            final_chunk(c - 2)
        return 0

    lax.fori_loop(0, NC + 2, scatter_step, 0)

    norms[me] = acc[...]
    vec_sq = jnp.sum(vfull[...] * vfull[...], keepdims=True)
    for copy in state_copies:
        copy.wait()

    def norm_copy(mask):
        return remote(norms.at[me], norms.at[me], ns_sem.at[mask - 1], nr_sem.at[mask - 1], mask)

    for mask in (6, 7, 2, 4, 3, 5, 1):
        norm_copy(mask).start()
    for c in (NC - 2, NC - 1):
        for b in send_slot:
            block_copy(b, c).wait_send()
        for h in (0, 1):
            rel_copy(h, c).wait_send()
    for mask in range(1, N_DEV):
        norm_copy(mask).wait_recv()
    total = norms[0]
    for k in range(1, N_DEV):
        total = total + norms[k]
    norm_sq = jnp.sum(total, keepdims=True) + vec_sq
    clip = jnp.minimum(1.0, MAX_NORM / (jnp.sqrt(norm_sq) + NORM_EPS))
    lr = lr_ref[...]

    upd_rows = 32
    clip_rows = jnp.broadcast_to(clip, (upd_rows, LANES))
    lr_rows = jnp.broadcast_to(lr, (upd_rows, LANES))

    def update_chunk(h, c, first=0, count=rc):
        def body(i, _):
            at = h * half + c * rc + first + i * upd_rows
            here = rows(at, upd_rows)
            new_p, new_m, new_v = adam_update(
                fin[here, :] * clip_rows, p_ref[here, :], m_ref[here, :], v_ref[here, :], lr_rows, WEIGHT_DECAY)
            p_ref[here, :] = new_p
            m_ref[here, :] = new_m
            v_ref[here, :] = new_v
            big[rows(me * piece_rows + at, upd_rows), :] = new_p.astype(BF16)
            return 0
        lax.fori_loop(0, count // upd_rows, body, 0, unroll=4)

    def gather_copy(mask, h, c, dest, ssem, slot):
        piece = flip(me, mask) if mask else me
        ref = big.at[rows(piece * piece_rows + h * half + c * rc, rc)]
        return remote(ref, ref, ag_sem.at[ssem], rs.at[slot, c], dest)

    def own_x(h, c):
        return gather_copy(0, h, c, 2, 0, h)

    def own_y(h, c):
        return gather_copy(0, h, c, 4, 1, 2 + h)

    def own_core(h, c):
        return gather_copy(0, h, c, 1, 2, 6 + h)

    def arrived(mask, h, c, slot):
        gather_copy(mask, h, c, 1, 0, slot).wait_recv()

    def to_core(mask, h, c):
        return gather_copy(mask, h, c, 1, {2: 5, 4: 6, 6: 7}[mask], {2: 8, 4: 10, 6: 12}[mask] + h)

    def diagonal(j):
        arrived(6, 0, j, 4)
        to_core(6, 0, j).start()
        arrived(6, 1, j, 5)
        to_core(6, 1, j).start()

    def first_half(i, _):
        @pl.when(i < NC)
        def _():
            @pl.when(i > 0)
            def _():
                update_chunk(0, i)
                own_x(0, i).start()
                update_chunk(1, i)
                own_y(1, i).start()
            own_core(0, i).start()
            own_core(1, i).start()

        @pl.when(i >= LAG)
        def _():
            j = i - LAG
            arrived(2, 0, j, 0)
            gather_copy(2, 0, j, 4, 3, 4).start()
            to_core(2, 0, j).start()
            arrived(4, 1, j, 3)
            gather_copy(4, 1, j, 2, 4, 5).start()
            to_core(4, 1, j).start()

        @pl.when(i >= DIAG_LAG)
        def _():
            diagonal(i - DIAG_LAG)

        @pl.when(i >= NC)
        def _():
            own_x(1, i - NC).start()
            own_y(0, i - NC).start()
        return 0

    for k in range(FIRST_PARTS):
        part = rc // FIRST_PARTS
        for h, dest, ssem in ((0, 2, 0), (1, 4, 1)):
            update_chunk(h, 0, k * part, part)
            ref = big.at[rows(me * piece_rows + h * half + k * part, part)]
            remote(ref, ref, ag_sem.at[ssem], rs.at[3 * h, 0], dest).start()
    lax.fori_loop(0, NC + LAG, first_half, 0)

    kept = half - TAIL * rc
    tail_copies = [
        pltpu.make_async_copy(
            big.at[rows(me * piece_rows + h * half + kept, TAIL * rc)], dst, px_sem.at[h])
        for h, dst in ((1, px_hbm), (0, py_hbm))
    ]
    for copy in tail_copies:
        copy.start()

    vrows = n_vec // LANES
    new_p, new_m, new_v = adam_update(
        vfull[pl.ds(0, vrows), :] * clip, pv_out[...], mv_out[...], vv_out[...], lr, 0.0)
    pv_out[...] = new_p
    mv_out[...] = new_m
    vv_out[...] = new_v

    def second_half(j, _):
        @pl.when(j + LAG < NC - TAIL)
        def _():
            own_x(1, j + LAG).start()
            own_y(0, j + LAG).start()
        @pl.when(j < DIAG_LAG - LAG)
        def _():
            diagonal(NC + LAG - DIAG_LAG + j)
        arrived(2, 1, j, 1)
        to_core(2, 1, j).start()
        arrived(4, 0, j, 2)
        to_core(4, 0, j).start()
        return 0

    lax.fori_loop(0, NC - TAIL, second_half, 0)

    def last_arrivals(c, _):
        for mask, h in ((1, 0), (1, 1), (3, 0), (5, 1), (7, 0), (7, 1)):
            arrived(mask, h, c, 5 + mask + h)

        @pl.when(c < NC - TAIL)
        def _():
            for mask, h in ((3, 1), (5, 0)):
                arrived(mask, h, c, 5 + mask + h)
        return 0

    lax.fori_loop(0, NC, last_arrivals, 0)
    for ssem, count in (
        (0, half + kept), (1, half + kept), (2, 2 * half), (3, half), (4, half),
        (5, half + kept), (6, half + kept), (7, 2 * half),
    ):
        ref = big.at[pl.ds(0, count)]
        remote(ref, ref, ag_sem.at[ssem], rs.at[0, 0], 1).wait_send()
    for mask in range(1, N_DEV):
        norm_copy(mask).wait_send()
    for copy in tail_copies:
        copy.wait()


def run_all(copies):
    for copy in copies:
        copy.start()
    for copy in copies:
        copy.wait()


def first_write(half, state, big, *refs):
    dsts, sem = refs[:-1], refs[-1]
    copies = []

    def add(src, src_at, dst, count, size):
        part = size // count
        for k in range(count):
            copies.append(pltpu.make_async_copy(
                src.at[pl.ds(src_at + k * part, part)], dst.at[pl.ds(k * part, part)], sem.at[len(copies)]))

    at = 0
    for dst in dsts[:6]:
        size = dst.shape[0]
        add(state, at, dst, 4 if size > 2 * VROWS else 1, size)
        at += max(size, 2 * VROWS)
    add(big, 0, dsts[6], SPLIT, SPLIT * half)
    run_all(copies)


def tail_copies_of(half, parts, dst, sem):
    me = lax.axis_index("dp")
    copies = []
    for i, (src, mask, h) in enumerate(parts):
        tail = src.shape[0]
        at = flip(me, mask) * (2 * half) + (h + 1) * half - tail
        copies.append(pltpu.make_async_copy(src, dst.at[pl.ds(pl.multiple_of(at, 16), tail)], sem.at[i]))
    return copies


def second_write(half, big, rx, ry, _, dst, sem):
    run_all([
        pltpu.make_async_copy(big.at[pl.ds(k * half, half)], dst.at[pl.ds(k * half, half)], sem.at[2 + k - SPLIT])
        for k in range(SPLIT, 2 * N_DEV)
    ])
    run_all(tail_copies_of(half, ((rx, 2, 1), (ry, 4, 0)), dst, sem))


def third_write(half, cx, cy, _, dst, sem):
    run_all(tail_copies_of(half, ((cx, 3, 1), (cy, 5, 0)), dst, sem))


def solution(mesh):
    axis_name = mesh.axis_names[0]

    def local_step(g_mat, g_vec, p_mat, m_mat, v_mat, p_vec, m_vec, v_vec, learn_rate):
        n_piece = p_mat.shape[0]
        n_vec = p_vec.shape[0]
        piece_rows = n_piece // LANES
        half = piece_rows // 2
        rc = half // NC
        state = (piece_rows, LANES)
        vec = (n_vec // LANES, LANES)
        full = (N_DEV * piece_rows, LANES)
        any_spec = pl.BlockSpec(memory_space=pl.ANY)
        vmem_spec = pl.BlockSpec(memory_space=pltpu.VMEM)
        state_new, big, px, py = pl.pallas_call(
            functools.partial(step_kernel, half, rc, n_vec),
            out_shape=[pltpu.VMEM((3 * piece_rows + 6 * VROWS, LANES), F32), pltpu.VMEM(full, BF16)]
            + [jax.ShapeDtypeStruct((TAIL * rc, LANES), BF16)] * 2,
            in_specs=[any_spec] * 9,
            out_specs=[vmem_spec] * 2 + [any_spec] * 2,
            scratch_shapes=[
                pltpu.VMEM(state, F32),
                pltpu.VMEM((NRAW, 1, rc * LANES), BF16),
                pltpu.VMEM((2, 12, rc, LANES), BF16),
                pltpu.VMEM((2, 2, rc, LANES), F32),
                pltpu.VMEM((8, LANES), F32),
                pltpu.VMEM((N_DEV, 8, LANES), F32),
                pltpu.VMEM((1, 2 * VROWS * LANES), BF16),
                pltpu.VMEM((2 * VROWS, LANES), BF16),
                pltpu.VMEM((VROWS, LANES), BF16),
                pltpu.VMEM((VROWS, LANES), F32),
                pltpu.VMEM((VROWS, LANES), F32),
                pltpu.VMEM((VROWS, LANES), F32),
                pltpu.VMEM((VROWS, LANES), F32),
                pltpu.VMEM((2 * VROWS, LANES), F32),
                pltpu.VMEM((1, 1), F32),
                pltpu.SemaphoreType.DMA((NRAW,)),
                pltpu.SemaphoreType.DMA((2, 12)),
                pltpu.SemaphoreType.DMA((2, 2)),
                pltpu.SemaphoreType.DMA((14, NC)),
                pltpu.SemaphoreType.DMA((8,)),
                pltpu.SemaphoreType.DMA((7,)),
                pltpu.SemaphoreType.DMA((7,)),
                pltpu.SemaphoreType.DMA((4,)),
                pltpu.SemaphoreType.DMA((4,)),
                pltpu.SemaphoreType.DMA((8,)),
                pltpu.SemaphoreType.DMA((2,)),
            ],
            compiler_params=pltpu.CompilerParams(
                collective_id=0, has_side_effects=True, vmem_limit_bytes=15 * 2 ** 20),
            name="step",
        )(
            g_mat, g_vec, p_mat.reshape(state), m_mat.reshape(state), v_mat.reshape(state),
            p_vec.reshape(vec), m_vec.reshape(vec), v_vec.reshape(vec), learn_rate.reshape(1, 1),
        )
        def permute(values, mask):
            return lax.ppermute(values, axis_name, [(d, d ^ mask) for d in range(N_DEV)])

        def cost(n_bytes):
            return pl.CostEstimate(flops=0, bytes_accessed=n_bytes, transcendentals=0)

        rx, ry = permute(px, 2), permute(py, 4)
        p_new, m_new, v_new, pv_new, mv_new, vv_new, pb = pl.pallas_call(
            functools.partial(first_write, half),
            out_shape=[jax.ShapeDtypeStruct(state, F32)] * 3 + [jax.ShapeDtypeStruct(vec, F32)] * 3
            + [jax.ShapeDtypeStruct(full, BF16)],
            in_specs=[vmem_spec] * 2,
            out_specs=[any_spec] * 7,
            scratch_shapes=[pltpu.SemaphoreType.DMA((15 + SPLIT,))],
            cost_estimate=cost(12 * n_piece + SPLIT * n_piece),
            compiler_params=pltpu.CompilerParams(vmem_limit_bytes=2 ** 20),
            name="write1",
        )(state_new, big)
        rx, ry, p_new = lax.optimization_barrier((rx, ry, p_new))
        cx, cy = permute(rx, 1), permute(ry, 1)
        pb = pl.pallas_call(
            functools.partial(second_write, half),
            out_shape=jax.ShapeDtypeStruct(full, BF16),
            in_specs=[vmem_spec] * 3 + [any_spec],
            out_specs=any_spec,
            input_output_aliases={3: 0},
            scratch_shapes=[pltpu.SemaphoreType.DMA((2 + 2 * N_DEV - SPLIT,))],
            cost_estimate=cost((2 * N_DEV - SPLIT) * n_piece),
            compiler_params=pltpu.CompilerParams(vmem_limit_bytes=2 * 2 ** 20),
            name="write2",
        )(big, rx, ry, pb)
        pb = pl.pallas_call(
            functools.partial(third_write, half),
            out_shape=jax.ShapeDtypeStruct(full, BF16),
            in_specs=[vmem_spec] * 2 + [any_spec],
            out_specs=any_spec,
            input_output_aliases={2: 0},
            scratch_shapes=[pltpu.SemaphoreType.DMA((2,))],
            compiler_params=pltpu.CompilerParams(vmem_limit_bytes=2 * 2 ** 20),
            name="write3",
        )(cx, cy, pb)
        return (
            p_new.reshape(-1), m_new.reshape(-1), v_new.reshape(-1),
            pv_new.reshape(-1), mv_new.reshape(-1), vv_new.reshape(-1), pb.reshape(-1),
        )

    return jax.shard_map(
        local_step,
        mesh=mesh,
        in_specs=(P(axis_name, None), P(axis_name, None), P(axis_name), P(axis_name), P(axis_name), P(), P(), P(), P()),
        out_specs=(P(axis_name), P(axis_name), P(axis_name), P(), P(), P(), P()),
        check_vma=False,
    )
```

```python
import functools

import jax
import jax.numpy as jnp
from jax import lax
from jax.experimental import pallas as pl
from jax.experimental.pallas import tpu as pltpu
from jax.sharding import PartitionSpec as P

STEP = 10
ADAM_BETA1 = 0.9
ADAM_BETA2 = 0.98
ADAM_EPS = 1e-8
WEIGHT_DECAY = 0.01
MAX_NORM = 1.0
NORM_EPS = 1e-6
BIAS_ONE = 1.0 - ADAM_BETA1 ** STEP
BIAS_TWO = 1.0 - ADAM_BETA2 ** STEP

LANES = 128
N_DEV = 8
NC = 12
NRAW = 8
EARLY = 4
FIRST_PARTS = 6
TAIL = 5
SPLIT = 15
DIAG_LAG = 4
LAG = 2
VROWS = 80
MESH = pl.DeviceIdType.MESH
F32 = jnp.float32
BF16 = jnp.bfloat16


def adam_update(grad_vals, param_vals, moment_one, moment_two, learn_rate, decay_rate):
    new_one = ADAM_BETA1 * moment_one + (1.0 - ADAM_BETA1) * grad_vals
    new_two = ADAM_BETA2 * moment_two + (1.0 - ADAM_BETA2) * grad_vals * grad_vals
    direction = (new_one / BIAS_ONE) / (jnp.sqrt(new_two / BIAS_TWO) + ADAM_EPS)
    return param_vals - learn_rate * (direction + decay_rate * param_vals), new_one, new_two


def flip(device, mask):
    for bit in (1, 2, 4):
        if mask & bit:
            device = device + bit - 2 * bit * lax.rem(lax.div(device, bit), 2)
    return device


def step_kernel(
    half, rc, n_vec,
    g_hbm, gv_hbm, p_hbm, m_hbm, v_hbm, pv_hbm, mv_hbm, vv_hbm, lr_hbm,
    state, big, px_hbm, py_hbm,
    fin, raw, pk, rel, acc, norms, vraw, vpk, vland, vs1, vlx, vs2, vly, vfull, lr_ref,
    raw_sem, send_sem, rel_sem, rs, st_sem, ns_sem, nr_sem, vs_sem, vr_sem, ag_sem, px_sem,
):
    piece_rows = 2 * half
    p_ref, m_ref, v_ref = (state.at[pl.ds(k * piece_rows, piece_rows)] for k in range(3))
    pv_out, mv_out, vv_out = (
        state.at[pl.ds(3 * piece_rows + k * 2 * VROWS, n_vec // LANES)] for k in range(3))
    me = lax.axis_index("dp")
    core = lax.rem(me, 2)
    peer = {mask: flip(me, mask) for mask in range(1, N_DEV)}

    def remote(src, dst, ssem, rsem, mask):
        return pltpu.make_async_remote_copy(
            src_ref=src, dst_ref=dst, send_sem=ssem, recv_sem=rsem,
            device_id=(peer[mask],), device_id_type=MESH,
        )

    def rows(first, count, align=16):
        return pl.ds(pl.multiple_of(first, align), count)

    blocks = []
    for j in (0, 1):
        for h in (0, 1):
            via = (4, 2)[h]
            blocks.append(("send", h, 6 ^ j, via ^ j, h * 3 + j))
    for h in (0, 1):
        blocks.append(("send", h, (2, 4)[h] ^ 1, 1, h * 3 + 2))
        blocks.append(("own", h, (2, 4)[h], None, 14 + h))
    for j in (0, 1):
        for h in (0, 1):
            via = (4, 2)[h]
            blocks.append(("send", h, via ^ j, via ^ j, 6 + h * 3 + j))
    for h in (0, 1):
        blocks.append(("send", h, 1, 1, 6 + h * 3 + 2))
        blocks.append(("own", h, 0, None, 12 + h))
    n_blocks = len(blocks)
    send_slot = {}
    for b, block in enumerate(blocks):
        if block[0] == "send":
            send_slot[b] = len(send_slot)

    def raw_copy(b, c):
        _, h, mask, _, _ = blocks[b]
        piece = flip(me, mask) if mask else me
        start = (piece * piece_rows + h * half + c * rc) * LANES
        return pltpu.make_async_copy(
            g_hbm.at[:, pl.ds(pl.multiple_of(start, 2048), rc * LANES)],
            raw.at[b % NRAW], raw_sem.at[b % NRAW],
        )

    def block_copy(b, c):
        _, h, _, dest, slot = blocks[b]
        s = send_slot[b]
        par = lax.rem(c, 2)
        return remote(
            pk.at[par, s], big.at[rows(slot * half + c * rc, rc)],
            send_sem.at[par, s], rs.at[slot, c], dest,
        )

    def landed(slot, c):
        ref = big.at[rows(slot * half + c * rc, rc)]
        return remote(ref, ref, send_sem.at[0, 0], rs.at[slot, c], 1)

    def rel_copy(h, c):
        par = lax.rem(c, 2)
        return remote(
            rel.at[par, h], fin.at[rows(h * half + c * rc, rc)],
            rel_sem.at[par, h], rs.at[12 + h, c], (2, 4)[h],
        )

    state_copies = [
        pltpu.make_async_copy(src, dst, st_sem.at[i])
        for i, (src, dst) in enumerate((
            (p_hbm, p_ref), (m_hbm, m_ref), (v_hbm, v_ref),
            (pv_hbm, pv_out), (mv_hbm, mv_out), (vv_hbm, vv_out), (lr_hbm, lr_ref)))
    ]
    vraw_copy = pltpu.make_async_copy(gv_hbm, vraw.at[:, pl.ds(0, n_vec)], st_sem.at[7])

    barrier = pltpu.get_barrier_semaphore()
    for mask in range(1, N_DEV):
        pl.semaphore_signal(barrier, inc=1, device_id=(peer[mask],), device_id_type=MESH)
    for b in range(NRAW):
        raw_copy(b, 0).start()
    vraw[:, pl.ds(n_vec // 1024 * 1024, 2 * VROWS * LANES - n_vec // 1024 * 1024)] = jnp.zeros(
        (1, 2 * VROWS * LANES - n_vec // 1024 * 1024), BF16)
    acc[...] = jnp.zeros_like(acc)
    step_rows = 64

    def pack_rows(src, dst, first):
        def body(i, _):
            vals = src[:, pl.ds(pl.multiple_of(i * step_rows * LANES, 2048), step_rows * LANES)]
            dst[rows(first + i * step_rows, step_rows), :] = (
                vals.astype(F32).reshape(step_rows, LANES).astype(BF16))
            return 0
        lax.fori_loop(0, rc // step_rows, body, 0, unroll=2)

    def load_block(b, c):
        kind, _, _, _, slot = blocks[b]
        raw_copy(b, c).wait()
        if kind == "send":
            @pl.when(c >= 2)
            def _():
                block_copy(b, c - 2).wait_send()
            pack_rows(raw.at[b % NRAW], pk.at[lax.rem(c, 2), send_slot[b]], 0)
        else:
            pack_rows(raw.at[b % NRAW], big, slot * half + c * rc)
        if b + NRAW < n_blocks:
            raw_copy(b + NRAW, c).start()
        else:
            @pl.when(c + 1 < NC)
            def _():
                raw_copy(b + NRAW - n_blocks, c + 1).start()

    for b in range(EARLY):
        load_block(b, 0)
    pl.semaphore_wait(barrier, N_DEV - 1)

    def send_chunk(c):
        waiting = None
        for b, (kind, h, mask, dest, slot) in enumerate(blocks):
            if b < EARLY:
                @pl.when(c >= 1)
                def _():
                    load_block(b, c)
            else:
                load_block(b, c)
            if waiting is not None:
                block_copy(waiting, c).start()
            waiting = b if kind == "send" else None
        if waiting is not None:
            block_copy(waiting, c).start()

    sum_rows = 32

    def relay_chunk(c):
        par = lax.rem(c, 2)
        for h in (0, 1):
            for j in range(3):
                landed(h * 3 + j, c).wait_recv()

            @pl.when(c >= 2)
            def _():
                rel_copy(h, c - 2).wait_send()

            def body(i, _):
                at = c * rc + i * sum_rows
                total = big[rows((14 + h) * half + at, sum_rows), :].astype(F32)
                for j in (2, 0, 1):
                    total = total + big[rows((h * 3 + j) * half + at, sum_rows), :].astype(F32)
                rel[par, h, rows(i * sum_rows, sum_rows), :] = total
                return 0
            lax.fori_loop(0, rc // sum_rows, body, 0, unroll=3)
        for h in (0, 1):
            rel_copy(h, c).start()

    def final_chunk(c):
        for h in (0, 1):
            for j in range(3):
                landed(6 + h * 3 + j, c).wait_recv()
            rel_copy(h, c).wait_recv()

            def body(i, sq):
                at = c * rc + i * sum_rows
                total = big[rows((12 + h) * half + at, sum_rows), :].astype(F32)
                for j in (2, 0, 1):
                    total = total + big[rows((6 + h * 3 + j) * half + at, sum_rows), :].astype(F32)
                total = (total + fin[rows(h * half + at, sum_rows), :]) * (1.0 / N_DEV)
                fin[rows(h * half + at, sum_rows), :] = total
                total = total * total
                for k in range(sum_rows // 8):
                    sq = sq + total[8 * k:8 * k + 8]
                return sq
            acc[...] = lax.fori_loop(0, rc // sum_rows, body, acc[...], unroll=6)

    mine = rows(core * VROWS, VROWS)
    other = rows((1 - core) * VROWS, VROWS)
    vec_core = remote(vpk.at[other], vland, vs_sem.at[0], vr_sem.at[0], 1)
    vec_x = remote(vs1, vlx, vs_sem.at[1], vr_sem.at[1], 2)
    vec_y = remote(vs2, vly, vs_sem.at[2], vr_sem.at[2], 4)
    vec_back = remote(vfull.at[mine], vfull.at[mine], vs_sem.at[3], vr_sem.at[3], 1)
    vec_back_in = remote(vfull.at[other], vfull.at[other], vs_sem.at[3], vr_sem.at[3], 1)

    def vec_step(c):
        @pl.when(c == 1)
        def _():
            vraw_copy.wait()
            vpk[...] = vraw[...].astype(F32).reshape(2 * VROWS, LANES).astype(BF16)

        @pl.when(c == 2)
        def _():
            vec_core.start()

        @pl.when(c == 3)
        def _():
            vec_core.wait_recv()
            vs1[...] = vpk[mine, :].astype(F32) + vland[...].astype(F32)

        @pl.when(c == 4)
        def _():
            vec_x.start()

        @pl.when(c == 6)
        def _():
            vec_x.wait_recv()
            vs2[...] = vs1[...] + vlx[...]

        @pl.when(c == 7)
        def _():
            vec_y.start()

        @pl.when(c == 9)
        def _():
            vec_y.wait_recv()
            vfull[mine, :] = (vs2[...] + vly[...]) * (1.0 / N_DEV)

        @pl.when(c == 10)
        def _():
            vec_back.start()

        @pl.when(c == 12)
        def _():
            vec_back_in.wait_recv()
            vec_core.wait_send()
            vec_x.wait_send()
            vec_y.wait_send()
            vec_back.wait_send()

    def scatter_step(c, _):
        @pl.when(c < NC)
        def _():
            send_chunk(c)

        @pl.when(c == 0)
        def _():
            vraw_copy.start()

        @pl.when(c == 3)
        def _():
            for copy in state_copies:
                copy.start()

        vec_step(c)

        @pl.when((c >= 1) & (c < NC + 1))
        def _():
            relay_chunk(c - 1)

        @pl.when(c >= 2)
        def _():
            final_chunk(c - 2)
        return 0

    lax.fori_loop(0, NC + 2, scatter_step, 0)

    norms[me] = acc[...]
    vec_sq = jnp.sum(vfull[...] * vfull[...], keepdims=True)
    for copy in state_copies:
        copy.wait()

    def norm_copy(mask):
        return remote(norms.at[me], norms.at[me], ns_sem.at[mask - 1], nr_sem.at[mask - 1], mask)

    for mask in (6, 7, 2, 4, 3, 5, 1):
        norm_copy(mask).start()
    for c in (NC - 2, NC - 1):
        for b in send_slot:
            block_copy(b, c).wait_send()
        for h in (0, 1):
            rel_copy(h, c).wait_send()
    for mask in range(1, N_DEV):
        norm_copy(mask).wait_recv()
    total = norms[0]
    for k in range(1, N_DEV):
        total = total + norms[k]
    norm_sq = jnp.sum(total, keepdims=True) + vec_sq
    clip = jnp.minimum(1.0, MAX_NORM / (jnp.sqrt(norm_sq) + NORM_EPS))
    lr = lr_ref[...]

    upd_rows = 32
    clip_rows = jnp.broadcast_to(clip, (upd_rows, LANES))
    lr_rows = jnp.broadcast_to(lr, (upd_rows, LANES))

    def update_chunk(h, c, first=0, count=rc):
        def body(i, _):
            at = h * half + c * rc + first + i * upd_rows
            here = rows(at, upd_rows)
            new_p, new_m, new_v = adam_update(
                fin[here, :] * clip_rows, p_ref[here, :], m_ref[here, :], v_ref[here, :], lr_rows, WEIGHT_DECAY)
            p_ref[here, :] = new_p
            m_ref[here, :] = new_m
            v_ref[here, :] = new_v
            big[rows(me * piece_rows + at, upd_rows), :] = new_p.astype(BF16)
            return 0
        lax.fori_loop(0, count // upd_rows, body, 0, unroll=3)

    def gather_copy(mask, h, c, dest, ssem, slot):
        piece = flip(me, mask) if mask else me
        ref = big.at[rows(piece * piece_rows + h * half + c * rc, rc)]
        return remote(ref, ref, ag_sem.at[ssem], rs.at[slot, c], dest)

    def own_x(h, c):
        return gather_copy(0, h, c, 2, 0, h)

    def own_y(h, c):
        return gather_copy(0, h, c, 4, 1, 2 + h)

    def own_core(h, c):
        return gather_copy(0, h, c, 1, 2, 6 + h)

    def arrived(mask, h, c, slot):
        gather_copy(mask, h, c, 1, 0, slot).wait_recv()

    def to_core(mask, h, c):
        return gather_copy(mask, h, c, 1, {2: 5, 4: 6, 6: 7}[mask], {2: 8, 4: 10, 6: 12}[mask] + h)

    def diagonal(j):
        arrived(6, 0, j, 4)
        to_core(6, 0, j).start()
        arrived(6, 1, j, 5)
        to_core(6, 1, j).start()

    def first_half(i, _):
        @pl.when(i < NC)
        def _():
            @pl.when(i > 0)
            def _():
                update_chunk(0, i)
                own_x(0, i).start()
                update_chunk(1, i)
                own_y(1, i).start()
            own_core(0, i).start()
            own_core(1, i).start()

        @pl.when(i >= LAG)
        def _():
            j = i - LAG
            arrived(2, 0, j, 0)
            gather_copy(2, 0, j, 4, 3, 4).start()
            to_core(2, 0, j).start()
            arrived(4, 1, j, 3)
            gather_copy(4, 1, j, 2, 4, 5).start()
            to_core(4, 1, j).start()

        @pl.when(i >= DIAG_LAG)
        def _():
            diagonal(i - DIAG_LAG)

        @pl.when(i >= NC)
        def _():
            own_x(1, i - NC).start()
            own_y(0, i - NC).start()
        return 0

    for k in range(FIRST_PARTS):
        part = rc // FIRST_PARTS
        for h, dest, ssem in ((0, 2, 0), (1, 4, 1)):
            update_chunk(h, 0, k * part, part)
            ref = big.at[rows(me * piece_rows + h * half + k * part, part)]
            remote(ref, ref, ag_sem.at[ssem], rs.at[3 * h, 0], dest).start()
    lax.fori_loop(0, NC + LAG, first_half, 0)

    kept = half - TAIL * rc
    tail_copies = [
        pltpu.make_async_copy(
            big.at[rows(me * piece_rows + h * half + kept, TAIL * rc)], dst, px_sem.at[h])
        for h, dst in ((1, px_hbm), (0, py_hbm))
    ]
    for copy in tail_copies:
        copy.start()

    vrows = n_vec // LANES
    new_p, new_m, new_v = adam_update(
        vfull[pl.ds(0, vrows), :] * clip, pv_out[...], mv_out[...], vv_out[...], lr, 0.0)
    pv_out[...] = new_p
    mv_out[...] = new_m
    vv_out[...] = new_v

    def second_half(j, _):
        @pl.when(j + LAG < NC - TAIL)
        def _():
            own_x(1, j + LAG).start()
            own_y(0, j + LAG).start()
        @pl.when(j < DIAG_LAG - LAG)
        def _():
            diagonal(NC + LAG - DIAG_LAG + j)
        arrived(2, 1, j, 1)
        to_core(2, 1, j).start()
        arrived(4, 0, j, 2)
        to_core(4, 0, j).start()
        return 0

    lax.fori_loop(0, NC - TAIL, second_half, 0)

    def last_arrivals(c, _):
        for mask, h in ((1, 0), (1, 1), (3, 0), (5, 1), (7, 0), (7, 1)):
            arrived(mask, h, c, 5 + mask + h)

        @pl.when(c < NC - TAIL)
        def _():
            for mask, h in ((3, 1), (5, 0)):
                arrived(mask, h, c, 5 + mask + h)
        return 0

    lax.fori_loop(0, NC, last_arrivals, 0)
    for ssem, count in (
        (0, half + kept), (1, half + kept), (2, 2 * half), (3, half), (4, half),
        (5, half + kept), (6, half + kept), (7, 2 * half),
    ):
        ref = big.at[pl.ds(0, count)]
        remote(ref, ref, ag_sem.at[ssem], rs.at[0, 0], 1).wait_send()
    for mask in range(1, N_DEV):
        norm_copy(mask).wait_send()
    for copy in tail_copies:
        copy.wait()


def run_all(copies):
    for copy in copies:
        copy.start()
    for copy in copies:
        copy.wait()


def first_write(half, state, big, *refs):
    dsts, sem = refs[:-1], refs[-1]
    copies = []

    def add(src, src_at, dst, count, size):
        part = size // count
        for k in range(count):
            copies.append(pltpu.make_async_copy(
                src.at[pl.ds(src_at + k * part, part)], dst.at[pl.ds(k * part, part)], sem.at[len(copies)]))

    at = 0
    for dst in dsts[:6]:
        size = dst.shape[0]
        add(state, at, dst, 4 if size > 2 * VROWS else 1, size)
        at += max(size, 2 * VROWS)
    add(big, 0, dsts[6], SPLIT, SPLIT * half)
    run_all(copies)


def tail_copies_of(half, parts, dst, sem):
    me = lax.axis_index("dp")
    copies = []
    for i, (src, mask, h) in enumerate(parts):
        tail = src.shape[0]
        at = flip(me, mask) * (2 * half) + (h + 1) * half - tail
        copies.append(pltpu.make_async_copy(src, dst.at[pl.ds(pl.multiple_of(at, 16), tail)], sem.at[i]))
    return copies


def second_write(half, big, rx, ry, _, dst, sem):
    run_all([
        pltpu.make_async_copy(big.at[pl.ds(k * half, half)], dst.at[pl.ds(k * half, half)], sem.at[2 + k - SPLIT])
        for k in range(SPLIT, 2 * N_DEV)
    ])
    run_all(tail_copies_of(half, ((rx, 2, 1), (ry, 4, 0)), dst, sem))


def third_write(half, cx, cy, _, dst, sem):
    run_all(tail_copies_of(half, ((cx, 3, 1), (cy, 5, 0)), dst, sem))


def solution(mesh):
    axis_name = mesh.axis_names[0]

    def local_step(g_mat, g_vec, p_mat, m_mat, v_mat, p_vec, m_vec, v_vec, learn_rate):
        n_piece = p_mat.shape[0]
        n_vec = p_vec.shape[0]
        piece_rows = n_piece // LANES
        half = piece_rows // 2
        rc = half // NC
        state = (piece_rows, LANES)
        vec = (n_vec // LANES, LANES)
        full = (N_DEV * piece_rows, LANES)
        any_spec = pl.BlockSpec(memory_space=pl.ANY)
        vmem_spec = pl.BlockSpec(memory_space=pltpu.VMEM)
        state_new, big, px, py = pl.pallas_call(
            functools.partial(step_kernel, half, rc, n_vec),
            out_shape=[pltpu.VMEM((3 * piece_rows + 6 * VROWS, LANES), F32), pltpu.VMEM(full, BF16)]
            + [jax.ShapeDtypeStruct((TAIL * rc, LANES), BF16)] * 2,
            in_specs=[any_spec] * 9,
            out_specs=[vmem_spec] * 2 + [any_spec] * 2,
            scratch_shapes=[
                pltpu.VMEM(state, F32),
                pltpu.VMEM((NRAW, 1, rc * LANES), BF16),
                pltpu.VMEM((2, 12, rc, LANES), BF16),
                pltpu.VMEM((2, 2, rc, LANES), F32),
                pltpu.VMEM((8, LANES), F32),
                pltpu.VMEM((N_DEV, 8, LANES), F32),
                pltpu.VMEM((1, 2 * VROWS * LANES), BF16),
                pltpu.VMEM((2 * VROWS, LANES), BF16),
                pltpu.VMEM((VROWS, LANES), BF16),
                pltpu.VMEM((VROWS, LANES), F32),
                pltpu.VMEM((VROWS, LANES), F32),
                pltpu.VMEM((VROWS, LANES), F32),
                pltpu.VMEM((VROWS, LANES), F32),
                pltpu.VMEM((2 * VROWS, LANES), F32),
                pltpu.VMEM((1, 1), F32),
                pltpu.SemaphoreType.DMA((NRAW,)),
                pltpu.SemaphoreType.DMA((2, 12)),
                pltpu.SemaphoreType.DMA((2, 2)),
                pltpu.SemaphoreType.DMA((14, NC)),
                pltpu.SemaphoreType.DMA((8,)),
                pltpu.SemaphoreType.DMA((7,)),
                pltpu.SemaphoreType.DMA((7,)),
                pltpu.SemaphoreType.DMA((4,)),
                pltpu.SemaphoreType.DMA((4,)),
                pltpu.SemaphoreType.DMA((8,)),
                pltpu.SemaphoreType.DMA((2,)),
            ],
            compiler_params=pltpu.CompilerParams(
                collective_id=0, has_side_effects=True, vmem_limit_bytes=15 * 2 ** 20),
            name="step",
        )(
            g_mat, g_vec, p_mat.reshape(state), m_mat.reshape(state), v_mat.reshape(state),
            p_vec.reshape(vec), m_vec.reshape(vec), v_vec.reshape(vec), learn_rate.reshape(1, 1),
        )
        def permute(values, mask):
            return lax.ppermute(values, axis_name, [(d, d ^ mask) for d in range(N_DEV)])

        def cost(n_bytes):
            return pl.CostEstimate(flops=0, bytes_accessed=n_bytes, transcendentals=0)

        rx, ry = permute(px, 2), permute(py, 4)
        p_new, m_new, v_new, pv_new, mv_new, vv_new, pb = pl.pallas_call(
            functools.partial(first_write, half),
            out_shape=[jax.ShapeDtypeStruct(state, F32)] * 3 + [jax.ShapeDtypeStruct(vec, F32)] * 3
            + [jax.ShapeDtypeStruct(full, BF16)],
            in_specs=[vmem_spec] * 2,
            out_specs=[any_spec] * 7,
            scratch_shapes=[pltpu.SemaphoreType.DMA((15 + SPLIT,))],
            cost_estimate=cost(12 * n_piece + SPLIT * n_piece),
            compiler_params=pltpu.CompilerParams(vmem_limit_bytes=2 ** 20),
            name="write1",
        )(state_new, big)
        rx, ry, p_new = lax.optimization_barrier((rx, ry, p_new))
        cx, cy = permute(rx, 1), permute(ry, 1)
        pb = pl.pallas_call(
            functools.partial(second_write, half),
            out_shape=jax.ShapeDtypeStruct(full, BF16),
            in_specs=[vmem_spec] * 3 + [any_spec],
            out_specs=any_spec,
            input_output_aliases={3: 0},
            scratch_shapes=[pltpu.SemaphoreType.DMA((2 + 2 * N_DEV - SPLIT,))],
            cost_estimate=cost((2 * N_DEV - SPLIT) * n_piece),
            compiler_params=pltpu.CompilerParams(vmem_limit_bytes=2 * 2 ** 20),
            name="write2",
        )(big, rx, ry, pb)
        pb = pl.pallas_call(
            functools.partial(third_write, half),
            out_shape=jax.ShapeDtypeStruct(full, BF16),
            in_specs=[vmem_spec] * 2 + [any_spec],
            out_specs=any_spec,
            input_output_aliases={2: 0},
            scratch_shapes=[pltpu.SemaphoreType.DMA((2,))],
            compiler_params=pltpu.CompilerParams(vmem_limit_bytes=2 * 2 ** 20),
            name="write3",
        )(cx, cy, pb)
        return (
            p_new.reshape(-1), m_new.reshape(-1), v_new.reshape(-1),
            pv_new.reshape(-1), mv_new.reshape(-1), vv_new.reshape(-1), pb.reshape(-1),
        )

    return jax.shard_map(
        local_step,
        mesh=mesh,
        in_specs=(P(axis_name, None), P(axis_name, None), P(axis_name), P(axis_name), P(axis_name), P(), P(), P(), P()),
        out_specs=(P(axis_name), P(axis_name), P(axis_name), P(), P(), P(), P()),
        check_vma=False,
    )
```

```python
import functools

import jax
import jax.numpy as jnp
from jax import lax
from jax.experimental import pallas as pl
from jax.experimental.pallas import tpu as pltpu
from jax.sharding import PartitionSpec as P

STEP = 10
ADAM_BETA1 = 0.9
ADAM_BETA2 = 0.98
ADAM_EPS = 1e-8
WEIGHT_DECAY = 0.01
MAX_NORM = 1.0
NORM_EPS = 1e-6
BIAS_ONE = 1.0 - ADAM_BETA1 ** STEP
BIAS_TWO = 1.0 - ADAM_BETA2 ** STEP

LANES = 128
N_DEV = 8
NC = 12
NRAW = 8
EARLY = 4
FIRST_PARTS = 6
TAIL = 5
SPLIT = 15
DIAG_LAG = 4
LAG = 2
VROWS = 80
MESH = pl.DeviceIdType.MESH
F32 = jnp.float32
BF16 = jnp.bfloat16


def adam_update(grad_vals, param_vals, moment_one, moment_two, learn_rate, decay_rate):
    new_one = ADAM_BETA1 * moment_one + (1.0 - ADAM_BETA1) * grad_vals
    new_two = ADAM_BETA2 * moment_two + (1.0 - ADAM_BETA2) * grad_vals * grad_vals
    direction = (new_one / BIAS_ONE) / (jnp.sqrt(new_two / BIAS_TWO) + ADAM_EPS)
    return param_vals - learn_rate * (direction + decay_rate * param_vals), new_one, new_two


def flip(device, mask):
    for bit in (1, 2, 4):
        if mask & bit:
            device = device + bit - 2 * bit * lax.rem(lax.div(device, bit), 2)
    return device


def step_kernel(
    half, rc, n_vec,
    g_hbm, gv_hbm, p_hbm, m_hbm, v_hbm, pv_hbm, mv_hbm, vv_hbm, lr_hbm,
    state, big, px_hbm, py_hbm,
    fin, raw, pk, rel, acc, norms, vraw, vpk, vland, vs1, vlx, vs2, vly, vfull, lr_ref,
    raw_sem, send_sem, rel_sem, rs, st_sem, ns_sem, nr_sem, vs_sem, vr_sem, ag_sem, px_sem,
):
    piece_rows = 2 * half
    p_ref, m_ref, v_ref = (state.at[pl.ds(k * piece_rows, piece_rows)] for k in range(3))
    pv_out, mv_out, vv_out = (
        state.at[pl.ds(3 * piece_rows + k * 2 * VROWS, n_vec // LANES)] for k in range(3))
    me = lax.axis_index("dp")
    core = lax.rem(me, 2)
    peer = {mask: flip(me, mask) for mask in range(1, N_DEV)}

    def remote(src, dst, ssem, rsem, mask):
        return pltpu.make_async_remote_copy(
            src_ref=src, dst_ref=dst, send_sem=ssem, recv_sem=rsem,
            device_id=(peer[mask],), device_id_type=MESH,
        )

    def rows(first, count, align=16):
        return pl.ds(pl.multiple_of(first, align), count)

    blocks = []
    for j in (0, 1):
        for h in (0, 1):
            via = (4, 2)[h]
            blocks.append(("send", h, 6 ^ j, via ^ j, h * 3 + j))
    for h in (0, 1):
        blocks.append(("send", h, (2, 4)[h] ^ 1, 1, h * 3 + 2))
        blocks.append(("own", h, (2, 4)[h], None, 14 + h))
    for j in (0, 1):
        for h in (0, 1):
            via = (4, 2)[h]
            blocks.append(("send", h, via ^ j, via ^ j, 6 + h * 3 + j))
    for h in (0, 1):
        blocks.append(("send", h, 1, 1, 6 + h * 3 + 2))
        blocks.append(("own", h, 0, None, 12 + h))
    n_blocks = len(blocks)
    send_slot = {}
    for b, block in enumerate(blocks):
        if block[0] == "send":
            send_slot[b] = len(send_slot)

    def raw_copy(b, c):
        _, h, mask, _, _ = blocks[b]
        piece = flip(me, mask) if mask else me
        start = (piece * piece_rows + h * half + c * rc) * LANES
        return pltpu.make_async_copy(
            g_hbm.at[:, pl.ds(pl.multiple_of(start, 2048), rc * LANES)],
            raw.at[b % NRAW], raw_sem.at[b % NRAW],
        )

    def block_copy(b, c):
        _, h, _, dest, slot = blocks[b]
        s = send_slot[b]
        par = lax.rem(c, 2)
        return remote(
            pk.at[par, s], big.at[rows(slot * half + c * rc, rc)],
            send_sem.at[par, s], rs.at[slot, c], dest,
        )

    def landed(slot, c):
        ref = big.at[rows(slot * half + c * rc, rc)]
        return remote(ref, ref, send_sem.at[0, 0], rs.at[slot, c], 1)

    def rel_copy(h, c):
        par = lax.rem(c, 2)
        return remote(
            rel.at[par, h], fin.at[rows(h * half + c * rc, rc)],
            rel_sem.at[par, h], rs.at[12 + h, c], (2, 4)[h],
        )

    state_copies = [
        pltpu.make_async_copy(src, dst, st_sem.at[i])
        for i, (src, dst) in enumerate((
            (p_hbm, p_ref), (m_hbm, m_ref), (v_hbm, v_ref),
            (pv_hbm, pv_out), (mv_hbm, mv_out), (vv_hbm, vv_out), (lr_hbm, lr_ref)))
    ]
    vraw_copy = pltpu.make_async_copy(gv_hbm, vraw.at[:, pl.ds(0, n_vec)], st_sem.at[7])

    barrier = pltpu.get_barrier_semaphore()
    for mask in range(1, N_DEV):
        pl.semaphore_signal(barrier, inc=1, device_id=(peer[mask],), device_id_type=MESH)
    for b in range(NRAW):
        raw_copy(b, 0).start()
    vraw[:, pl.ds(n_vec // 1024 * 1024, 2 * VROWS * LANES - n_vec // 1024 * 1024)] = jnp.zeros(
        (1, 2 * VROWS * LANES - n_vec // 1024 * 1024), BF16)
    acc[...] = jnp.zeros_like(acc)
    step_rows = 64

    def pack_rows(src, dst, first):
        def body(i, _):
            vals = src[:, pl.ds(pl.multiple_of(i * step_rows * LANES, 2048), step_rows * LANES)]
            dst[rows(first + i * step_rows, step_rows), :] = (
                vals.astype(F32).reshape(step_rows, LANES).astype(BF16))
            return 0
        lax.fori_loop(0, rc // step_rows, body, 0, unroll=2)

    def load_block(b, c):
        kind, _, _, _, slot = blocks[b]
        raw_copy(b, c).wait()
        if kind == "send":
            @pl.when(c >= 2)
            def _():
                block_copy(b, c - 2).wait_send()
            pack_rows(raw.at[b % NRAW], pk.at[lax.rem(c, 2), send_slot[b]], 0)
        else:
            pack_rows(raw.at[b % NRAW], big, slot * half + c * rc)
        if b + NRAW < n_blocks:
            raw_copy(b + NRAW, c).start()
        else:
            @pl.when(c + 1 < NC)
            def _():
                raw_copy(b + NRAW - n_blocks, c + 1).start()

    for b in range(EARLY):
        load_block(b, 0)
    pl.semaphore_wait(barrier, N_DEV - 1)

    def send_chunk(c):
        waiting = None
        for b, (kind, h, mask, dest, slot) in enumerate(blocks):
            if b < EARLY:
                @pl.when(c >= 1)
                def _():
                    load_block(b, c)
            else:
                load_block(b, c)
            if waiting is not None:
                block_copy(waiting, c).start()
            waiting = b if kind == "send" else None
        if waiting is not None:
            block_copy(waiting, c).start()

    sum_rows = 32

    def relay_chunk(c):
        par = lax.rem(c, 2)
        for h in (0, 1):
            for j in range(3):
                landed(h * 3 + j, c).wait_recv()
            if h == 1:
                rel_copy(0, c).start()

            @pl.when(c >= 2)
            def _():
                rel_copy(h, c - 2).wait_send()

            def body(i, _):
                at = c * rc + i * sum_rows
                total = big[rows((14 + h) * half + at, sum_rows), :].astype(F32)
                for j in (2, 0, 1):
                    total = total + big[rows((h * 3 + j) * half + at, sum_rows), :].astype(F32)
                rel[par, h, rows(i * sum_rows, sum_rows), :] = total
                return 0
            lax.fori_loop(0, rc // sum_rows, body, 0, unroll=3)
        rel_copy(1, c).start()

    def final_chunk(c):
        for h in (0, 1):
            for j in range(3):
                landed(6 + h * 3 + j, c).wait_recv()
            rel_copy(h, c).wait_recv()

            def body(i, sq):
                at = c * rc + i * sum_rows
                total = big[rows((12 + h) * half + at, sum_rows), :].astype(F32)
                for j in (2, 0, 1):
                    total = total + big[rows((6 + h * 3 + j) * half + at, sum_rows), :].astype(F32)
                total = (total + fin[rows(h * half + at, sum_rows), :]) * (1.0 / N_DEV)
                fin[rows(h * half + at, sum_rows), :] = total
                total = total * total
                for k in range(sum_rows // 8):
                    sq = sq + total[8 * k:8 * k + 8]
                return sq
            acc[...] = lax.fori_loop(0, rc // sum_rows, body, acc[...], unroll=6)

    mine = rows(core * VROWS, VROWS)
    other = rows((1 - core) * VROWS, VROWS)
    vec_core = remote(vpk.at[other], vland, vs_sem.at[0], vr_sem.at[0], 1)
    vec_x = remote(vs1, vlx, vs_sem.at[1], vr_sem.at[1], 2)
    vec_y = remote(vs2, vly, vs_sem.at[2], vr_sem.at[2], 4)
    vec_back = remote(vfull.at[mine], vfull.at[mine], vs_sem.at[3], vr_sem.at[3], 1)
    vec_back_in = remote(vfull.at[other], vfull.at[other], vs_sem.at[3], vr_sem.at[3], 1)

    def vec_step(c):
        @pl.when(c == 1)
        def _():
            vraw_copy.wait()
            vpk[...] = vraw[...].astype(F32).reshape(2 * VROWS, LANES).astype(BF16)

        @pl.when(c == 2)
        def _():
            vec_core.start()

        @pl.when(c == 3)
        def _():
            vec_core.wait_recv()
            vs1[...] = vpk[mine, :].astype(F32) + vland[...].astype(F32)

        @pl.when(c == 4)
        def _():
            vec_x.start()

        @pl.when(c == 6)
        def _():
            vec_x.wait_recv()
            vs2[...] = vs1[...] + vlx[...]

        @pl.when(c == 7)
        def _():
            vec_y.start()

        @pl.when(c == 9)
        def _():
            vec_y.wait_recv()
            vfull[mine, :] = (vs2[...] + vly[...]) * (1.0 / N_DEV)

        @pl.when(c == 10)
        def _():
            vec_back.start()

        @pl.when(c == 12)
        def _():
            vec_back_in.wait_recv()
            vec_core.wait_send()
            vec_x.wait_send()
            vec_y.wait_send()
            vec_back.wait_send()

    def scatter_step(c, _):
        @pl.when(c < NC)
        def _():
            send_chunk(c)

        @pl.when(c == 0)
        def _():
            vraw_copy.start()

        @pl.when(c == 3)
        def _():
            for copy in state_copies:
                copy.start()

        vec_step(c)

        @pl.when((c >= 1) & (c < NC + 1))
        def _():
            relay_chunk(c - 1)

        @pl.when(c >= 2)
        def _():
            final_chunk(c - 2)
        return 0

    lax.fori_loop(0, NC + 2, scatter_step, 0)

    norms[me] = acc[...]
    vec_sq = jnp.sum(vfull[...] * vfull[...], keepdims=True)
    for copy in state_copies:
        copy.wait()

    def norm_copy(mask):
        return remote(norms.at[me], norms.at[me], ns_sem.at[mask - 1], nr_sem.at[mask - 1], mask)

    for mask in (6, 7, 2, 4, 3, 5, 1):
        norm_copy(mask).start()
    for c in (NC - 2, NC - 1):
        for b in send_slot:
            block_copy(b, c).wait_send()
        for h in (0, 1):
            rel_copy(h, c).wait_send()
    for mask in range(1, N_DEV):
        norm_copy(mask).wait_recv()
    total = norms[0]
    for k in range(1, N_DEV):
        total = total + norms[k]
    norm_sq = jnp.sum(total, keepdims=True) + vec_sq
    clip = jnp.minimum(1.0, MAX_NORM / (jnp.sqrt(norm_sq) + NORM_EPS))
    lr = lr_ref[...]

    upd_rows = 32
    clip_rows = jnp.broadcast_to(clip, (upd_rows, LANES))
    lr_rows = jnp.broadcast_to(lr, (upd_rows, LANES))

    def update_chunk(h, c, first=0, count=rc):
        def body(i, _):
            at = h * half + c * rc + first + i * upd_rows
            here = rows(at, upd_rows)
            new_p, new_m, new_v = adam_update(
                fin[here, :] * clip_rows, p_ref[here, :], m_ref[here, :], v_ref[here, :], lr_rows, WEIGHT_DECAY)
            p_ref[here, :] = new_p
            m_ref[here, :] = new_m
            v_ref[here, :] = new_v
            big[rows(me * piece_rows + at, upd_rows), :] = new_p.astype(BF16)
            return 0
        lax.fori_loop(0, count // upd_rows, body, 0, unroll=3)

    def gather_copy(mask, h, c, dest, ssem, slot):
        piece = flip(me, mask) if mask else me
        ref = big.at[rows(piece * piece_rows + h * half + c * rc, rc)]
        return remote(ref, ref, ag_sem.at[ssem], rs.at[slot, c], dest)

    def own_x(h, c):
        return gather_copy(0, h, c, 2, 0, h)

    def own_y(h, c):
        return gather_copy(0, h, c, 4, 1, 2 + h)

    def own_core(h, c):
        return gather_copy(0, h, c, 1, 2, 6 + h)

    def arrived(mask, h, c, slot):
        gather_copy(mask, h, c, 1, 0, slot).wait_recv()

    def to_core(mask, h, c):
        return gather_copy(mask, h, c, 1, {2: 5, 4: 6, 6: 7}[mask], {2: 8, 4: 10, 6: 12}[mask] + h)

    def diagonal(j):
        arrived(6, 0, j, 4)
        to_core(6, 0, j).start()
        arrived(6, 1, j, 5)
        to_core(6, 1, j).start()

    def first_half(i, _):
        @pl.when(i < NC)
        def _():
            @pl.when(i > 0)
            def _():
                update_chunk(0, i)
                own_x(0, i).start()
                update_chunk(1, i)
                own_y(1, i).start()
            own_core(0, i).start()
            own_core(1, i).start()

        @pl.when(i >= LAG)
        def _():
            j = i - LAG
            arrived(2, 0, j, 0)
            gather_copy(2, 0, j, 4, 3, 4).start()
            to_core(2, 0, j).start()
            arrived(4, 1, j, 3)
            gather_copy(4, 1, j, 2, 4, 5).start()
            to_core(4, 1, j).start()

        @pl.when(i >= DIAG_LAG)
        def _():
            diagonal(i - DIAG_LAG)

        @pl.when(i >= NC)
        def _():
            own_x(1, i - NC).start()
            own_y(0, i - NC).start()
        return 0

    for k in range(FIRST_PARTS):
        part = rc // FIRST_PARTS
        for h, dest, ssem in ((0, 2, 0), (1, 4, 1)):
            update_chunk(h, 0, k * part, part)
            ref = big.at[rows(me * piece_rows + h * half + k * part, part)]
            remote(ref, ref, ag_sem.at[ssem], rs.at[3 * h, 0], dest).start()
    lax.fori_loop(0, NC + LAG, first_half, 0)

    kept = half - TAIL * rc
    tail_copies = [
        pltpu.make_async_copy(
            big.at[rows(me * piece_rows + h * half + kept, TAIL * rc)], dst, px_sem.at[h])
        for h, dst in ((1, px_hbm), (0, py_hbm))
    ]
    for copy in tail_copies:
        copy.start()

    vrows = n_vec // LANES
    new_p, new_m, new_v = adam_update(
        vfull[pl.ds(0, vrows), :] * clip, pv_out[...], mv_out[...], vv_out[...], lr, 0.0)
    pv_out[...] = new_p
    mv_out[...] = new_m
    vv_out[...] = new_v

    def second_half(j, _):
        @pl.when(j + LAG < NC - TAIL)
        def _():
            own_x(1, j + LAG).start()
            own_y(0, j + LAG).start()
        @pl.when(j < DIAG_LAG - LAG)
        def _():
            diagonal(NC + LAG - DIAG_LAG + j)
        arrived(2, 1, j, 1)
        to_core(2, 1, j).start()
        arrived(4, 0, j, 2)
        to_core(4, 0, j).start()
        return 0

    lax.fori_loop(0, NC - TAIL, second_half, 0)

    def last_arrivals(c, _):
        for mask, h in ((1, 0), (1, 1), (3, 0), (5, 1), (7, 0), (7, 1)):
            arrived(mask, h, c, 5 + mask + h)

        @pl.when(c < NC - TAIL)
        def _():
            for mask, h in ((3, 1), (5, 0)):
                arrived(mask, h, c, 5 + mask + h)
        return 0

    lax.fori_loop(0, NC, last_arrivals, 0)
    for ssem, count in (
        (0, half + kept), (1, half + kept), (2, 2 * half), (3, half), (4, half),
        (5, half + kept), (6, half + kept), (7, 2 * half),
    ):
        ref = big.at[pl.ds(0, count)]
        remote(ref, ref, ag_sem.at[ssem], rs.at[0, 0], 1).wait_send()
    for mask in range(1, N_DEV):
        norm_copy(mask).wait_send()
    for copy in tail_copies:
        copy.wait()


def run_all(copies):
    for copy in copies:
        copy.start()
    for copy in copies:
        copy.wait()


def first_write(half, state, big, *refs):
    dsts, sem = refs[:-1], refs[-1]
    copies = []

    def add(src, src_at, dst, count, size):
        part = size // count
        for k in range(count):
            copies.append(pltpu.make_async_copy(
                src.at[pl.ds(src_at + k * part, part)], dst.at[pl.ds(k * part, part)], sem.at[len(copies)]))

    at = 0
    for dst in dsts[:6]:
        size = dst.shape[0]
        add(state, at, dst, 4 if size > 2 * VROWS else 1, size)
        at += max(size, 2 * VROWS)
    add(big, 0, dsts[6], SPLIT, SPLIT * half)
    run_all(copies)


def tail_copies_of(half, parts, dst, sem):
    me = lax.axis_index("dp")
    copies = []
    for i, (src, mask, h) in enumerate(parts):
        tail = src.shape[0]
        at = flip(me, mask) * (2 * half) + (h + 1) * half - tail
        copies.append(pltpu.make_async_copy(src, dst.at[pl.ds(pl.multiple_of(at, 16), tail)], sem.at[i]))
    return copies


def second_write(half, big, rx, ry, _, dst, sem):
    run_all([
        pltpu.make_async_copy(big.at[pl.ds(k * half, half)], dst.at[pl.ds(k * half, half)], sem.at[2 + k - SPLIT])
        for k in range(SPLIT, 2 * N_DEV)
    ])
    run_all(tail_copies_of(half, ((rx, 2, 1), (ry, 4, 0)), dst, sem))


def third_write(half, cx, cy, _, dst, sem):
    run_all(tail_copies_of(half, ((cx, 3, 1), (cy, 5, 0)), dst, sem))


def solution(mesh):
    axis_name = mesh.axis_names[0]

    def local_step(g_mat, g_vec, p_mat, m_mat, v_mat, p_vec, m_vec, v_vec, learn_rate):
        n_piece = p_mat.shape[0]
        n_vec = p_vec.shape[0]
        piece_rows = n_piece // LANES
        half = piece_rows // 2
        rc = half // NC
        state = (piece_rows, LANES)
        vec = (n_vec // LANES, LANES)
        full = (N_DEV * piece_rows, LANES)
        any_spec = pl.BlockSpec(memory_space=pl.ANY)
        vmem_spec = pl.BlockSpec(memory_space=pltpu.VMEM)
        state_new, big, px, py = pl.pallas_call(
            functools.partial(step_kernel, half, rc, n_vec),
            out_shape=[pltpu.VMEM((3 * piece_rows + 6 * VROWS, LANES), F32), pltpu.VMEM(full, BF16)]
            + [jax.ShapeDtypeStruct((TAIL * rc, LANES), BF16)] * 2,
            in_specs=[any_spec] * 9,
            out_specs=[vmem_spec] * 2 + [any_spec] * 2,
            scratch_shapes=[
                pltpu.VMEM(state, F32),
                pltpu.VMEM((NRAW, 1, rc * LANES), BF16),
                pltpu.VMEM((2, 12, rc, LANES), BF16),
                pltpu.VMEM((2, 2, rc, LANES), F32),
                pltpu.VMEM((8, LANES), F32),
                pltpu.VMEM((N_DEV, 8, LANES), F32),
                pltpu.VMEM((1, 2 * VROWS * LANES), BF16),
                pltpu.VMEM((2 * VROWS, LANES), BF16),
                pltpu.VMEM((VROWS, LANES), BF16),
                pltpu.VMEM((VROWS, LANES), F32),
                pltpu.VMEM((VROWS, LANES), F32),
                pltpu.VMEM((VROWS, LANES), F32),
                pltpu.VMEM((VROWS, LANES), F32),
                pltpu.VMEM((2 * VROWS, LANES), F32),
                pltpu.VMEM((1, 1), F32),
                pltpu.SemaphoreType.DMA((NRAW,)),
                pltpu.SemaphoreType.DMA((2, 12)),
                pltpu.SemaphoreType.DMA((2, 2)),
                pltpu.SemaphoreType.DMA((14, NC)),
                pltpu.SemaphoreType.DMA((8,)),
                pltpu.SemaphoreType.DMA((7,)),
                pltpu.SemaphoreType.DMA((7,)),
                pltpu.SemaphoreType.DMA((4,)),
                pltpu.SemaphoreType.DMA((4,)),
                pltpu.SemaphoreType.DMA((8,)),
                pltpu.SemaphoreType.DMA((2,)),
            ],
            compiler_params=pltpu.CompilerParams(
                collective_id=0, has_side_effects=True, vmem_limit_bytes=15 * 2 ** 20),
            name="step",
        )(
            g_mat, g_vec, p_mat.reshape(state), m_mat.reshape(state), v_mat.reshape(state),
            p_vec.reshape(vec), m_vec.reshape(vec), v_vec.reshape(vec), learn_rate.reshape(1, 1),
        )
        def permute(values, mask):
            return lax.ppermute(values, axis_name, [(d, d ^ mask) for d in range(N_DEV)])

        def cost(n_bytes):
            return pl.CostEstimate(flops=0, bytes_accessed=n_bytes, transcendentals=0)

        rx, ry = permute(px, 2), permute(py, 4)
        p_new, m_new, v_new, pv_new, mv_new, vv_new, pb = pl.pallas_call(
            functools.partial(first_write, half),
            out_shape=[jax.ShapeDtypeStruct(state, F32)] * 3 + [jax.ShapeDtypeStruct(vec, F32)] * 3
            + [jax.ShapeDtypeStruct(full, BF16)],
            in_specs=[vmem_spec] * 2,
            out_specs=[any_spec] * 7,
            scratch_shapes=[pltpu.SemaphoreType.DMA((15 + SPLIT,))],
            cost_estimate=cost(12 * n_piece + SPLIT * n_piece),
            compiler_params=pltpu.CompilerParams(vmem_limit_bytes=2 ** 20),
            name="write1",
        )(state_new, big)
        rx, ry, p_new = lax.optimization_barrier((rx, ry, p_new))
        cx, cy = permute(rx, 1), permute(ry, 1)
        pb = pl.pallas_call(
            functools.partial(second_write, half),
            out_shape=jax.ShapeDtypeStruct(full, BF16),
            in_specs=[vmem_spec] * 3 + [any_spec],
            out_specs=any_spec,
            input_output_aliases={3: 0},
            scratch_shapes=[pltpu.SemaphoreType.DMA((2 + 2 * N_DEV - SPLIT,))],
            cost_estimate=cost((2 * N_DEV - SPLIT) * n_piece),
            compiler_params=pltpu.CompilerParams(vmem_limit_bytes=2 * 2 ** 20),
            name="write2",
        )(big, rx, ry, pb)
        pb = pl.pallas_call(
            functools.partial(third_write, half),
            out_shape=jax.ShapeDtypeStruct(full, BF16),
            in_specs=[vmem_spec] * 2 + [any_spec],
            out_specs=any_spec,
            input_output_aliases={2: 0},
            scratch_shapes=[pltpu.SemaphoreType.DMA((2,))],
            compiler_params=pltpu.CompilerParams(vmem_limit_bytes=2 * 2 ** 20),
            name="write3",
        )(cx, cy, pb)
        return (
            p_new.reshape(-1), m_new.reshape(-1), v_new.reshape(-1),
            pv_new.reshape(-1), mv_new.reshape(-1), vv_new.reshape(-1), pb.reshape(-1),
        )

    return jax.shard_map(
        local_step,
        mesh=mesh,
        in_specs=(P(axis_name, None), P(axis_name, None), P(axis_name), P(axis_name), P(axis_name), P(), P(), P(), P()),
        out_specs=(P(axis_name), P(axis_name), P(axis_name), P(), P(), P(), P()),
        check_vma=False,
    )
```

```python
import functools

import jax
import jax.numpy as jnp
from jax import lax
from jax.experimental import pallas as pl
from jax.experimental.pallas import tpu as pltpu
from jax.sharding import PartitionSpec as P

STEP = 10
ADAM_BETA1 = 0.9
ADAM_BETA2 = 0.98
ADAM_EPS = 1e-8
WEIGHT_DECAY = 0.01
MAX_NORM = 1.0
NORM_EPS = 1e-6
BIAS_ONE = 1.0 - ADAM_BETA1 ** STEP
BIAS_TWO = 1.0 - ADAM_BETA2 ** STEP

LANES = 128
N_DEV = 8
NC = 12
NRAW = 8
EARLY = 4
FIRST_PARTS = 6
TAIL = 5
SPLIT = 16
DIAG_LAG = 4
LAG = 2
VROWS = 80
MESH = pl.DeviceIdType.MESH
F32 = jnp.float32
BF16 = jnp.bfloat16


def adam_update(grad_vals, param_vals, moment_one, moment_two, learn_rate, decay_rate):
    new_one = ADAM_BETA1 * moment_one + (1.0 - ADAM_BETA1) * grad_vals
    new_two = ADAM_BETA2 * moment_two + (1.0 - ADAM_BETA2) * grad_vals * grad_vals
    direction = (new_one / BIAS_ONE) / (jnp.sqrt(new_two / BIAS_TWO) + ADAM_EPS)
    return param_vals - learn_rate * (direction + decay_rate * param_vals), new_one, new_two


def flip(device, mask):
    for bit in (1, 2, 4):
        if mask & bit:
            device = device + bit - 2 * bit * lax.rem(lax.div(device, bit), 2)
    return device


def step_kernel(
    half, rc, n_vec,
    g_hbm, gv_hbm, p_hbm, m_hbm, v_hbm, pv_hbm, mv_hbm, vv_hbm, lr_hbm,
    state, big, px_hbm, py_hbm,
    fin, raw, pk, rel, acc, norms, vraw, vpk, vland, vs1, vlx, vs2, vly, vfull, lr_ref,
    raw_sem, send_sem, rel_sem, rs, st_sem, ns_sem, nr_sem, vs_sem, vr_sem, ag_sem, px_sem,
):
    piece_rows = 2 * half
    p_ref, m_ref, v_ref = (state.at[pl.ds(k * piece_rows, piece_rows)] for k in range(3))
    pv_out, mv_out, vv_out = (
        state.at[pl.ds(3 * piece_rows + k * 2 * VROWS, n_vec // LANES)] for k in range(3))
    me = lax.axis_index("dp")
    core = lax.rem(me, 2)
    peer = {mask: flip(me, mask) for mask in range(1, N_DEV)}

    def remote(src, dst, ssem, rsem, mask):
        return pltpu.make_async_remote_copy(
            src_ref=src, dst_ref=dst, send_sem=ssem, recv_sem=rsem,
            device_id=(peer[mask],), device_id_type=MESH,
        )

    def rows(first, count, align=16):
        return pl.ds(pl.multiple_of(first, align), count)

    blocks = []
    for j in (0, 1):
        for h in (0, 1):
            via = (4, 2)[h]
            blocks.append(("send", h, 6 ^ j, via ^ j, h * 3 + j))
    for h in (0, 1):
        blocks.append(("send", h, (2, 4)[h] ^ 1, 1, h * 3 + 2))
        blocks.append(("own", h, (2, 4)[h], None, 14 + h))
    for j in (0, 1):
        for h in (0, 1):
            via = (4, 2)[h]
            blocks.append(("send", h, via ^ j, via ^ j, 6 + h * 3 + j))
    for h in (0, 1):
        blocks.append(("send", h, 1, 1, 6 + h * 3 + 2))
        blocks.append(("own", h, 0, None, 12 + h))
    n_blocks = len(blocks)
    send_slot = {}
    for b, block in enumerate(blocks):
        if block[0] == "send":
            send_slot[b] = len(send_slot)

    def raw_copy(b, c):
        _, h, mask, _, _ = blocks[b]
        piece = flip(me, mask) if mask else me
        start = (piece * piece_rows + h * half + c * rc) * LANES
        return pltpu.make_async_copy(
            g_hbm.at[:, pl.ds(pl.multiple_of(start, 2048), rc * LANES)],
            raw.at[b % NRAW], raw_sem.at[b % NRAW],
        )

    def block_copy(b, c):
        _, h, _, dest, slot = blocks[b]
        s = send_slot[b]
        par = lax.rem(c, 2)
        return remote(
            pk.at[par, s], big.at[rows(slot * half + c * rc, rc)],
            send_sem.at[par, s], rs.at[slot, c], dest,
        )

    def landed(slot, c):
        ref = big.at[rows(slot * half + c * rc, rc)]
        return remote(ref, ref, send_sem.at[0, 0], rs.at[slot, c], 1)

    def rel_copy(h, c):
        par = lax.rem(c, 2)
        return remote(
            rel.at[par, h], fin.at[rows(h * half + c * rc, rc)],
            rel_sem.at[par, h], rs.at[12 + h, c], (2, 4)[h],
        )

    state_copies = [
        pltpu.make_async_copy(src, dst, st_sem.at[i])
        for i, (src, dst) in enumerate((
            (p_hbm, p_ref), (m_hbm, m_ref), (v_hbm, v_ref),
            (pv_hbm, pv_out), (mv_hbm, mv_out), (vv_hbm, vv_out), (lr_hbm, lr_ref)))
    ]
    vraw_copy = pltpu.make_async_copy(gv_hbm, vraw.at[:, pl.ds(0, n_vec)], st_sem.at[7])

    barrier = pltpu.get_barrier_semaphore()
    for mask in range(1, N_DEV):
        pl.semaphore_signal(barrier, inc=1, device_id=(peer[mask],), device_id_type=MESH)
    for b in range(NRAW):
        raw_copy(b, 0).start()
    vraw[:, pl.ds(n_vec // 1024 * 1024, 2 * VROWS * LANES - n_vec // 1024 * 1024)] = jnp.zeros(
        (1, 2 * VROWS * LANES - n_vec // 1024 * 1024), BF16)
    acc[...] = jnp.zeros_like(acc)
    step_rows = 64

    def pack_rows(src, dst, first):
        def body(i, _):
            vals = src[:, pl.ds(pl.multiple_of(i * step_rows * LANES, 2048), step_rows * LANES)]
            dst[rows(first + i * step_rows, step_rows), :] = (
                vals.astype(F32).reshape(step_rows, LANES).astype(BF16))
            return 0
        lax.fori_loop(0, rc // step_rows, body, 0, unroll=2)

    def load_block(b, c):
        kind, _, _, _, slot = blocks[b]
        raw_copy(b, c).wait()
        if kind == "send":
            @pl.when(c >= 2)
            def _():
                block_copy(b, c - 2).wait_send()
            pack_rows(raw.at[b % NRAW], pk.at[lax.rem(c, 2), send_slot[b]], 0)
        else:
            pack_rows(raw.at[b % NRAW], big, slot * half + c * rc)
        if b + NRAW < n_blocks:
            raw_copy(b + NRAW, c).start()
        else:
            @pl.when(c + 1 < NC)
            def _():
                raw_copy(b + NRAW - n_blocks, c + 1).start()

    for b in range(EARLY):
        load_block(b, 0)
    pl.semaphore_wait(barrier, N_DEV - 1)

    def send_chunk(c):
        waiting = None
        for b, (kind, h, mask, dest, slot) in enumerate(blocks):
            if b < EARLY:
                @pl.when(c >= 1)
                def _():
                    load_block(b, c)
            else:
                load_block(b, c)
            if waiting is not None:
                block_copy(waiting, c).start()
            waiting = b if kind == "send" else None
        if waiting is not None:
            block_copy(waiting, c).start()

    sum_rows = 32

    def relay_chunk(c):
        par = lax.rem(c, 2)
        for h in (0, 1):
            for j in range(3):
                landed(h * 3 + j, c).wait_recv()

            @pl.when(c >= 2)
            def _():
                rel_copy(h, c - 2).wait_send()

            def body(i, _):
                at = c * rc + i * sum_rows
                total = big[rows((14 + h) * half + at, sum_rows), :].astype(F32)
                for j in (2, 0, 1):
                    total = total + big[rows((h * 3 + j) * half + at, sum_rows), :].astype(F32)
                rel[par, h, rows(i * sum_rows, sum_rows), :] = total
                return 0
            lax.fori_loop(0, rc // sum_rows, body, 0, unroll=3)
        for h in (0, 1):
            rel_copy(h, c).start()

    def final_chunk(c):
        for h in (0, 1):
            for j in range(3):
                landed(6 + h * 3 + j, c).wait_recv()
            rel_copy(h, c).wait_recv()

            def body(i, sq):
                at = c * rc + i * sum_rows
                total = big[rows((12 + h) * half + at, sum_rows), :].astype(F32)
                for j in (2, 0, 1):
                    total = total + big[rows((6 + h * 3 + j) * half + at, sum_rows), :].astype(F32)
                total = (total + fin[rows(h * half + at, sum_rows), :]) * (1.0 / N_DEV)
                fin[rows(h * half + at, sum_rows), :] = total
                total = total * total
                for k in range(sum_rows // 8):
                    sq = sq + total[8 * k:8 * k + 8]
                return sq
            acc[...] = lax.fori_loop(0, rc // sum_rows, body, acc[...], unroll=6)

    mine = rows(core * VROWS, VROWS)
    other = rows((1 - core) * VROWS, VROWS)
    vec_core = remote(vpk.at[other], vland, vs_sem.at[0], vr_sem.at[0], 1)
    vec_x = remote(vs1, vlx, vs_sem.at[1], vr_sem.at[1], 2)
    vec_y = remote(vs2, vly, vs_sem.at[2], vr_sem.at[2], 4)
    vec_back = remote(vfull.at[mine], vfull.at[mine], vs_sem.at[3], vr_sem.at[3], 1)
    vec_back_in = remote(vfull.at[other], vfull.at[other], vs_sem.at[3], vr_sem.at[3], 1)

    def vec_step(c):
        @pl.when(c == 1)
        def _():
            vraw_copy.wait()
            vpk[...] = vraw[...].astype(F32).reshape(2 * VROWS, LANES).astype(BF16)

        @pl.when(c == 2)
        def _():
            vec_core.start()

        @pl.when(c == 3)
        def _():
            vec_core.wait_recv()
            vs1[...] = vpk[mine, :].astype(F32) + vland[...].astype(F32)

        @pl.when(c == 4)
        def _():
            vec_x.start()

        @pl.when(c == 6)
        def _():
            vec_x.wait_recv()
            vs2[...] = vs1[...] + vlx[...]

        @pl.when(c == 7)
        def _():
            vec_y.start()

        @pl.when(c == 9)
        def _():
            vec_y.wait_recv()
            vfull[mine, :] = (vs2[...] + vly[...]) * (1.0 / N_DEV)

        @pl.when(c == 10)
        def _():
            vec_back.start()

        @pl.when(c == 12)
        def _():
            vec_back_in.wait_recv()
            vec_core.wait_send()
            vec_x.wait_send()
            vec_y.wait_send()
            vec_back.wait_send()

    def scatter_step(c, _):
        @pl.when(c < NC)
        def _():
            send_chunk(c)

        @pl.when(c == 0)
        def _():
            vraw_copy.start()

        @pl.when(c == 3)
        def _():
            for copy in state_copies:
                copy.start()

        vec_step(c)

        @pl.when((c >= 1) & (c < NC + 1))
        def _():
            relay_chunk(c - 1)

        @pl.when(c >= 2)
        def _():
            final_chunk(c - 2)
        return 0

    lax.fori_loop(0, NC + 2, scatter_step, 0)

    norms[me] = acc[...]
    vec_sq = jnp.sum(vfull[...] * vfull[...], keepdims=True)
    for copy in state_copies:
        copy.wait()

    def norm_copy(mask):
        return remote(norms.at[me], norms.at[me], ns_sem.at[mask - 1], nr_sem.at[mask - 1], mask)

    for mask in (6, 7, 2, 4, 3, 5, 1):
        norm_copy(mask).start()
    for c in (NC - 2, NC - 1):
        for b in send_slot:
            block_copy(b, c).wait_send()
        for h in (0, 1):
            rel_copy(h, c).wait_send()
    for mask in range(1, N_DEV):
        norm_copy(mask).wait_recv()
    total = norms[0]
    for k in range(1, N_DEV):
        total = total + norms[k]
    norm_sq = jnp.sum(total, keepdims=True) + vec_sq
    clip = jnp.minimum(1.0, MAX_NORM / (jnp.sqrt(norm_sq) + NORM_EPS))
    lr = lr_ref[...]

    upd_rows = 32
    clip_rows = jnp.broadcast_to(clip, (upd_rows, LANES))
    lr_rows = jnp.broadcast_to(lr, (upd_rows, LANES))

    def update_chunk(h, c, first=0, count=rc):
        def body(i, _):
            at = h * half + c * rc + first + i * upd_rows
            here = rows(at, upd_rows)
            new_p, new_m, new_v = adam_update(
                fin[here, :] * clip_rows, p_ref[here, :], m_ref[here, :], v_ref[here, :], lr_rows, WEIGHT_DECAY)
            p_ref[here, :] = new_p
            m_ref[here, :] = new_m
            v_ref[here, :] = new_v
            big[rows(me * piece_rows + at, upd_rows), :] = new_p.astype(BF16)
            return 0
        lax.fori_loop(0, count // upd_rows, body, 0, unroll=3)

    def gather_copy(mask, h, c, dest, ssem, slot):
        piece = flip(me, mask) if mask else me
        ref = big.at[rows(piece * piece_rows + h * half + c * rc, rc)]
        return remote(ref, ref, ag_sem.at[ssem], rs.at[slot, c], dest)

    def own_x(h, c):
        return gather_copy(0, h, c, 2, 0, h)

    def own_y(h, c):
        return gather_copy(0, h, c, 4, 1, 2 + h)

    def own_core(h, c):
        return gather_copy(0, h, c, 1, 2, 6 + h)

    def arrived(mask, h, c, slot):
        gather_copy(mask, h, c, 1, 0, slot).wait_recv()

    def to_core(mask, h, c):
        return gather_copy(mask, h, c, 1, {2: 5, 4: 6, 6: 7}[mask], {2: 8, 4: 10, 6: 12}[mask] + h)

    def diagonal(j):
        arrived(6, 0, j, 4)
        to_core(6, 0, j).start()
        arrived(6, 1, j, 5)
        to_core(6, 1, j).start()

    def first_half(i, _):
        @pl.when(i < NC)
        def _():
            @pl.when(i > 0)
            def _():
                update_chunk(0, i)
                own_x(0, i).start()
                update_chunk(1, i)
                own_y(1, i).start()
            own_core(0, i).start()
            own_core(1, i).start()

        @pl.when(i >= LAG)
        def _():
            j = i - LAG
            arrived(2, 0, j, 0)
            gather_copy(2, 0, j, 4, 3, 4).start()
            to_core(2, 0, j).start()
            arrived(4, 1, j, 3)
            gather_copy(4, 1, j, 2, 4, 5).start()
            to_core(4, 1, j).start()

        @pl.when(i >= DIAG_LAG)
        def _():
            diagonal(i - DIAG_LAG)

        @pl.when(i >= NC)
        def _():
            own_x(1, i - NC).start()
            own_y(0, i - NC).start()
        return 0

    for k in range(FIRST_PARTS):
        part = rc // FIRST_PARTS
        for h, dest, ssem in ((0, 2, 0), (1, 4, 1)):
            update_chunk(h, 0, k * part, part)
            ref = big.at[rows(me * piece_rows + h * half + k * part, part)]
            remote(ref, ref, ag_sem.at[ssem], rs.at[3 * h, 0], dest).start()
    lax.fori_loop(0, NC + LAG, first_half, 0)

    kept = half - TAIL * rc
    tail_copies = [
        pltpu.make_async_copy(
            big.at[rows(me * piece_rows + h * half + kept, TAIL * rc)], dst, px_sem.at[h])
        for h, dst in ((1, px_hbm), (0, py_hbm))
    ]
    for copy in tail_copies:
        copy.start()

    vrows = n_vec // LANES
    new_p, new_m, new_v = adam_update(
        vfull[pl.ds(0, vrows), :] * clip, pv_out[...], mv_out[...], vv_out[...], lr, 0.0)
    pv_out[...] = new_p
    mv_out[...] = new_m
    vv_out[...] = new_v

    def second_half(j, _):
        @pl.when(j + LAG < NC - TAIL)
        def _():
            own_x(1, j + LAG).start()
            own_y(0, j + LAG).start()
        @pl.when(j < DIAG_LAG - LAG)
        def _():
            diagonal(NC + LAG - DIAG_LAG + j)
        arrived(2, 1, j, 1)
        to_core(2, 1, j).start()
        arrived(4, 0, j, 2)
        to_core(4, 0, j).start()
        return 0

    lax.fori_loop(0, NC - TAIL, second_half, 0)

    def last_arrivals(c, _):
        for mask, h in ((1, 0), (1, 1), (3, 0), (5, 1), (7, 0), (7, 1)):
            arrived(mask, h, c, 5 + mask + h)

        @pl.when(c < NC - TAIL)
        def _():
            for mask, h in ((3, 1), (5, 0)):
                arrived(mask, h, c, 5 + mask + h)
        return 0

    lax.fori_loop(0, NC, last_arrivals, 0)
    for ssem, count in (
        (0, half + kept), (1, half + kept), (2, 2 * half), (3, half), (4, half),
        (5, half + kept), (6, half + kept), (7, 2 * half),
    ):
        ref = big.at[pl.ds(0, count)]
        remote(ref, ref, ag_sem.at[ssem], rs.at[0, 0], 1).wait_send()
    for mask in range(1, N_DEV):
        norm_copy(mask).wait_send()
    for copy in tail_copies:
        copy.wait()


def run_all(copies):
    for copy in copies:
        copy.start()
    for copy in copies:
        copy.wait()


def first_write(half, state, big, *refs):
    dsts, sem = refs[:-1], refs[-1]
    copies = []

    def add(src, src_at, dst, count, size):
        part = size // count
        for k in range(count):
            copies.append(pltpu.make_async_copy(
                src.at[pl.ds(src_at + k * part, part)], dst.at[pl.ds(k * part, part)], sem.at[len(copies)]))

    at = 0
    for dst in dsts[:6]:
        size = dst.shape[0]
        add(state, at, dst, 4 if size > 2 * VROWS else 1, size)
        at += max(size, 2 * VROWS)
    add(big, 0, dsts[6], SPLIT, SPLIT * half)
    run_all(copies)


def tail_copies_of(half, parts, dst, sem):
    me = lax.axis_index("dp")
    copies = []
    for i, (src, mask, h) in enumerate(parts):
        tail = src.shape[0]
        at = flip(me, mask) * (2 * half) + (h + 1) * half - tail
        copies.append(pltpu.make_async_copy(src, dst.at[pl.ds(pl.multiple_of(at, 16), tail)], sem.at[i]))
    return copies


def second_write(half, big, rx, ry, _, dst, sem):
    run_all([
        pltpu.make_async_copy(big.at[pl.ds(k * half, half)], dst.at[pl.ds(k * half, half)], sem.at[2 + k - SPLIT])
        for k in range(SPLIT, 2 * N_DEV)
    ])
    run_all(tail_copies_of(half, ((rx, 2, 1), (ry, 4, 0)), dst, sem))


def third_write(half, cx, cy, _, dst, sem):
    run_all(tail_copies_of(half, ((cx, 3, 1), (cy, 5, 0)), dst, sem))


def solution(mesh):
    axis_name = mesh.axis_names[0]

    def local_step(g_mat, g_vec, p_mat, m_mat, v_mat, p_vec, m_vec, v_vec, learn_rate):
        n_piece = p_mat.shape[0]
        n_vec = p_vec.shape[0]
        piece_rows = n_piece // LANES
        half = piece_rows // 2
        rc = half // NC
        state = (piece_rows, LANES)
        vec = (n_vec // LANES, LANES)
        full = (N_DEV * piece_rows, LANES)
        any_spec = pl.BlockSpec(memory_space=pl.ANY)
        vmem_spec = pl.BlockSpec(memory_space=pltpu.VMEM)
        state_new, big, px, py = pl.pallas_call(
            functools.partial(step_kernel, half, rc, n_vec),
            out_shape=[pltpu.VMEM((3 * piece_rows + 6 * VROWS, LANES), F32), pltpu.VMEM(full, BF16)]
            + [jax.ShapeDtypeStruct((TAIL * rc, LANES), BF16)] * 2,
            in_specs=[any_spec] * 9,
            out_specs=[vmem_spec] * 2 + [any_spec] * 2,
            scratch_shapes=[
                pltpu.VMEM(state, F32),
                pltpu.VMEM((NRAW, 1, rc * LANES), BF16),
                pltpu.VMEM((2, 12, rc, LANES), BF16),
                pltpu.VMEM((2, 2, rc, LANES), F32),
                pltpu.VMEM((8, LANES), F32),
                pltpu.VMEM((N_DEV, 8, LANES), F32),
                pltpu.VMEM((1, 2 * VROWS * LANES), BF16),
                pltpu.VMEM((2 * VROWS, LANES), BF16),
                pltpu.VMEM((VROWS, LANES), BF16),
                pltpu.VMEM((VROWS, LANES), F32),
                pltpu.VMEM((VROWS, LANES), F32),
                pltpu.VMEM((VROWS, LANES), F32),
                pltpu.VMEM((VROWS, LANES), F32),
                pltpu.VMEM((2 * VROWS, LANES), F32),
                pltpu.VMEM((1, 1), F32),
                pltpu.SemaphoreType.DMA((NRAW,)),
                pltpu.SemaphoreType.DMA((2, 12)),
                pltpu.SemaphoreType.DMA((2, 2)),
                pltpu.SemaphoreType.DMA((14, NC)),
                pltpu.SemaphoreType.DMA((8,)),
                pltpu.SemaphoreType.DMA((7,)),
                pltpu.SemaphoreType.DMA((7,)),
                pltpu.SemaphoreType.DMA((4,)),
                pltpu.SemaphoreType.DMA((4,)),
                pltpu.SemaphoreType.DMA((8,)),
                pltpu.SemaphoreType.DMA((2,)),
            ],
            compiler_params=pltpu.CompilerParams(
                collective_id=0, has_side_effects=True, vmem_limit_bytes=15 * 2 ** 20),
            name="step",
        )(
            g_mat, g_vec, p_mat.reshape(state), m_mat.reshape(state), v_mat.reshape(state),
            p_vec.reshape(vec), m_vec.reshape(vec), v_vec.reshape(vec), learn_rate.reshape(1, 1),
        )
        def permute(values, mask):
            return lax.ppermute(values, axis_name, [(d, d ^ mask) for d in range(N_DEV)])

        def cost(n_bytes):
            return pl.CostEstimate(flops=0, bytes_accessed=n_bytes, transcendentals=0)

        rx, ry = permute(px, 2), permute(py, 4)
        p_new, m_new, v_new, pv_new, mv_new, vv_new, pb = pl.pallas_call(
            functools.partial(first_write, half),
            out_shape=[jax.ShapeDtypeStruct(state, F32)] * 3 + [jax.ShapeDtypeStruct(vec, F32)] * 3
            + [jax.ShapeDtypeStruct(full, BF16)],
            in_specs=[vmem_spec] * 2,
            out_specs=[any_spec] * 7,
            scratch_shapes=[pltpu.SemaphoreType.DMA((15 + SPLIT,))],
            cost_estimate=cost(12 * n_piece + SPLIT * n_piece),
            compiler_params=pltpu.CompilerParams(vmem_limit_bytes=2 ** 20),
            name="write1",
        )(state_new, big)
        rx, ry, p_new = lax.optimization_barrier((rx, ry, p_new))
        cx, cy = permute(rx, 1), permute(ry, 1)
        pb = pl.pallas_call(
            functools.partial(second_write, half),
            out_shape=jax.ShapeDtypeStruct(full, BF16),
            in_specs=[vmem_spec] * 3 + [any_spec],
            out_specs=any_spec,
            input_output_aliases={3: 0},
            scratch_shapes=[pltpu.SemaphoreType.DMA((2 + 2 * N_DEV - SPLIT,))],
            cost_estimate=cost((2 * N_DEV - SPLIT) * n_piece),
            compiler_params=pltpu.CompilerParams(vmem_limit_bytes=2 * 2 ** 20),
            name="write2",
        )(big, rx, ry, pb)
        pb = pl.pallas_call(
            functools.partial(third_write, half),
            out_shape=jax.ShapeDtypeStruct(full, BF16),
            in_specs=[vmem_spec] * 2 + [any_spec],
            out_specs=any_spec,
            input_output_aliases={2: 0},
            scratch_shapes=[pltpu.SemaphoreType.DMA((2,))],
            compiler_params=pltpu.CompilerParams(vmem_limit_bytes=2 * 2 ** 20),
            name="write3",
        )(cx, cy, pb)
        return (
            p_new.reshape(-1), m_new.reshape(-1), v_new.reshape(-1),
            pv_new.reshape(-1), mv_new.reshape(-1), vv_new.reshape(-1), pb.reshape(-1),
        )

    return jax.shard_map(
        local_step,
        mesh=mesh,
        in_specs=(P(axis_name, None), P(axis_name, None), P(axis_name), P(axis_name), P(axis_name), P(), P(), P(), P()),
        out_specs=(P(axis_name), P(axis_name), P(axis_name), P(), P(), P(), P()),
        check_vma=False,
    )
```
